128 devices in a mesh: grp: 4 (over z), dom: 32 (over y, x, core).
Axes of the slice: x: 4, y: 4, z: 4, core: 2. Of those that a mesh axis runs over, the one named last changes fastest.
Arguments:
- fluid_start: float32 [4, 1024, 96, 128], P('grp', 'dom'), may hold values from -6 to 6
- fluid_rate: float32 [4, 1024, 96, 128], P('grp', 'dom'), may hold values from 0.15 to 0.45
- fluid_coupling: float32 [4, 1024, 128], P('grp', 'dom'), may hold values from 0.1 to 0.5
- solid_start: float32 [4, 512, 24, 128], P('grp', 'dom'), may hold values from -6 to 6
- solid_rate: float32 [4, 512, 24, 128], P('grp', 'dom'), may hold values from 0.2 to 0.6
- solid_coupling: float32 [4, 512, 128], P('grp', 'dom'), may hold values from 0.1 to 0.5
- solid_block: int32 [12288], P(('grp', 'dom')), may hold values from 0 to 511, as said below
- to_solid: bfloat16 [12288, 128, 128], P(('grp', 'dom')), as said below
- to_fluid: bfloat16 [12288, 128, 128], P(('grp', 'dom')), as said below
Outputs:
- fluid_temp: float32 [4, 1024, 96, 128], P('grp', 'dom')
- solid_temp: float32 [4, 512, 24, 128], P('grp', 'dom')
The draws below stay inside these ranges and needn't reach their ends.
Inputs may be any that keep to these rules, and one draw needn't show every extreme that they name: For segment s of fluid block x of its zone (x = (s // 3) mod 1024), solid_block[s] lies within x // 2 - 2 to x // 2 + 2, taken modulo 512. `to_solid`: entry [s, i, j] is zero unless i and j differ by at most one; all entries are nonnegative. `to_fluid`: entry [s, i, j] is zero unless i and j differ by at most one; all entries are nonnegative.
All inputs are finite; a program needn't handle non-finite values.
Results may differ from the reference program's by a relative error of at most 0.0003.
Values may be sent and summed in bfloat16 or wider, within the bound.
A program may use at most 128 MiB of HBM per device.

```python
import math
import jax
import jax.numpy as jnp
from jax import lax

FX = 32
FY = 96
FZ = 128
SX = 16
SEG_BLOCK = 3
PICARD = 4
SWEEPS = 2
SY = 24
SEG_DEV = 96
NXF = 1024
NXS = 512
NFB = 4096
NSEG = 12288
N_GRP = 4
N_DOM = 32


def parity_pattern(shape):
    along_x = lax.broadcasted_iota(jnp.int32, shape, 1)
    along_y = lax.broadcasted_iota(jnp.int32, shape, 2)
    along_z = lax.broadcasted_iota(jnp.int32, shape, 3)
    return (1 - 2 * ((along_x + along_y + along_z) % 2)).astype(jnp.float32)


def draw_fluid_start(key, part):
    shape = (N_GRP, NXF, FY, FZ)
    inner_key = jax.random.fold_in(key, 41)
    magnitude = jnp.clip(2.0 + 0.8 * jax.random.normal(inner_key, shape, jnp.float32), 0.25, 5.0)
    return (parity_pattern(shape) * magnitude).astype(jnp.float32)


def draw_solid_start(key, part):
    shape = (N_GRP, NXS, SY, FZ)
    inner_key = jax.random.fold_in(key, 43)
    magnitude = jnp.clip(2.0 + 0.8 * jax.random.normal(inner_key, shape, jnp.float32), 0.25, 5.0)
    return (parity_pattern(shape) * magnitude).astype(jnp.float32)


def draw_solid_block(key, part):
    jitter = jax.random.randint(jax.random.fold_in(key, 11), (NFB,), 0, 3).astype(jnp.int32)
    position = jnp.arange(NFB, dtype=jnp.int32) % NXF
    within = position % FX
    jitter = jnp.where(within == 0, 0, jnp.where(within == FX - 1, 2, jitter)).astype(jnp.int32)
    lowest = position // 2 + jitter - 2
    spread = lowest[:, None] + jnp.arange(SEG_BLOCK, dtype=jnp.int32)[None, :]
    return (spread % NXS).reshape(-1).astype(jnp.int32)


def intersect_fractions(key):
    shares = jax.random.uniform(jax.random.fold_in(key, 5), (NSEG // SEG_BLOCK, SEG_BLOCK), jnp.float32, 0.5, 1.5)
    return (shares / jnp.sum(shares, axis=1, keepdims=True)).reshape(-1)


def banded(key, salt):
    fractions = intersect_fractions(key)
    main_key, upper_key, lower_key = jax.random.split(jax.random.fold_in(key, salt), 3)
    centre = jax.random.uniform(main_key, (NSEG, FZ), jnp.float32, 1.0, 2.0)
    upper = jax.random.uniform(upper_key, (NSEG, FZ), jnp.float32, 0.2, 0.5)
    lower = jax.random.uniform(lower_key, (NSEG, FZ), jnp.float32, 0.2, 0.5)
    column = jnp.arange(FZ, dtype=jnp.int32)[None, :]
    upper = jnp.where(column >= 1, upper, 0.0)
    lower = jnp.where(column <= FZ - 2, lower, 0.0)
    scaling = fractions[:, None] / (centre + upper + lower)
    centre = centre * scaling
    upper = upper * scaling
    lower = lower * scaling

    def build(pieces):
        centre_part, upper_part, lower_part = pieces
        rows = lax.broadcasted_iota(jnp.int32, (FZ, FZ), 0)
        cols = lax.broadcasted_iota(jnp.int32, (FZ, FZ), 1)
        matrix = jnp.where(rows == cols, centre_part[:, None, :], jnp.where(rows == cols - 1, upper_part[:, None, :], jnp.where(rows == cols + 1, lower_part[:, None, :], 0.0)))
        return matrix.astype(jnp.bfloat16)
    groups = NSEG // SEG_DEV
    built = lax.map(build, (centre.reshape(groups, SEG_DEV, FZ), upper.reshape(groups, SEG_DEV, FZ), lower.reshape(groups, SEG_DEV, FZ)))
    return built.reshape(NSEG, FZ, FZ)


def draw_to_solid(key, part):
    return banded(key, 21)


def draw_to_fluid(key, part):
    return banded(key, 23)


def shard_levels(key, dims, cuts, least, top_value):
    gain, own = 1.0, jax.random.fold_in(key, 6)
    for dim, shards_of in cuts:
        draws = jnp.exp(jax.random.uniform(jax.random.fold_in(own, dim), (shards_of,), jnp.float32, least / len(cuts), top_value / len(cuts)))
        gain = gain * jnp.repeat(draws, dims[dim] // shards_of).reshape([-1 if axis == dim else 1 for axis in range(len(dims))])
    return gain


def setup_inputs(seed: int = 0) -> dict:
    streams_of = jax.random.split(jax.random.key(seed), 10)
    return {
        "fluid_start": draw_fluid_start(jax.random.fold_in(streams_of[9], 71), 0),
        "fluid_rate": jnp.clip(jnp.exp(math.log(0.45) - 1.0986122 * jax.random.uniform(streams_of[1], (N_GRP, NXF, FY, FZ), jnp.float32) ** shard_levels(streams_of[1], (N_GRP, NXF, FY, FZ), ((0, 4), (1, 32)), -0.2, 0.2)), 0.15, 0.45),
        "fluid_coupling": jnp.clip(jnp.exp(math.log(0.5) - 1.609438 * jax.random.uniform(streams_of[2], (N_GRP, NXF, FZ), jnp.float32) ** shard_levels(streams_of[2], (N_GRP, NXF, FZ), ((0, 4), (1, 32)), -0.2, 0.2)), 0.1, 0.5),
        "solid_start": draw_solid_start(jax.random.fold_in(streams_of[9], 71), 0),
        "solid_rate": jnp.clip(jnp.exp(math.log(0.6) - 1.0986123 * jax.random.uniform(streams_of[4], (N_GRP, NXS, SY, FZ), jnp.float32) ** shard_levels(streams_of[4], (N_GRP, NXS, SY, FZ), ((0, 4), (1, 32)), -0.2, 0.2)), 0.2, 0.6),
        "solid_coupling": jnp.clip(jnp.exp(math.log(0.5) - 1.609438 * jax.random.uniform(streams_of[5], (N_GRP, NXS, FZ), jnp.float32) ** shard_levels(streams_of[5], (N_GRP, NXS, FZ), ((0, 4), (1, 32)), -0.2, 0.2)), 0.1, 0.5),
        "solid_block": draw_solid_block(jax.random.fold_in(streams_of[9], 71), 0),
        "to_solid": draw_to_solid(jax.random.fold_in(streams_of[9], 71), 0),
        "to_fluid": draw_to_fluid(jax.random.fold_in(streams_of[9], 71), 0),
    }


def neighbours(field_now):
    padded = jnp.pad(field_now, ((0, 0), (1, 1), (1, 1), (1, 1)))
    summed = padded[:, 2:, 1:-1, 1:-1] + padded[:, :-2, 1:-1, 1:-1]
    summed = summed + padded[:, 1:-1, 2:, 1:-1] + padded[:, 1:-1, :-2, 1:-1]
    summed = summed + padded[:, 1:-1, 1:-1, 2:] + padded[:, 1:-1, 1:-1, :-2]
    return summed


def relax(summed, base_value, rate_value, film_value, incoming, plane_row):
    numerator = base_value + rate_value * summed
    denominator = 1.0 + 6.0 * rate_value
    numerator = numerator.at[:, :, plane_row, :].add(film_value * incoming)
    denominator = denominator.at[:, :, plane_row, :].add(film_value)
    return numerator / denominator


def reference(fluid_start, fluid_rate, fluid_coupling, solid_start, solid_rate, solid_coupling, solid_block, to_solid, to_fluid):
    devices = N_GRP * N_DOM
    fluid_blocks = devices * FX
    solid_blocks = devices * SX
    seg_ids = jnp.arange(NSEG, dtype=jnp.int32)
    fluid_ids = seg_ids // SEG_BLOCK
    zone_ids = seg_ids // (SEG_DEV * N_DOM)
    solid_ids = ((zone_ids + 1) % N_GRP) * NXS + solid_block
    fluid_now = fluid_start
    solid_now = solid_start
    for iteration in range(PICARD):
        fluid_face = fluid_now[:, :, 0, :].reshape(fluid_blocks, FZ).astype(jnp.bfloat16)
        solid_face = solid_now[:, :, -1, :].reshape(solid_blocks, FZ).astype(jnp.bfloat16)

        def project(pieces):
            fluid_part, solid_part, solid_mats, fluid_mats = pieces
            solid_terms = jnp.einsum("sk,skm->sm", fluid_face[fluid_part].astype(jnp.float32), solid_mats.astype(jnp.float32))
            fluid_terms = jnp.einsum("sk,skm->sm", solid_face[solid_part].astype(jnp.float32), fluid_mats.astype(jnp.float32))
            return solid_terms, fluid_terms

        solid_terms, fluid_terms = lax.map(project, (
            fluid_ids.reshape(devices, SEG_DEV),
            solid_ids.reshape(devices, SEG_DEV),
            to_solid.reshape(devices, SEG_DEV, FZ, FZ),
            to_fluid.reshape(devices, SEG_DEV, FZ, FZ)))
        solid_in = jax.ops.segment_sum(solid_terms.reshape(-1, FZ), solid_ids, num_segments=solid_blocks)
        fluid_in = jax.ops.segment_sum(fluid_terms.reshape(-1, FZ), fluid_ids, num_segments=fluid_blocks)
        solid_in = solid_in.reshape(N_GRP, NXS, FZ)
        fluid_in = fluid_in.reshape(N_GRP, NXF, FZ)
        for sweep_no in range(SWEEPS):
            fluid_now = relax(neighbours(fluid_now), fluid_start, fluid_rate, fluid_coupling, fluid_in, 0)
            solid_now = relax(neighbours(solid_now), solid_start, solid_rate, solid_coupling, solid_in, -1)
    return fluid_now, solid_now
```

```python
import jax
import jax.numpy as jnp
from jax import lax
from jax.experimental import pallas as pl
from jax.experimental.pallas import tpu as pltpu
from jax.sharding import PartitionSpec as P

MESH = pl.DeviceIdType.MESH
F32 = jnp.float32
BF16 = jnp.bfloat16
FX, FY, FZ = 32, 96, 128
SX, SY = 16, 24
SEG = 96
GROUP = 16


def lane_iota(shape):
    return lax.broadcasted_iota(jnp.int32, shape, 1)


def zsum(v):
    lane = lane_iota(v.shape)
    return jnp.where(lane == 0, 0.0, pltpu.roll(v, 1, 1)) + jnp.where(
        lane == FZ - 1, 0.0, pltpu.roll(v, FZ - 1, 1)
    )


def ysum(v):
    zero = jnp.zeros((1, FZ), F32)
    return jnp.concatenate([zero, v[:-1]], axis=0) + jnp.concatenate([v[1:], zero], axis=0)


def rows_loop(lo, hi, unroll, body):
    count = hi - lo
    groups = count // unroll if count > unroll else 0
    if groups:

        def step(i, carry):
            for j in range(unroll):
                body(lo + i * unroll + j)
            return carry

        lax.fori_loop(0, groups, step, 0)
    for x in range(lo + groups * unroll, hi):
        body(x)


def at_row(x, pitch):
    return x * pitch if isinstance(x, int) else pl.multiple_of(x * pitch, 8)


def to_f32(v):
    return v.astype(F32)


def rounded(v):
    return v.astype(BF16).astype(F32)


def kernel(
    n_grp, n_dom,
    fs, fr, fc, ss, sr, sc, sb, ts, tf,
    fo, so,
    p, q, a, b, bt, sp, sq, sa, sbb, sbt,
    mt, yy, xf0, xf1, xf2, xr, xa, xb, xs0, xs1, xsr, xsa, xsb,
    dx, vv, ww, pad, tpad, fin, sin, sins, fxx, fsx, xoff,
    fcv, scv, sbv,
    ifs, is_, wb, bhl, bhr, shl, shr, mhl, mhr,
    rfl, rfr, fcl, fcr, sbl, sbr, rso, rsr, rsl, sco, scr, scl, scbr, scbl,
    wr, wl, bhrr, bhlr, shrr, shlr, mhrr, mhlr, sinr,
    load_sem, send_sem, recv_sem,
):
    g = lax.axis_index("grp")
    d = lax.axis_index("dom")
    gm, gp = lax.rem(g + n_grp - 1, n_grp), lax.rem(g + 1, n_grp)
    dm, dp = lax.rem(d + n_dom - 1, n_dom), lax.rem(d + 1, n_dom)
    ml = jnp.where(d > 0, 1.0, 0.0).astype(F32)
    mr = jnp.where(d < n_dom - 1, 1.0, 0.0).astype(F32)

    barrier = pltpu.get_barrier_semaphore()
    peers = ((g, dm), (g, dp), (gm, d), (gp, d), (gm, dm), (gm, dp), (gp, dm), (gp, dp))
    for peer in peers:
        pl.semaphore_signal(barrier, inc=1, device_id=peer, device_id_type=MESH)

    loads = {}

    def load(name, src, dst, index):
        loads[name] = pltpu.make_async_copy(src, dst, load_sem.at[index])
        loads[name].start()

    load("ss", ss, sp.at[pl.ds(8 * SY, SX * SY)], 0)
    load("sr", sr, sa.at[pl.ds(8 * SY, SX * SY)], 1)
    load("fs", fs, p.at[pl.ds(4 * FY, FX * FY)], 2)
    load("fr", fr, a.at[pl.ds(4 * FY, FX * FY)], 3)
    load("sc", sc, scv, 4)
    load("fc", fc, fcv, 5)
    load("sb", sb, sbv, 6)
    chunk = GROUP * FZ
    for t, src in ((0, ts), (1, tf)):
        for c in range(SEG // GROUP):
            load(
                ("m", t, c), src.at[pl.ds(c * chunk, chunk)],
                mt.at[pl.ds((t * SEG * FZ) + c * chunk, chunk)], 7 + t * 6 + c,
            )

    sends = []

    def send(src, dst, index, peer):
        copy = pltpu.make_async_remote_copy(
            src_ref=src, dst_ref=dst, send_sem=send_sem.at[index], recv_sem=recv_sem.at[index],
            device_id=peer, device_id_type=MESH,
        )
        copy.start()
        sends.append(copy)
        return copy

    loads["ss"].wait()
    loads["sr"].wait()
    for f, ref in ((0, sp), (1, sa)):
        for i in range(SX // 2):
            lo = (8 + 2 * i) * SY + 16
            is_[f, pl.ds(16 * i, 16), :] = jnp.concatenate(
                [ref[pl.ds(lo, 8), :], ref[pl.ds(lo + SY, 8), :]], axis=0
            ).astype(BF16)
        shl[f] = ref[pl.ds(8 * SY, 8 * SY), :].astype(BF16)
        shr[f] = ref[pl.ds(16 * SY, 8 * SY), :].astype(BF16)
    loads["fs"].wait()
    loads["fr"].wait()
    for f, ref in ((0, p), (1, a)):
        for i in range(FX // 2):
            lo = (4 + 2 * i) * FY
            pair = jnp.concatenate([ref[pl.ds(lo, 8), :], ref[pl.ds(lo + FY, 8), :]], axis=0)
            ifs[f, pl.ds(16 * i, 16), :] = pair.astype(BF16)
            own = xf0 if f == 0 else xr
            own[pl.ds((FX + 2 * i) * 8, 16), :] = pair
    loads["sc"].wait()
    loads["fc"].wait()
    loads["sb"].wait()
    pl.semaphore_wait(barrier, 8)

    recv = {}
    recv["rso"] = send(is_, rso, 6, (gm, d))
    recv["rsr"] = send(is_, rsr, 7, (gm, dm))
    recv["rsl"] = send(is_, rsl, 8, (gm, dp))
    recv["rfr"] = send(ifs.at[:, pl.ds(0, 192)], rfr, 0, (g, dm))
    recv["rfl"] = send(ifs.at[:, pl.ds(64, 192)], rfl, 1, (g, dp))
    recv["fcr"] = send(fcv, fcr, 2, (g, dm))
    recv["fcl"] = send(fcv, fcl, 3, (g, dp))
    recv["sbr"] = send(sbv, sbr, 4, (g, dm))
    recv["sbl"] = send(sbv, sbl, 5, (g, dp))
    recv["sco"] = send(scv, sco, 9, (gm, d))
    recv["scr"] = send(scv, scr, 10, (gm, dm))
    recv["scl"] = send(scv, scl, 11, (gm, dp))
    recv["scbr"] = send(scv, scbr, 12, (g, dm))
    recv["scbl"] = send(scv, scbl, 13, (g, dp))

    prow = lax.broadcasted_iota(jnp.int32, (8, FZ), 0)
    pcol = lane_iota((8, FZ))
    probe = jnp.where(lax.rem(pcol, 3) == prow, 1.0, 0.0).astype(BF16)
    for t in range(2):
        for c in range(SEG // GROUP):
            loads[("m", t, c)].wait()
            for s in range(GROUP):
                at = t * SEG + c * GROUP + s
                yy[pl.ds(at * 8, 8), :] = jnp.dot(
                    probe, mt[pl.ds(at * FZ, FZ), :], preferred_element_type=F32
                )
        y3 = [yy[pl.ds(t * SEG * 8 + c, SEG, stride=8), :] for c in range(3)]
        phase = lax.rem(lane_iota((SEG, FZ)), 3)
        for k, shift in enumerate((0, 2, 1)):
            picked = y3[(0 + shift) % 3]
            picked = jnp.where(phase == 1, y3[(1 + shift) % 3], picked)
            picked = jnp.where(phase == 2, y3[(2 + shift) % 3], picked)
            if k == 1:
                picked = jnp.where(lane_iota((SEG, FZ)) == 0, 0.0, picked)
            if k == 2:
                picked = jnp.where(lane_iota((SEG, FZ)) == FZ - 1, 0.0, picked)
            dx[3 * t + k, pl.ds(SEG, SEG), :] = picked
            wb[3 * t + k] = picked.astype(BF16)
    recv["wr"] = send(wb.at[:, pl.ds(0, 80)], wr, 14, (g, dm))
    recv["wl"] = send(wb.at[:, pl.ds(16, 80)], wl, 15, (g, dp))

    for i in range(4):
        bhl[pl.ds(i * FY, FY), :] = p[pl.ds((4 + i) * FY, FY), :].astype(BF16)
        bhr[pl.ds(i * FY, FY), :] = p[pl.ds((32 + i) * FY, FY), :].astype(BF16)
    for i in range(3):
        bhl[pl.ds((4 + i) * FY, FY), :] = a[pl.ds((4 + i) * FY, FY), :].astype(BF16)
        bhr[pl.ds((4 + i) * FY, FY), :] = a[pl.ds((33 + i) * FY, FY), :].astype(BF16)
    recv["bhrr"] = send(bhl, bhrr, 16, (g, dm))
    recv["bhlr"] = send(bhr, bhlr, 17, (g, dp))
    recv["shrr"] = send(shl, shrr, 18, (g, dm))
    recv["shlr"] = send(shr, shlr, 19, (g, dp))

    def coef(start_ref, rate_ref, a_ref, b_ref, lo, size):
        r = rate_ref[pl.ds(lo, size), :]
        inv = 1.0 / (1.0 + 6.0 * r)
        b_ref[pl.ds(lo, size), :] = start_ref[pl.ds(lo, size), :] * inv
        a_ref[pl.ds(lo, size), :] = r * inv

    def film_coef(r0, s0, film):
        inv0 = 1.0 / (1.0 + 6.0 * r0 + film)
        return r0 * inv0, s0 * inv0, film * inv0

    own_rows = pl.ds(4 * FY, FX, stride=FY)
    a0, b0, _ = film_coef(a[own_rows, :], p[own_rows, :], fcv[...])
    rows_loop(4, 36, 4, lambda x: coef(p, a, a, b, at_row(x, FY), FY))
    a[own_rows, :] = a0
    b[own_rows, :] = b0

    def fluid_row(src, dst, variant, x):
        base = at_row(x, FY)
        cur = src[pl.ds(base, FY), :]
        summed = src[pl.ds(base - FY, FY), :] + src[pl.ds(base + FY, FY), :]
        summed = summed + ysum(cur) + zsum(cur)
        if variant is None:
            fixed = b[pl.ds(base, FY), :]
        else:
            low = bt[pl.ds(variant * 320 + at_row(x, 8), 8), :]
            fixed = jnp.concatenate([low, b[pl.ds(base + 8, FY - 8), :]], axis=0)
        dst[pl.ds(base, FY), :] = fixed + a[pl.ds(base, FY), :] * summed

    def interior(variants):
        for m in range(4):
            src, dst = (p, q) if m % 2 == 0 else (q, p)
            rows_loop(
                5 + m, 35 - m, 8, lambda x: fluid_row(src, dst, variants[m], x)
            )

    def edges(variants):
        for m in range(4):
            src, dst = (p, q) if m % 2 == 0 else (q, p)
            for x0 in (1 + m, 35 - m):
                for x in range(x0, x0 + 4):
                    fluid_row(src, dst, variants[m], x)

    interior((None,) * 4)

    recv["rfl"].wait_recv()
    recv["rfr"].wait_recv()
    recv["fcl"].wait_recv()
    recv["fcr"].wait_recv()
    for f, ref in ((0, xf0), (1, xr)):
        ref[pl.ds(64, 192), :] = to_f32(rfl[f])
        ref[pl.ds(512, 192), :] = to_f32(rfr[f])
    fxx[pl.ds(0, FX), :] = fcl[...]
    fxx[pl.ds(FX, FX), :] = fcv[...]
    fxx[pl.ds(2 * FX, FX), :] = fcr[...]
    rows_loop(1, 11, 2, lambda x: coef(xf0, xr, xa, xb, at_row(x, 64), 64))
    xc = []
    xb0 = []
    for par in range(2):
        rows = pl.ds(par * 8, 48, stride=16)
        film = fxx[pl.ds(par, 48, stride=2), :]
        a0, b0, c0 = film_coef(xr[rows, :], xf0[rows, :], film)
        xa[rows, :] = a0
        fin[par] = b0
        fin[2 + par] = c0
        xc.append(2 + par)
        xb0.append(par)

    for name in ("rso", "rsr", "rsl", "sco", "scr", "scl"):
        recv[name].wait_recv()
    for f, ref in ((0, xs0), (1, xsr)):
        ref[pl.ds(0, 128), :] = to_f32(rsl[f])
        ref[pl.ds(128, 128), :] = to_f32(rso[f])
        ref[pl.ds(256, 128), :] = to_f32(rsr[f])
    rows_loop(0, 6, 2, lambda x: coef(xs0, xsr, xsa, xsb, at_row(x, 64), 64))
    srows = pl.ds(7, 48, stride=8)
    film = jnp.concatenate([scl[...], sco[...], scr[...]], axis=0)
    a0, b0, c0 = film_coef(xsr[srows, :], xs0[srows, :], film)
    xsa[srows, :] = a0
    sin[0] = b0
    sin[1] = c0

    for name in ("sbl", "sbr", "wl", "wr"):
        recv[name].wait_recv()
    for k in range(6):
        dx[k, pl.ds(16, 80), :] = to_f32(wl[k])
        dx[k, pl.ds(192, 80), :] = to_f32(wr[k])
    for n, ref in enumerate((sbl, sbv, sbr)):
        spread = jnp.broadcast_to(ref[...].astype(F32), (FZ, FZ)).T
        xoff[pl.ds(n * SEG, SEG), :] = spread[:SEG].astype(jnp.int32)
    first = SX * (d + n_dom - 1) - 2
    zone = SX * n_dom
    half = lax.broadcasted_iota(jnp.int32, (48, FZ), 0) + first
    for par in range(2):
        offs = [
            lax.rem(xoff[pl.ds(3 * par + j, 48, stride=6), :] - half + 3 * zone, zone)
            for j in range(3)
        ]
        for t in range(2):
            for k in range(3):
                diag = [dx[3 * t + k, pl.ds(3 * par + j, 48, stride=6), :] for j in range(3)]
                for o in range(5):
                    total = jnp.where(offs[0] == o, diag[0], 0.0)
                    total = total + jnp.where(offs[1] == o, diag[1], 0.0)
                    total = total + jnp.where(offs[2] == o, diag[2], 0.0)
                    at = (o * 3 + k) * 2 + par
                    if t == 0:
                        ww[at] = total
                    else:
                        vv[at] = total * fin[xc[par]]

    def shifts(v):
        return (v, pltpu.roll(v, 1, 1), pltpu.roll(v, FZ - 1, 1))

    def project_fluid(solid_ref, k):
        for n, v in enumerate(shifts(rounded(solid_ref[srows, :]))):
            pad[n, pl.ds(8, 48), :] = v
        for par in range(2):
            total = jnp.zeros((48, FZ), F32)
            for o in range(5):
                for n in range(3):
                    total = total + vv[(o * 3 + n) * 2 + par] * pad[n, pl.ds(6 + o, 48), :]
            fin[4 + 2 * k + par] = total

    def project_solid(fluid_ref, k):
        faces = [shifts(rounded(fluid_ref[pl.ds(par * 8, 48, stride=16), :])) for par in range(2)]
        for o in range(5):
            total = jnp.zeros((48, FZ), F32)
            for par in range(2):
                for n in range(3):
                    total = total + ww[(o * 3 + n) * 2 + par] * faces[par][n]
            tpad[o, pl.ds(8, 48), :] = total
        total = tpad[0, pl.ds(10, 48), :]
        for o in range(1, 5):
            total = total + tpad[o, pl.ds(10 - o, 48), :]
        sin[2 + k] = total
        sins[k] = total[8:40]

    def face_row(src, dst, a_ref, b_ref, cut_left, cut_right, x):
        base = at_row(x, 8)
        cur = src[pl.ds(base, 8), :]
        keep_left = jnp.where(cut_left(x), 0.0, 1.0).astype(F32)
        keep_right = jnp.where(cut_right(x), 0.0, 1.0).astype(F32)
        summed = src[pl.ds(base - 8, 8), :] * keep_left + src[pl.ds(base + 8, 8), :] * keep_right
        summed = summed + ysum(cur) + zsum(cur)
        dst[pl.ds(base, 8), :] = b_ref[pl.ds(base, 8), :] + a_ref[pl.ds(base, 8), :] * summed

    at_first, at_last = d == 0, d == n_dom - 1

    def cuts(width):
        def cut_left(x):
            return ((x == width) & at_first) | ((x == 2 * width) & at_last)

        def cut_right(x):
            return ((x == width - 1) & at_first) | ((x == 2 * width - 1) & at_last)

        return cut_left, cut_right

    fcut, scut = cuts(FX), cuts(SX)
    fluid_span = (((13, 83), (14, 82)), ((19, 77), (20, 76)), ((25, 71), (26, 70)))
    solid_span = (((6, 42), (7, 41)), ((9, 39), (10, 38)), ((12, 36), (13, 35)))
    fluid_refs = (xf0, xf0, xf2)
    fluid_out = (xf0, xf2, xf0)
    for k in range(4):
        fluid_ref = (xf0, xf0, xf2, xf0)[k]
        project_fluid(xs0, k)
        project_solid(fluid_ref, k)
        if k == 3:
            break
        for par in range(2):
            xb[pl.ds(par * 8, 48, stride=16), :] = fin[xb0[par]] + fin[4 + 2 * k + par]
        xsb[srows, :] = sin[0] + sin[1] * sin[2 + k]
        for n in range(2):
            lo, hi = fluid_span[k][n]
            src, dst = (fluid_refs[k], xf1) if n == 0 else (xf1, fluid_out[k])
            rows_loop(lo, hi, 8, lambda x: face_row(src, dst, xa, xb, *fcut, x))
            lo, hi = solid_span[k][n]
            src, dst = (xs0, xs1) if n == 0 else (xs1, xs0)
            rows_loop(lo, hi, 8, lambda x: face_row(src, dst, xsa, xsb, *scut, x))
    recv["sinr"] = send(sins, sinr, 22, (gp, d))

    recv["bhlr"].wait_recv()
    recv["bhrr"].wait_recv()
    for ref, first_row, mask, film_at in ((bhlr, 0, ml, 28), (bhrr, 36, mr, 64)):
        for i in range(4):
            p[pl.ds((first_row + i) * FY, FY), :] = to_f32(ref[pl.ds(i * FY, FY), :]) * mask
        skip = 1 if first_row == 0 else 0
        for i in range(3):
            row = first_row + skip + i
            a[pl.ds(row * FY, FY), :] = to_f32(ref[pl.ds((4 + i) * FY, FY), :]) * mask
        for i in range(3):
            row = first_row + skip + i
            film = fxx[pl.ds(film_at + skip + i, 1), :]
            r0, s0 = a[pl.ds(row * FY, 1), :], p[pl.ds(row * FY, 1), :]
            a0, b0, _ = film_coef(r0, s0, film)
            coef(p, a, a, b, row * FY, FY)
            a[pl.ds(row * FY, 1), :] = a0
            b[pl.ds(row * FY, 1), :] = b0
    edges((None,) * 4)
    mhl[...] = p[pl.ds(4 * FY, 4 * FY), :].astype(BF16)
    mhr[...] = p[pl.ds(32 * FY, 4 * FY), :].astype(BF16)
    recv["mhrr"] = send(mhl, mhrr, 20, (g, dm))
    recv["mhlr"] = send(mhr, mhlr, 21, (g, dp))

    wide = lax.broadcasted_iota(jnp.int32, (20, FZ), 0)
    inside = jnp.where(wide < 2, ml, jnp.where(wide >= 18, mr, 1.0))
    for v in range(2):
        for i in range(1, 39):
            bt[pl.ds(v * 320 + i * 8, 8), :] = b[pl.ds(i * FY, 8), :]
        for par in range(2):
            rows = pl.ds(v * 320 + par * 8, 20, stride=16)
            bt[rows, :] = bt[rows, :] + fin[4 + 2 * (2 + v) + par][14:34] * inside

    def patch(i, mask):
        low = lax.broadcasted_iota(jnp.int32, (8, FZ), 0) < 4
        fresh = xf2[pl.ds((28 + i) * 8, 8), :]
        if mask is not None:
            fresh = fresh * mask
        p[pl.ds(i * FY, 8), :] = jnp.where(low, fresh, p[pl.ds(i * FY, 8), :])

    for i in range(4, 36):
        patch(i, None)
    second = (0, 0, 1, 1)
    interior(second)
    out_mid = pltpu.make_async_copy(
        p.at[pl.ds(8 * FY, 24 * FY)], fo.at[pl.ds(4 * FY, 24 * FY)], load_sem.at[19]
    )
    out_mid.start()

    for name in ("scbl", "scbr", "shlr", "shrr", "sinr"):
        recv[name].wait_recv()
    for f, ref in ((0, sp), (1, sa)):
        ref[pl.ds(0, 8 * SY), :] = to_f32(shlr[f]) * ml
        ref[pl.ds(24 * SY, 8 * SY), :] = to_f32(shrr[f]) * mr
    fsx[pl.ds(0, 8), :] = scbl[pl.ds(8, 8), :] * ml
    fsx[pl.ds(8, SX), :] = scv[...]
    fsx[pl.ds(24, 8), :] = scbr[pl.ds(0, 8), :] * mr
    last_rows = pl.ds(SY - 1, 32, stride=SY)
    a0, b0, c0 = film_coef(sa[last_rows, :], sp[last_rows, :], fsx[...])
    rows_loop(0, 8, 2, lambda x: coef(sp, sa, sa, sbb, at_row(x, 96), 96))
    sa[last_rows, :] = a0
    sbb[last_rows, :] = b0
    for k in range(4):
        for i in range(32):
            sbt[pl.ds(k * 256 + i * 8, 8), :] = sbb[pl.ds(i * SY + 16, 8), :]
        sbt[pl.ds(k * 256 + 7, 32, stride=8), :] = b0 + c0 * sinr[k]

    def solid_row(src, dst, variant, x):
        base = at_row(x, SY)
        cur = src[pl.ds(base, SY), :]
        summed = src[pl.ds(base - SY, SY), :] + src[pl.ds(base + SY, SY), :]
        summed = summed + ysum(cur) + zsum(cur)
        high = sbt[pl.ds(variant * 256 + at_row(x, 8), 8), :]
        fixed = jnp.concatenate([sbb[pl.ds(base, 16), :], high], axis=0)
        dst[pl.ds(base, SY), :] = fixed + sa[pl.ds(base, SY), :] * summed

    for m in range(8):
        src, dst = (sp, sq) if m % 2 == 0 else (sq, sp)
        rows_loop(1 + m, 31 - m, 8, lambda x: solid_row(src, dst, m // 2, x))
    out_solid = pltpu.make_async_copy(sp.at[pl.ds(8 * SY, SX * SY)], so, load_sem.at[20])
    out_solid.start()

    recv["mhlr"].wait_recv()
    recv["mhrr"].wait_recv()
    p[pl.ds(0, 4 * FY), :] = to_f32(mhlr[...]) * ml
    p[pl.ds(36 * FY, 4 * FY), :] = to_f32(mhrr[...]) * mr
    for i in range(4):
        patch(i, ml)
        patch(36 + i, mr)
    edges(second)
    outs = []
    for n, i in enumerate((4, 32)):
        copy = pltpu.make_async_copy(
            p.at[pl.ds(i * FY, 4 * FY)], fo.at[pl.ds((i - 4) * FY, 4 * FY)], load_sem.at[21 + n]
        )
        copy.start()
        outs.append(copy)
    for copy in sends:
        copy.wait_send()
    for copy in (out_mid, out_solid, *outs):
        copy.wait()


def vm(*shape, dtype=F32):
    return pltpu.VMEM(shape, dtype)


SCRATCH = [
    *(vm(40 * FY, FZ) for _ in range(4)), vm(2 * 320, FZ),
    *(vm(32 * SY, FZ) for _ in range(4)), vm(4 * 256, FZ),
    vm(2 * SEG * FZ, FZ, dtype=BF16), vm(2 * SEG * 8, FZ),
    *(vm(96 * 8, FZ) for _ in range(6)), *(vm(48 * 8, FZ) for _ in range(5)),
    vm(6, 3 * SEG, FZ), vm(30, 48, FZ), vm(30, 48, FZ), vm(3, 64, FZ), vm(5, 64, FZ),
    vm(12, 48, FZ), vm(6, 48, FZ), vm(4, 32, FZ), vm(96, FZ), vm(32, FZ),
    vm(3 * SEG, FZ, dtype=jnp.int32),
    vm(FX, FZ), vm(SX, FZ), vm(1, FZ, dtype=jnp.int32),
    vm(2, 256, FZ, dtype=BF16), vm(2, 128, FZ, dtype=BF16), vm(6, SEG, FZ, dtype=BF16),
    vm(7 * FY, FZ, dtype=BF16), vm(7 * FY, FZ, dtype=BF16),
    vm(2, 8 * SY, FZ, dtype=BF16), vm(2, 8 * SY, FZ, dtype=BF16),
    vm(4 * FY, FZ, dtype=BF16), vm(4 * FY, FZ, dtype=BF16),
    vm(2, 192, FZ, dtype=BF16), vm(2, 192, FZ, dtype=BF16), vm(FX, FZ), vm(FX, FZ),
    vm(1, FZ, dtype=jnp.int32), vm(1, FZ, dtype=jnp.int32),
    *(vm(2, 128, FZ, dtype=BF16) for _ in range(3)), *(vm(SX, FZ) for _ in range(5)),
    vm(6, 80, FZ, dtype=BF16), vm(6, 80, FZ, dtype=BF16),
    vm(7 * FY, FZ, dtype=BF16), vm(7 * FY, FZ, dtype=BF16),
    vm(2, 8 * SY, FZ, dtype=BF16), vm(2, 8 * SY, FZ, dtype=BF16),
    vm(4 * FY, FZ, dtype=BF16), vm(4 * FY, FZ, dtype=BF16), vm(4, 32, FZ),
    pltpu.SemaphoreType.DMA((24,)), pltpu.SemaphoreType.DMA((23,)), pltpu.SemaphoreType.DMA((23,)),
]


def solution(mesh):
    n_grp, n_dom = mesh.shape["grp"], mesh.shape["dom"]

    def local(fs, fr, fc, ss, sr, sc, sb, ts, tf):
        fo, so = pl.pallas_call(
            lambda *refs: kernel(n_grp, n_dom, *refs),
            out_shape=(
                jax.ShapeDtypeStruct((FX * FY, FZ), F32),
                jax.ShapeDtypeStruct((SX * SY, FZ), F32),
            ),
            in_specs=[pl.BlockSpec(memory_space=pl.ANY)] * 9,
            out_specs=[pl.BlockSpec(memory_space=pl.ANY)] * 2,
            scratch_shapes=SCRATCH,
            compiler_params=pltpu.CompilerParams(
                collective_id=0, has_side_effects=True, vmem_limit_bytes=56 * 1024 * 1024
            ),
            name="coupled",
        )(
            fs.reshape(FX * FY, FZ), fr.reshape(FX * FY, FZ), fc.reshape(FX, FZ),
            ss.reshape(SX * SY, FZ), sr.reshape(SX * SY, FZ), sc.reshape(SX, FZ),
            jnp.pad(sb, (0, FZ - SEG)).reshape(1, FZ),
            ts.reshape(SEG * FZ, FZ), tf.reshape(SEG * FZ, FZ),
        )
        return fo.reshape(1, FX, FY, FZ), so.reshape(1, SX, SY, FZ)

    cells = P("grp", "dom", None, None)
    faces = P("grp", "dom", None)
    split = P(("grp", "dom"))
    mats = P(("grp", "dom"), None, None)
    return jax.shard_map(
        local,
        mesh=mesh,
        in_specs=(cells, cells, faces, cells, cells, faces, split, mats, mats),
        out_specs=(cells, cells),
        check_vma=False,
    )
```

```python
import jax
import jax.numpy as jnp
from jax import lax
from jax.experimental import pallas as pl
from jax.experimental.pallas import tpu as pltpu
from jax.sharding import PartitionSpec as P

MESH = pl.DeviceIdType.MESH
F32 = jnp.float32
BF16 = jnp.bfloat16
FX, FY, FZ = 32, 96, 128
SX, SY = 16, 24
SEG = 96
GROUP = 16


def lane_iota(shape):
    return lax.broadcasted_iota(jnp.int32, shape, 1)


def zsum(v):
    lane = lane_iota(v.shape)
    return jnp.where(lane == 0, 0.0, pltpu.roll(v, 1, 1)) + jnp.where(
        lane == FZ - 1, 0.0, pltpu.roll(v, FZ - 1, 1)
    )


def split_terms(v):
    head = v.astype(BF16)
    return jnp.concatenate([head, (v - head.astype(F32)).astype(BF16)], axis=1)


def zsum_by_product(values, tt):
    return jnp.dot(
        jnp.concatenate([split_terms(v) for v in values], axis=0), tt, preferred_element_type=F32
    )


def ysum(v):
    zero = jnp.zeros((1, FZ), F32)
    return jnp.concatenate([zero, v[:-1]], axis=0) + jnp.concatenate([v[1:], zero], axis=0)


def rows_loop(lo, hi, unroll, body):
    count = hi - lo
    groups = count // unroll if count > unroll else 0
    if groups:

        def step(i, carry):
            for j in range(unroll):
                body(lo + i * unroll + j)
            return carry

        lax.fori_loop(0, groups, step, 0)
    for x in range(lo + groups * unroll, hi):
        body(x)


def at_row(x, pitch):
    return x * pitch if isinstance(x, int) else pl.multiple_of(x * pitch, 8)


def ysum_tile(ref, at, tile, tiles, cur):
    zero = jnp.zeros((1, FZ), F32)
    if 0 < tile < tiles - 1 and tile % 2 == 0:
        return ref[pl.ds(at - 1, 8), :] + ref[pl.ds(at + 1, 8), :]
    low = zero if tile == 0 else ref[pl.ds(at - 1, 1), :]
    high = zero if tile == tiles - 1 else ref[pl.ds(at + 8, 1), :]
    return jnp.concatenate([low, cur[:-1]], axis=0) + jnp.concatenate([cur[1:], high], axis=0)


def sweep_rows(groups, tiles, rolled, tt, coef_a, fixed):
    products = []
    for group in groups:
        halves = [group[: len(group) // 2], group[len(group) // 2 :]]
        for part in halves if len(group) > 1 and tiles > rolled else [group]:
            if tiles == rolled:
                products.extend([None] * len(part))
                continue
            height = 8 * (tiles - rolled)
            total = zsum_by_product(
                [ref[pl.ds(at + 8 * rolled, height), :] for _, (ref, at), _, _ in part], tt
            )
            products.extend(total[n * height : (n + 1) * height] for n in range(len(part)))
    for tile in range(tiles):
        n = 0
        for group in groups:
            cur = None
            for left, row, right, target in group:
                here = row[1] + 8 * tile
                before = cur if cur is not None else left[0][pl.ds(left[1] + 8 * tile, 8), :]
                cur = after if cur is not None else row[0][pl.ds(here, 8), :]
                after = right[0][pl.ds(right[1] + 8 * tile, 8), :]
                summed = (before + after) + ysum_tile(row[0], here, tile, tiles, cur)
                if tile < rolled:
                    summed = summed + zsum(cur)
                else:
                    summed = summed + products[n][8 * (tile - rolled) : 8 * (tile - rolled + 1)]
                target[0][pl.ds(target[1] + 8 * tile, 8), :] = (
                    fixed(n, tile) + coef_a(n, tile) * summed
                )
                n += 1


def to_f32(v):
    return v.astype(F32)


def rounded(v):
    return v.astype(BF16).astype(F32)


def kernel(
    n_grp, n_dom,
    fs, fr, fc, ss, sr, sc, sb, ts, tf,
    fo, so,
    p, q, a, b, bt, sp, sq, sa, sbb, sbt,
    mt, yy, xf0, xf1, xf2, xr, xa, xb, xs0, xs1, xsr, xsa, xsb,
    dx, vv, ww, pad, tpad, fin, sin, sins, fxx, fsx, xoff,
    fcv, scv, sbv, tt,
    ifs, is_, wb, bhl, bhr, shl, shr, mhl, mhr,
    rfl, rfr, fcl, fcr, sbl, sbr, rso, rsr, rsl, sco, scr, scl, scbr, scbl,
    wr, wl, bhrr, bhlr, shrr, shlr, mhrr, mhlr, sinr,
    load_sem, send_sem, recv_sem,
):
    g = lax.axis_index("grp")
    d = lax.axis_index("dom")
    gm, gp = lax.rem(g + n_grp - 1, n_grp), lax.rem(g + 1, n_grp)
    dm, dp = lax.rem(d + n_dom - 1, n_dom), lax.rem(d + 1, n_dom)
    ml = jnp.where(d > 0, 1.0, 0.0).astype(F32)
    mr = jnp.where(d < n_dom - 1, 1.0, 0.0).astype(F32)

    barrier = pltpu.get_barrier_semaphore()
    peers = ((g, dm), (g, dp), (gm, d), (gp, d), (gm, dm), (gm, dp), (gp, dm), (gp, dp))
    for peer in peers:
        pl.semaphore_signal(barrier, inc=1, device_id=peer, device_id_type=MESH)

    loads = {}

    def load(name, src, dst, index):
        loads[name] = pltpu.make_async_copy(src, dst, load_sem.at[index])
        loads[name].start()

    load("ss", ss, sp.at[pl.ds(8 * SY, SX * SY)], 0)
    load("sr", sr, sa.at[pl.ds(8 * SY, SX * SY)], 1)
    load("fs", fs, p.at[pl.ds(4 * FY, FX * FY)], 2)
    load("fr", fr, a.at[pl.ds(4 * FY, FX * FY)], 3)
    load("sc", sc, scv, 4)
    load("fc", fc, fcv, 5)
    load("sb", sb, sbv, 6)
    chunk = GROUP * FZ
    for t, src in ((0, ts), (1, tf)):
        for c in (0, 3, 1, 4, 2, 5):
            load(
                ("m", t, c), src.at[pl.ds(c * chunk, chunk)],
                mt.at[pl.ds((t * SEG * FZ) + c * chunk, chunk)], 7 + t * 6 + c,
            )

    sends = []
    apart = (lax.broadcasted_iota(jnp.int32, (2 * FZ, FZ), 0) & (FZ - 1)) - lane_iota((2 * FZ, FZ))
    tt[...] = jnp.where((apart == 1) | (apart == -1), 1.0, 0.0).astype(BF16)

    def send(src, dst, index, peer):
        copy = pltpu.make_async_remote_copy(
            src_ref=src, dst_ref=dst, send_sem=send_sem.at[index], recv_sem=recv_sem.at[index],
            device_id=peer, device_id_type=MESH,
        )
        copy.start()
        sends.append(copy)
        return copy

    loads["ss"].wait()
    loads["sr"].wait()
    for f, ref in ((0, sp), (1, sa)):
        for i in range(SX // 2):
            lo = (8 + 2 * i) * SY + 16
            is_[f, pl.ds(16 * i, 16), :] = jnp.concatenate(
                [ref[pl.ds(lo, 8), :], ref[pl.ds(lo + SY, 8), :]], axis=0
            ).astype(BF16)
        shl[f] = ref[pl.ds(8 * SY, 8 * SY), :].astype(BF16)
        shr[f] = ref[pl.ds(16 * SY, 8 * SY), :].astype(BF16)
    loads["fs"].wait()
    loads["fr"].wait()
    for f, ref in ((0, p), (1, a)):
        for i in range(FX // 2):
            lo = (4 + 2 * i) * FY
            pair = jnp.concatenate([ref[pl.ds(lo, 8), :], ref[pl.ds(lo + FY, 8), :]], axis=0)
            ifs[f, pl.ds(16 * i, 16), :] = pair.astype(BF16)
            own = xf0 if f == 0 else xr
            own[pl.ds((FX + 2 * i) * 8, 16), :] = pair
    loads["sc"].wait()
    loads["fc"].wait()
    loads["sb"].wait()
    pl.semaphore_wait(barrier, 8)

    recv = {}
    recv["rso"] = send(is_, rso, 6, (gm, d))
    recv["rsr"] = send(is_, rsr, 7, (gm, dm))
    recv["rsl"] = send(is_, rsl, 8, (gm, dp))
    recv["rfr"] = send(ifs.at[:, pl.ds(0, 192)], rfr, 0, (g, dm))
    recv["rfl"] = send(ifs.at[:, pl.ds(64, 192)], rfl, 1, (g, dp))
    recv["fcr"] = send(fcv, fcr, 2, (g, dm))
    recv["fcl"] = send(fcv, fcl, 3, (g, dp))
    recv["sbr"] = send(sbv, sbr, 4, (g, dm))
    recv["sbl"] = send(sbv, sbl, 5, (g, dp))
    recv["sco"] = send(scv, sco, 9, (gm, d))
    recv["scr"] = send(scv, scr, 10, (gm, dm))
    recv["scl"] = send(scv, scl, 11, (gm, dp))
    recv["scbr"] = send(scv, scbr, 12, (g, dm))
    recv["scbl"] = send(scv, scbl, 13, (g, dp))

    prow = lax.broadcasted_iota(jnp.int32, (8, 2 * FZ), 0)
    pcol = lane_iota((8, 2 * FZ))
    wanted = jnp.where(pcol < FZ, lax.rem(pcol, 3), lax.rem(pcol - FZ, 3) + 3)
    probe = jnp.where(wanted == prow, 1.0, 0.0).astype(BF16)
    phase = lax.rem(lane_iota((24, FZ)), 3)
    for t in range(2):
        for c in range(3):
            loads[("m", t, c)].wait()
            loads[("m", t, 3 + c)].wait()
            for v in range(8 * c, 8 * c + 8):
                at = (t * SEG + 2 * v) * FZ
                four = jnp.concatenate(
                    [mt[pl.ds(at, 2 * FZ), :], mt[pl.ds(at + 48 * FZ, 2 * FZ), :]], axis=1
                )
                found = jnp.dot(probe, four, preferred_element_type=F32)
                yy[pl.ds(t * 384 + v * 8, 8), :] = found[:, :FZ]
                yy[pl.ds(t * 384 + 192 + v * 8, 8), :] = found[:, FZ:]
        for h in range(2):
            for e in range(2):
                y3 = [
                    yy[pl.ds(t * 384 + h * 192 + 3 * e + c, 24, stride=8), :] for c in range(3)
                ]
                for k, shift in enumerate((0, 2, 1)):
                    picked = jnp.where(phase == 1, y3[(1 + shift) % 3], y3[shift])
                    picked = jnp.where(phase == 2, y3[(2 + shift) % 3], picked)
                    dx[3 * t + k, pl.ds(SEG + 48 * h + e, 24, stride=2), :] = picked
        for k in range(3):
            wb[3 * t + k] = dx[3 * t + k, pl.ds(SEG, SEG), :].astype(BF16)
    recv["wr"] = send(wb.at[:, pl.ds(0, 80)], wr, 14, (g, dm))
    recv["wl"] = send(wb.at[:, pl.ds(16, 80)], wl, 15, (g, dp))

    for i in range(4):
        bhl[pl.ds(i * FY, FY), :] = p[pl.ds((4 + i) * FY, FY), :].astype(BF16)
        bhr[pl.ds(i * FY, FY), :] = p[pl.ds((32 + i) * FY, FY), :].astype(BF16)
    for i in range(3):
        bhl[pl.ds((4 + i) * FY, FY), :] = a[pl.ds((4 + i) * FY, FY), :].astype(BF16)
        bhr[pl.ds((4 + i) * FY, FY), :] = a[pl.ds((33 + i) * FY, FY), :].astype(BF16)
    recv["bhrr"] = send(bhl, bhrr, 16, (g, dm))
    recv["bhlr"] = send(bhr, bhlr, 17, (g, dp))
    recv["shrr"] = send(shl, shrr, 18, (g, dm))
    recv["shlr"] = send(shr, shlr, 19, (g, dp))

    def coef(start_ref, rate_ref, a_ref, b_ref, lo, size):
        r = rate_ref[pl.ds(lo, size), :]
        inv = 1.0 / (1.0 + 6.0 * r)
        b_ref[pl.ds(lo, size), :] = start_ref[pl.ds(lo, size), :] * inv
        a_ref[pl.ds(lo, size), :] = r * inv

    def film_coef(r0, s0, film):
        inv0 = 1.0 / (1.0 + 6.0 * r0 + film)
        return r0 * inv0, s0 * inv0, film * inv0

    own_rows = pl.ds(4 * FY, FX, stride=FY)
    a0, b0, _ = film_coef(a[own_rows, :], p[own_rows, :], fcv[...])
    rows_loop(4, 36, 4, lambda x: coef(p, a, a, b, at_row(x, FY), FY))
    a[own_rows, :] = a0
    b[own_rows, :] = b0

    def fluid_sweep(src, dst, variant, spans):
        groups, bases, rows = [], [], []
        for x0, count in spans:
            group = []
            for n in range(count):
                base = x0 * FY + n * FY if isinstance(x0, int) else pl.multiple_of(x0 * FY, 8) + n * FY
                bases.append(base)
                rows.append(x0 + n)
                group.append(((src, base - FY), (src, base), (src, base + FY), (dst, base)))
            groups.append(group)

        def fixed(n, tile):
            if tile == 0 and variant is not None:
                return bt[pl.ds(variant * 320 + at_row(rows[n], 8), 8), :]
            return b[pl.ds(bases[n] + 8 * tile, 8), :]

        sweep_rows(
            groups, 12, 6, tt[...], lambda n, tile: a[pl.ds(bases[n] + 8 * tile, 8), :], fixed
        )

    def interior(variants):
        for m, block in enumerate((10, 7, 13, 8)):
            src, dst = (p, q) if m % 2 == 0 else (q, p)

            def step(i, carry):
                fluid_sweep(src, dst, variants[m], ((5 + m + i * block, block),))
                return carry

            lax.fori_loop(0, (30 - 2 * m) // block, step, 0)

    def edges(variants):
        for m in range(4):
            src, dst = (p, q) if m % 2 == 0 else (q, p)
            fluid_sweep(src, dst, variants[m], ((1 + m, 4), (35 - m, 4)))

    interior((None,) * 4)

    recv["rfl"].wait_recv()
    recv["rfr"].wait_recv()
    recv["fcl"].wait_recv()
    recv["fcr"].wait_recv()
    for f, ref in ((0, xf0), (1, xr)):
        ref[pl.ds(64, 192), :] = to_f32(rfl[f])
        ref[pl.ds(512, 192), :] = to_f32(rfr[f])
    fxx[pl.ds(0, FX), :] = fcl[...]
    fxx[pl.ds(FX, FX), :] = fcv[...]
    fxx[pl.ds(2 * FX, FX), :] = fcr[...]
    rows_loop(1, 11, 2, lambda x: coef(xf0, xr, xa, xb, at_row(x, 64), 64))
    xc = []
    xb0 = []
    for par in range(2):
        rows = pl.ds(64 + par * 8, 40, stride=16)
        film = fxx[pl.ds(8 + par, 40, stride=2), :]
        a0, b0, c0 = film_coef(xr[rows, :], xf0[rows, :], film)
        xa[rows, :] = a0
        fin[par] = b0
        fin[2 + par] = c0
        xc.append(2 + par)
        xb0.append(par)

    for name in ("rso", "rsr", "rsl", "sco", "scr", "scl"):
        recv[name].wait_recv()
    for f, ref in ((0, xs0), (1, xsr)):
        ref[pl.ds(0, 128), :] = to_f32(rsl[f])
        ref[pl.ds(128, 128), :] = to_f32(rso[f])
        ref[pl.ds(256, 128), :] = to_f32(rsr[f])
    rows_loop(0, 6, 2, lambda x: coef(xs0, xsr, xsa, xsb, at_row(x, 64), 64))
    srows = pl.ds(32 + 7, 40, stride=8)
    film = jnp.concatenate([scl[...], sco[...], scr[...]], axis=0)[4:44]
    a0, b0, c0 = film_coef(xsr[srows, :], xs0[srows, :], film)
    xsa[srows, :] = a0
    sin[0] = b0
    sin[1] = c0

    for name in ("sbl", "sbr", "wl", "wr"):
        recv[name].wait_recv()
    for k in range(6):
        dx[k, pl.ds(16, 80), :] = to_f32(wl[k])
        dx[k, pl.ds(192, 80), :] = to_f32(wr[k])
    for n, ref in enumerate((sbl, sbv, sbr)):
        spread = jnp.broadcast_to(ref[...].astype(F32), (FZ, FZ)).T
        xoff[pl.ds(n * SEG, SEG), :] = spread[:SEG].astype(jnp.int32)
    first = SX * (d + n_dom - 1) - 2
    zone = SX * n_dom
    half = lax.broadcasted_iota(jnp.int32, (40, FZ), 0) + (first + 4)
    for par in range(2):
        offs = [
            lax.rem(xoff[pl.ds(24 + 3 * par + j, 40, stride=6), :] - half + 3 * zone, zone)
            for j in range(3)
        ]
        for t in range(2):
            for k in range(3):
                diag = [dx[3 * t + k, pl.ds(24 + 3 * par + j, 40, stride=6), :] for j in range(3)]
                for o in range(5):
                    total = jnp.where(offs[0] == o, diag[0], 0.0)
                    total = total + jnp.where(offs[1] == o, diag[1], 0.0)
                    total = total + jnp.where(offs[2] == o, diag[2], 0.0)
                    at = (o * 3 + k) * 2 + par
                    if t == 0:
                        ww[at] = total
                    else:
                        vv[at] = total * fin[xc[par]]

    def shifts(v):
        return (v, pltpu.roll(v, 1, 1), pltpu.roll(v, FZ - 1, 1))

    def project_fluid(solid_ref, k):
        for n, v in enumerate(shifts(rounded(solid_ref[srows, :]))):
            pad[n, pl.ds(8, 40), :] = v
        for par in range(2):
            total = jnp.zeros((40, FZ), F32)
            for o in range(5):
                for n in range(3):
                    total = total + vv[(o * 3 + n) * 2 + par] * pad[n, pl.ds(6 + o, 40), :]
            fin[4 + 2 * k + par] = total

    def project_solid(fluid_ref, k):
        faces = [
            shifts(rounded(fluid_ref[pl.ds(64 + par * 8, 40, stride=16), :])) for par in range(2)
        ]
        for o in range(5):
            total = jnp.zeros((40, FZ), F32)
            for par in range(2):
                for n in range(3):
                    total = total + ww[(o * 3 + n) * 2 + par] * faces[par][n]
            tpad[o, pl.ds(8, 40), :] = total
        total = tpad[0, pl.ds(10, 40), :]
        for o in range(1, 5):
            total = total + tpad[o, pl.ds(10 - o, 40), :]
        sin[2 + k] = total
        sins[k] = total[4:36]

    def face_sweep(src, dst, a_ref, b_ref, width, lo, hi):
        count = hi - lo
        by_rolls = count - 2 * (count // 4)

        def beside(step, first):
            pieces, x = [], lo + step
            for cut, keep in ((width, keep_first), (2 * width, keep_last)):
                row = cut - 1 if first else cut
                if x < row:
                    pieces.append(src[pl.ds(x * 8, (row - x) * 8), :])
                pieces.append(src[pl.ds(row * 8, 8), :] * keep)
                x = row + 1
            if x < hi + step:
                pieces.append(src[pl.ds(x * 8, (hi + step - x) * 8), :])
            return jnp.concatenate(pieces, axis=0)

        cur = src[pl.ds(lo * 8, count * 8), :]
        sub = lax.broadcasted_iota(jnp.int32, (count * 8, FZ), 0) & 7
        above = jnp.where(sub == 0, 0.0, src[pl.ds(lo * 8 - 1, count * 8), :])
        below = jnp.where(sub == 7, 0.0, src[pl.ds(lo * 8 + 1, count * 8), :])
        along = jnp.concatenate(
            [zsum(cur[: by_rolls * 8]), zsum_by_product([cur[by_rolls * 8 :]], tt[...])], axis=0
        )
        summed = (beside(-1, True) + beside(1, False)) + (above + below) + along
        span = pl.ds(lo * 8, count * 8)
        dst[span, :] = b_ref[span, :] + a_ref[span, :] * summed

    keep_first, keep_last = ml, mr
    fluid_span = (((13, 83), (14, 82)), ((19, 77), (20, 76)), ((25, 71), (26, 70)))
    solid_span = (((6, 42), (7, 41)), ((9, 39), (10, 38)), ((12, 36), (13, 35)))
    fluid_refs = (xf0, xf0, xf2)
    fluid_out = (xf0, xf2, xf0)
    for k in range(4):
        fluid_ref = (xf0, xf0, xf2, xf0)[k]
        project_fluid(xs0, k)
        project_solid(fluid_ref, k)
        if k == 3:
            break
        for par in range(2):
            xb[pl.ds(64 + par * 8, 40, stride=16), :] = fin[xb0[par]] + fin[4 + 2 * k + par]
        xsb[srows, :] = sin[0] + sin[1] * sin[2 + k]
        for n in range(2):
            lo, hi = fluid_span[k][n]
            src, dst = (fluid_refs[k], xf1) if n == 0 else (xf1, fluid_out[k])
            face_sweep(src, dst, xa, xb, FX, lo, hi)
            lo, hi = solid_span[k][n]
            src, dst = (xs0, xs1) if n == 0 else (xs1, xs0)
            face_sweep(src, dst, xsa, xsb, SX, lo, hi)
    recv["sinr"] = send(sins, sinr, 22, (gp, d))

    recv["bhlr"].wait_recv()
    recv["bhrr"].wait_recv()
    for ref, first_row, mask, film_at in ((bhlr, 0, ml, 28), (bhrr, 36, mr, 64)):
        for i in range(4):
            p[pl.ds((first_row + i) * FY, FY), :] = to_f32(ref[pl.ds(i * FY, FY), :]) * mask
        skip = 1 if first_row == 0 else 0
        for i in range(3):
            row = first_row + skip + i
            a[pl.ds(row * FY, FY), :] = to_f32(ref[pl.ds((4 + i) * FY, FY), :]) * mask
        for i in range(3):
            row = first_row + skip + i
            film = fxx[pl.ds(film_at + skip + i, 1), :]
            r0, s0 = a[pl.ds(row * FY, 1), :], p[pl.ds(row * FY, 1), :]
            a0, b0, _ = film_coef(r0, s0, film)
            coef(p, a, a, b, row * FY, FY)
            a[pl.ds(row * FY, 1), :] = a0
            b[pl.ds(row * FY, 1), :] = b0
    edges((None,) * 4)
    mhl[...] = p[pl.ds(4 * FY, 4 * FY), :].astype(BF16)
    mhr[...] = p[pl.ds(32 * FY, 4 * FY), :].astype(BF16)
    recv["mhrr"] = send(mhl, mhrr, 20, (g, dm))
    recv["mhlr"] = send(mhr, mhlr, 21, (g, dp))

    wide = lax.broadcasted_iota(jnp.int32, (20, FZ), 0)
    inside = jnp.where(wide < 2, ml, jnp.where(wide >= 18, mr, 1.0))
    for v in range(2):
        for i in range(1, 39):
            bt[pl.ds(v * 320 + i * 8, 8), :] = b[pl.ds(i * FY, 8), :]
        for par in range(2):
            rows = pl.ds(v * 320 + par * 8, 20, stride=16)
            bt[rows, :] = bt[rows, :] + fin[4 + 2 * (2 + v) + par][10:30] * inside

    def patch(i, mask):
        low = lax.broadcasted_iota(jnp.int32, (8, FZ), 0) < 4
        fresh = xf2[pl.ds((28 + i) * 8, 8), :]
        if mask is not None:
            fresh = fresh * mask
        p[pl.ds(i * FY, 8), :] = jnp.where(low, fresh, p[pl.ds(i * FY, 8), :])

    for i in range(4, 36):
        patch(i, None)
    second = (0, 0, 1, 1)
    interior(second)
    out_mid = pltpu.make_async_copy(
        p.at[pl.ds(8 * FY, 24 * FY)], fo.at[pl.ds(4 * FY, 24 * FY)], load_sem.at[19]
    )
    out_mid.start()

    for name in ("scbl", "scbr", "shlr", "shrr", "sinr"):
        recv[name].wait_recv()
    for f, ref in ((0, sp), (1, sa)):
        ref[pl.ds(0, 8 * SY), :] = to_f32(shlr[f]) * ml
        ref[pl.ds(24 * SY, 8 * SY), :] = to_f32(shrr[f]) * mr
    fsx[pl.ds(0, 8), :] = scbl[pl.ds(8, 8), :] * ml
    fsx[pl.ds(8, SX), :] = scv[...]
    fsx[pl.ds(24, 8), :] = scbr[pl.ds(0, 8), :] * mr
    last_rows = pl.ds(SY - 1, 32, stride=SY)
    a0, b0, c0 = film_coef(sa[last_rows, :], sp[last_rows, :], fsx[...])
    rows_loop(0, 8, 2, lambda x: coef(sp, sa, sa, sbb, at_row(x, 96), 96))
    sa[last_rows, :] = a0
    sbb[last_rows, :] = b0
    for k in range(4):
        for i in range(32):
            sbt[pl.ds(k * 256 + i * 8, 8), :] = sbb[pl.ds(i * SY + 16, 8), :]
        sbt[pl.ds(k * 256 + 7, 32, stride=8), :] = b0 + c0 * sinr[k]

    for m in range(8):
        src, dst = (sp, sq) if m % 2 == 0 else (sq, sp)
        rows = range(1 + m, 31 - m)

        def fixed(n, tile):
            if tile == 2:
                return sbt[pl.ds((m // 2) * 256 + rows[n] * 8, 8), :]
            return sbb[pl.ds(rows[n] * SY + 8 * tile, 8), :]

        sweep_rows(
            [[((src, (x - 1) * SY), (src, x * SY), (src, (x + 1) * SY), (dst, x * SY)) for x in rows]],
            3, 1, tt[...], lambda n, tile: sa[pl.ds(rows[n] * SY + 8 * tile, 8), :], fixed,
        )
    out_solid = pltpu.make_async_copy(sp.at[pl.ds(8 * SY, SX * SY)], so, load_sem.at[20])
    out_solid.start()

    recv["mhlr"].wait_recv()
    recv["mhrr"].wait_recv()
    p[pl.ds(0, 4 * FY), :] = to_f32(mhlr[...]) * ml
    p[pl.ds(36 * FY, 4 * FY), :] = to_f32(mhrr[...]) * mr
    for i in range(4):
        patch(i, ml)
        patch(36 + i, mr)
    edges(second)
    outs = []
    for n, i in enumerate((4, 32)):
        copy = pltpu.make_async_copy(
            p.at[pl.ds(i * FY, 4 * FY)], fo.at[pl.ds((i - 4) * FY, 4 * FY)], load_sem.at[21 + n]
        )
        copy.start()
        outs.append(copy)
    for copy in sends:
        copy.wait_send()
    for copy in (out_mid, out_solid, *outs):
        copy.wait()


def vm(*shape, dtype=F32):
    return pltpu.VMEM(shape, dtype)


SCRATCH = [
    *(vm(40 * FY, FZ) for _ in range(4)), vm(2 * 320, FZ),
    *(vm(32 * SY, FZ) for _ in range(4)), vm(4 * 256, FZ),
    vm(2 * SEG * FZ, FZ, dtype=BF16), vm(2 * SEG * 8, FZ),
    *(vm(96 * 8, FZ) for _ in range(6)), *(vm(48 * 8, FZ) for _ in range(5)),
    vm(6, 3 * SEG, FZ), vm(30, 40, FZ), vm(30, 40, FZ), vm(3, 64, FZ), vm(5, 64, FZ),
    vm(12, 40, FZ), vm(6, 40, FZ), vm(4, 32, FZ), vm(96, FZ), vm(32, FZ),
    vm(3 * SEG, FZ, dtype=jnp.int32),
    vm(FX, FZ), vm(SX, FZ), vm(1, FZ, dtype=jnp.int32), vm(2 * FZ, FZ, dtype=BF16),
    vm(2, 256, FZ, dtype=BF16), vm(2, 128, FZ, dtype=BF16), vm(6, SEG, FZ, dtype=BF16),
    vm(7 * FY, FZ, dtype=BF16), vm(7 * FY, FZ, dtype=BF16),
    vm(2, 8 * SY, FZ, dtype=BF16), vm(2, 8 * SY, FZ, dtype=BF16),
    vm(4 * FY, FZ, dtype=BF16), vm(4 * FY, FZ, dtype=BF16),
    vm(2, 192, FZ, dtype=BF16), vm(2, 192, FZ, dtype=BF16), vm(FX, FZ), vm(FX, FZ),
    vm(1, FZ, dtype=jnp.int32), vm(1, FZ, dtype=jnp.int32),
    *(vm(2, 128, FZ, dtype=BF16) for _ in range(3)), *(vm(SX, FZ) for _ in range(5)),
    vm(6, 80, FZ, dtype=BF16), vm(6, 80, FZ, dtype=BF16),
    vm(7 * FY, FZ, dtype=BF16), vm(7 * FY, FZ, dtype=BF16),
    vm(2, 8 * SY, FZ, dtype=BF16), vm(2, 8 * SY, FZ, dtype=BF16),
    vm(4 * FY, FZ, dtype=BF16), vm(4 * FY, FZ, dtype=BF16), vm(4, 32, FZ),
    pltpu.SemaphoreType.DMA((24,)), pltpu.SemaphoreType.DMA((23,)), pltpu.SemaphoreType.DMA((23,)),
]


def solution(mesh):
    n_grp, n_dom = mesh.shape["grp"], mesh.shape["dom"]

    def local(fs, fr, fc, ss, sr, sc, sb, ts, tf):
        fo, so = pl.pallas_call(
            lambda *refs: kernel(n_grp, n_dom, *refs),
            out_shape=(
                jax.ShapeDtypeStruct((FX * FY, FZ), F32),
                jax.ShapeDtypeStruct((SX * SY, FZ), F32),
            ),
            in_specs=[pl.BlockSpec(memory_space=pl.ANY)] * 9,
            out_specs=[pl.BlockSpec(memory_space=pl.ANY)] * 2,
            scratch_shapes=SCRATCH,
            compiler_params=pltpu.CompilerParams(
                collective_id=0, has_side_effects=True, vmem_limit_bytes=56 * 1024 * 1024
            ),
            name="coupled",
        )(
            fs.reshape(FX * FY, FZ), fr.reshape(FX * FY, FZ), fc.reshape(FX, FZ),
            ss.reshape(SX * SY, FZ), sr.reshape(SX * SY, FZ), sc.reshape(SX, FZ),
            jnp.pad(sb, (0, FZ - SEG)).reshape(1, FZ),
            ts.reshape(SEG * FZ, FZ), tf.reshape(SEG * FZ, FZ),
        )
        return fo.reshape(1, FX, FY, FZ), so.reshape(1, SX, SY, FZ)

    cells = P("grp", "dom", None, None)
    faces = P("grp", "dom", None)
    split = P(("grp", "dom"))
    mats = P(("grp", "dom"), None, None)
    return jax.shard_map(
        local,
        mesh=mesh,
        in_specs=(cells, cells, faces, cells, cells, faces, split, mats, mats),
        out_specs=(cells, cells),
        check_vma=False,
    )
```

```python
import jax
import jax.numpy as jnp
from jax import lax
from jax.experimental import pallas as pl
from jax.experimental.pallas import tpu as pltpu
from jax.sharding import PartitionSpec as P

MESH = pl.DeviceIdType.MESH
F32 = jnp.float32
BF16 = jnp.bfloat16
FX, FY, FZ = 32, 96, 128
SX, SY = 16, 24
SEG = 96
GROUP = 16


def lane_iota(shape):
    return lax.broadcasted_iota(jnp.int32, shape, 1)


def zsum(v):
    lane = lane_iota(v.shape)
    return jnp.where(lane == 0, 0.0, pltpu.roll(v, 1, 1)) + jnp.where(
        lane == FZ - 1, 0.0, pltpu.roll(v, FZ - 1, 1)
    )


def split_terms(v):
    head = v.astype(BF16)
    return jnp.concatenate([head, (v - head.astype(F32)).astype(BF16)], axis=1)


def band(tt):
    apart = (lax.broadcasted_iota(jnp.int32, (2 * FZ, FZ), 0) & (FZ - 1)) - lane_iota((2 * FZ, FZ))
    tt[...] = jnp.where((apart == 1) | (apart == -1), 1.0, 0.0).astype(BF16)


def zsum_by_product(values, tt):
    return jnp.dot(
        jnp.concatenate([split_terms(v) for v in values], axis=0), tt, preferred_element_type=F32
    )


def ysum(v):
    zero = jnp.zeros((1, FZ), F32)
    return jnp.concatenate([zero, v[:-1]], axis=0) + jnp.concatenate([v[1:], zero], axis=0)


def rows_loop(lo, hi, unroll, body):
    count = hi - lo
    groups = count // unroll if count > unroll else 0
    if groups:

        def step(i, carry):
            for j in range(unroll):
                body(lo + i * unroll + j)
            return carry

        lax.fori_loop(0, groups, step, 0)
    for x in range(lo + groups * unroll, hi):
        body(x)


def at_row(x, pitch):
    return x * pitch if isinstance(x, int) else pl.multiple_of(x * pitch, 8)


def ysum_tile(ref, at, tile, tiles, cur):
    zero = jnp.zeros((1, FZ), F32)
    if 0 < tile < tiles - 1 and tile % 2 == 0:
        return ref[pl.ds(at - 1, 8), :] + ref[pl.ds(at + 1, 8), :]
    low = zero if tile == 0 else ref[pl.ds(at - 1, 1), :]
    high = zero if tile == tiles - 1 else ref[pl.ds(at + 8, 1), :]
    return jnp.concatenate([low, cur[:-1]], axis=0) + jnp.concatenate([cur[1:], high], axis=0)


def sweep_rows(groups, tiles, rolled, tt, coef_a, fixed):
    products = []
    for group in groups:
        halves = [group[: len(group) // 2], group[len(group) // 2 :]]
        for part in halves if len(group) > 1 and tiles > rolled else [group]:
            if tiles == rolled:
                products.extend([None] * len(part))
                continue
            height = 8 * (tiles - rolled)
            total = zsum_by_product(
                [ref[pl.ds(at + 8 * rolled, height), :] for _, (ref, at), _, _ in part], tt
            )
            products.extend(total[n * height : (n + 1) * height] for n in range(len(part)))
    for tile in range(tiles):
        n = 0
        for group in groups:
            cur = None
            for left, row, right, target in group:
                here = row[1] + 8 * tile
                before = cur if cur is not None else left[0][pl.ds(left[1] + 8 * tile, 8), :]
                cur = after if cur is not None else row[0][pl.ds(here, 8), :]
                after = right[0][pl.ds(right[1] + 8 * tile, 8), :]
                summed = (before + after) + ysum_tile(row[0], here, tile, tiles, cur)
                if tile < rolled:
                    summed = summed + zsum(cur)
                else:
                    summed = summed + products[n][8 * (tile - rolled) : 8 * (tile - rolled + 1)]
                target[0][pl.ds(target[1] + 8 * tile, 8), :] = (
                    fixed(n, tile) + coef_a(n, tile) * summed
                )
                n += 1


def to_f32(v):
    return v.astype(F32)


def rounded(v):
    return v.astype(BF16).astype(F32)


def kernel(
    n_grp, n_dom,
    fs, fr, fc, ss, sr, sc, sb, ts, tf,
    p, q, a, b, bt, sp,
    sq, sa, sbb, sbt,
    mt, yy, xf0, xf1, xf2, xr, xa, xb, xs0, xs1, xsr, xsa, xsb,
    dx, vv, ww, pad, tpad, fin, sin, sins, fxx, fsx, xoff,
    fcv, scv, sbv, tt,
    ifs, is_, wb, bhl, bhr, shl, shr, mhl, mhr,
    rfl, rfr, fcl, fcr, sbl, sbr, rso, rsr, rsl, sco, scr, scl, scbr, scbl,
    wr, wl, bhrr, bhlr, shrr, shlr, mhrr, mhlr, sinr,
    load_sem, send_sem, recv_sem,
):
    g = lax.axis_index("grp")
    d = lax.axis_index("dom")
    gm, gp = lax.rem(g + n_grp - 1, n_grp), lax.rem(g + 1, n_grp)
    dm, dp = lax.rem(d + n_dom - 1, n_dom), lax.rem(d + 1, n_dom)
    ml = jnp.where(d > 0, 1.0, 0.0).astype(F32)
    mr = jnp.where(d < n_dom - 1, 1.0, 0.0).astype(F32)

    barrier = pltpu.get_barrier_semaphore()
    peers = ((g, dm), (g, dp), (gm, d), (gp, d), (gm, dm), (gm, dp), (gp, dm), (gp, dp))
    for peer in peers:
        pl.semaphore_signal(barrier, inc=1, device_id=peer, device_id_type=MESH)

    loads = {}

    def load(name, src, dst, index):
        loads[name] = pltpu.make_async_copy(src, dst, load_sem.at[index])
        loads[name].start()

    load("ss", ss, sp.at[pl.ds(8 * SY, SX * SY)], 0)
    load("sr", sr, sa.at[pl.ds(8 * SY, SX * SY)], 1)
    load("fs", fs, p.at[pl.ds(4 * FY, FX * FY)], 2)
    load("fr", fr, a.at[pl.ds(4 * FY, FX * FY)], 3)
    load("sc", sc, scv, 4)
    load("fc", fc, fcv, 5)
    load("sb", sb, sbv, 6)
    chunk = GROUP * FZ
    for t, src in ((0, ts), (1, tf)):
        for c in (0, 3, 1, 4, 2, 5):
            load(
                ("m", t, c), src.at[pl.ds(c * chunk, chunk)],
                mt.at[pl.ds((t * SEG * FZ) + c * chunk, chunk)], 7 + t * 6 + c,
            )

    sends = []
    band(tt)

    def send(src, dst, index, peer):
        copy = pltpu.make_async_remote_copy(
            src_ref=src, dst_ref=dst, send_sem=send_sem.at[index], recv_sem=recv_sem.at[index],
            device_id=peer, device_id_type=MESH,
        )
        copy.start()
        sends.append(copy)
        return copy

    loads["ss"].wait()
    loads["sr"].wait()
    for f, ref in ((0, sp), (1, sa)):
        for i in range(SX // 2):
            lo = (8 + 2 * i) * SY + 16
            is_[f, pl.ds(16 * i, 16), :] = jnp.concatenate(
                [ref[pl.ds(lo, 8), :], ref[pl.ds(lo + SY, 8), :]], axis=0
            ).astype(BF16)
        shl[f] = ref[pl.ds(8 * SY, 8 * SY), :].astype(BF16)
        shr[f] = ref[pl.ds(16 * SY, 8 * SY), :].astype(BF16)
    loads["fs"].wait()
    loads["fr"].wait()
    for f, ref in ((0, p), (1, a)):
        for i in range(FX // 2):
            lo = (4 + 2 * i) * FY
            pair = jnp.concatenate([ref[pl.ds(lo, 8), :], ref[pl.ds(lo + FY, 8), :]], axis=0)
            ifs[f, pl.ds(16 * i, 16), :] = pair.astype(BF16)
            own = xf0 if f == 0 else xr
            own[pl.ds((FX + 2 * i) * 8, 16), :] = pair
    loads["sc"].wait()
    loads["fc"].wait()
    loads["sb"].wait()
    pl.semaphore_wait(barrier, 8)

    recv = {}
    recv["rso"] = send(is_, rso, 6, (gm, d))
    recv["rsr"] = send(is_, rsr, 7, (gm, dm))
    recv["rsl"] = send(is_, rsl, 8, (gm, dp))
    recv["rfr"] = send(ifs.at[:, pl.ds(0, 192)], rfr, 0, (g, dm))
    recv["rfl"] = send(ifs.at[:, pl.ds(64, 192)], rfl, 1, (g, dp))
    recv["fcr"] = send(fcv, fcr, 2, (g, dm))
    recv["fcl"] = send(fcv, fcl, 3, (g, dp))
    recv["sbr"] = send(sbv, sbr, 4, (g, dm))
    recv["sbl"] = send(sbv, sbl, 5, (g, dp))
    recv["sco"] = send(scv, sco, 9, (gm, d))
    recv["scr"] = send(scv, scr, 10, (gm, dm))
    recv["scl"] = send(scv, scl, 11, (gm, dp))
    recv["scbr"] = send(scv, scbr, 12, (g, dm))
    recv["scbl"] = send(scv, scbl, 13, (g, dp))

    prow = lax.broadcasted_iota(jnp.int32, (8, 2 * FZ), 0)
    pcol = lane_iota((8, 2 * FZ))
    wanted = jnp.where(pcol < FZ, lax.rem(pcol, 3), lax.rem(pcol - FZ, 3) + 3)
    probe = jnp.where(wanted == prow, 1.0, 0.0).astype(BF16)
    phase = lax.rem(lane_iota((24, FZ)), 3)
    for t in range(2):
        for c in range(3):
            loads[("m", t, c)].wait()
            loads[("m", t, 3 + c)].wait()
            for v in range(8 * c, 8 * c + 8):
                at = (t * SEG + 2 * v) * FZ
                four = jnp.concatenate(
                    [mt[pl.ds(at, 2 * FZ), :], mt[pl.ds(at + 48 * FZ, 2 * FZ), :]], axis=1
                )
                found = jnp.dot(probe, four, preferred_element_type=F32)
                yy[pl.ds(t * 384 + v * 8, 8), :] = found[:, :FZ]
                yy[pl.ds(t * 384 + 192 + v * 8, 8), :] = found[:, FZ:]
        for h in range(2):
            for e in range(2):
                y3 = [
                    yy[pl.ds(t * 384 + h * 192 + 3 * e + c, 24, stride=8), :] for c in range(3)
                ]
                for k, shift in enumerate((0, 2, 1)):
                    picked = jnp.where(phase == 1, y3[(1 + shift) % 3], y3[shift])
                    picked = jnp.where(phase == 2, y3[(2 + shift) % 3], picked)
                    dx[3 * t + k, pl.ds(SEG + 48 * h + e, 24, stride=2), :] = picked
        for k in range(3):
            wb[3 * t + k] = dx[3 * t + k, pl.ds(SEG, SEG), :].astype(BF16)
    recv["wr"] = send(wb.at[:, pl.ds(0, 80)], wr, 14, (g, dm))
    recv["wl"] = send(wb.at[:, pl.ds(16, 80)], wl, 15, (g, dp))

    for i in range(4):
        bhl[pl.ds(i * FY, FY), :] = p[pl.ds((4 + i) * FY, FY), :].astype(BF16)
        bhr[pl.ds(i * FY, FY), :] = p[pl.ds((32 + i) * FY, FY), :].astype(BF16)
    for i in range(3):
        bhl[pl.ds((4 + i) * FY, FY), :] = a[pl.ds((4 + i) * FY, FY), :].astype(BF16)
        bhr[pl.ds((4 + i) * FY, FY), :] = a[pl.ds((33 + i) * FY, FY), :].astype(BF16)
    recv["bhrr"] = send(bhl, bhrr, 16, (g, dm))
    recv["bhlr"] = send(bhr, bhlr, 17, (g, dp))
    recv["shrr"] = send(shl, shrr, 18, (g, dm))
    recv["shlr"] = send(shr, shlr, 19, (g, dp))

    def coef(start_ref, rate_ref, a_ref, b_ref, lo, size):
        r = rate_ref[pl.ds(lo, size), :]
        inv = 1.0 / (1.0 + 6.0 * r)
        b_ref[pl.ds(lo, size), :] = start_ref[pl.ds(lo, size), :] * inv
        a_ref[pl.ds(lo, size), :] = r * inv

    def film_coef(r0, s0, film):
        inv0 = 1.0 / (1.0 + 6.0 * r0 + film)
        return r0 * inv0, s0 * inv0, film * inv0

    own_rows = pl.ds(4 * FY, FX, stride=FY)
    a0, b0, _ = film_coef(a[own_rows, :], p[own_rows, :], fcv[...])
    rows_loop(4, 36, 4, lambda x: coef(p, a, a, b, at_row(x, FY), FY))
    a[own_rows, :] = a0
    b[own_rows, :] = b0

    def fluid_sweep(src, dst, variant, spans):
        groups, bases, rows = [], [], []
        for x0, count in spans:
            group = []
            for n in range(count):
                base = x0 * FY + n * FY if isinstance(x0, int) else pl.multiple_of(x0 * FY, 8) + n * FY
                bases.append(base)
                rows.append(x0 + n)
                group.append(((src, base - FY), (src, base), (src, base + FY), (dst, base)))
            groups.append(group)

        def fixed(n, tile):
            if tile == 0 and variant is not None:
                return bt[pl.ds(variant * 320 + at_row(rows[n], 8), 8), :]
            return b[pl.ds(bases[n] + 8 * tile, 8), :]

        sweep_rows(
            groups, 12, 6, tt[...], lambda n, tile: a[pl.ds(bases[n] + 8 * tile, 8), :], fixed
        )

    def interior(variants):
        for m, block in enumerate((10, 7, 13, 8)):
            src, dst = (p, q) if m % 2 == 0 else (q, p)

            def step(i, carry):
                fluid_sweep(src, dst, variants[m], ((5 + m + i * block, block),))
                return carry

            lax.fori_loop(0, (30 - 2 * m) // block, step, 0)

    def edges(variants):
        for m in range(4):
            src, dst = (p, q) if m % 2 == 0 else (q, p)
            fluid_sweep(src, dst, variants[m], ((1 + m, 4), (35 - m, 4)))

    interior((None,) * 4)

    recv["rfl"].wait_recv()
    recv["rfr"].wait_recv()
    recv["fcl"].wait_recv()
    recv["fcr"].wait_recv()
    for f, ref in ((0, xf0), (1, xr)):
        ref[pl.ds(64, 192), :] = to_f32(rfl[f])
        ref[pl.ds(512, 192), :] = to_f32(rfr[f])
    fxx[pl.ds(0, FX), :] = fcl[...]
    fxx[pl.ds(FX, FX), :] = fcv[...]
    fxx[pl.ds(2 * FX, FX), :] = fcr[...]
    rows_loop(1, 11, 2, lambda x: coef(xf0, xr, xa, xb, at_row(x, 64), 64))
    xc = []
    xb0 = []
    for par in range(2):
        rows = pl.ds(64 + par * 8, 40, stride=16)
        film = fxx[pl.ds(8 + par, 40, stride=2), :]
        a0, b0, c0 = film_coef(xr[rows, :], xf0[rows, :], film)
        xa[rows, :] = a0
        fin[par] = b0
        fin[2 + par] = c0
        xc.append(2 + par)
        xb0.append(par)

    for name in ("rso", "rsr", "rsl", "sco", "scr", "scl"):
        recv[name].wait_recv()
    for f, ref in ((0, xs0), (1, xsr)):
        ref[pl.ds(0, 128), :] = to_f32(rsl[f])
        ref[pl.ds(128, 128), :] = to_f32(rso[f])
        ref[pl.ds(256, 128), :] = to_f32(rsr[f])
    rows_loop(0, 6, 2, lambda x: coef(xs0, xsr, xsa, xsb, at_row(x, 64), 64))
    srows = pl.ds(32 + 7, 40, stride=8)
    film = jnp.concatenate([scl[...], sco[...], scr[...]], axis=0)[4:44]
    a0, b0, c0 = film_coef(xsr[srows, :], xs0[srows, :], film)
    xsa[srows, :] = a0
    sin[0] = b0
    sin[1] = c0

    for name in ("sbl", "sbr", "wl", "wr"):
        recv[name].wait_recv()
    for k in range(6):
        dx[k, pl.ds(16, 80), :] = to_f32(wl[k])
        dx[k, pl.ds(192, 80), :] = to_f32(wr[k])
    for n, ref in enumerate((sbl, sbv, sbr)):
        row = jnp.concatenate([ref[...].astype(F32), jnp.zeros((1, FZ - SEG), F32)], axis=1)
        spread = jnp.broadcast_to(row, (FZ, FZ)).T
        xoff[pl.ds(n * SEG, SEG), :] = spread[:SEG].astype(jnp.int32)
    first = SX * (d + n_dom - 1) - 2
    zone = SX * n_dom
    half = lax.broadcasted_iota(jnp.int32, (40, FZ), 0) + (first + 4)
    for par in range(2):
        offs = [
            lax.rem(xoff[pl.ds(24 + 3 * par + j, 40, stride=6), :] - half + 3 * zone, zone)
            for j in range(3)
        ]
        for t in range(2):
            for k in range(3):
                diag = [dx[3 * t + k, pl.ds(24 + 3 * par + j, 40, stride=6), :] for j in range(3)]
                for o in range(5):
                    total = jnp.where(offs[0] == o, diag[0], 0.0)
                    total = total + jnp.where(offs[1] == o, diag[1], 0.0)
                    total = total + jnp.where(offs[2] == o, diag[2], 0.0)
                    at = (o * 3 + k) * 2 + par
                    if t == 0:
                        ww[at] = total
                    else:
                        vv[at] = total * fin[xc[par]]

    def shifts(v):
        return (v, pltpu.roll(v, 1, 1), pltpu.roll(v, FZ - 1, 1))

    def project_fluid(solid_ref, k):
        for n, v in enumerate(shifts(rounded(solid_ref[srows, :]))):
            pad[n, pl.ds(8, 40), :] = v
        for par in range(2):
            total = jnp.zeros((40, FZ), F32)
            for o in range(5):
                for n in range(3):
                    total = total + vv[(o * 3 + n) * 2 + par] * pad[n, pl.ds(6 + o, 40), :]
            fin[4 + 2 * k + par] = total

    def project_solid(fluid_ref, k):
        faces = [
            shifts(rounded(fluid_ref[pl.ds(64 + par * 8, 40, stride=16), :])) for par in range(2)
        ]
        for o in range(5):
            total = jnp.zeros((40, FZ), F32)
            for par in range(2):
                for n in range(3):
                    total = total + ww[(o * 3 + n) * 2 + par] * faces[par][n]
            tpad[o, pl.ds(8, 40), :] = total
        total = tpad[0, pl.ds(10, 40), :]
        for o in range(1, 5):
            total = total + tpad[o, pl.ds(10 - o, 40), :]
        sin[2 + k] = total
        sins[k] = total[4:36]

    def face_sweep(src, dst, a_ref, b_ref, width, lo, hi):
        count = hi - lo
        by_rolls = count - 2 * (count // 4)

        def beside(step, first):
            pieces, x = [], lo + step
            for cut, keep in ((width, keep_first), (2 * width, keep_last)):
                row = cut - 1 if first else cut
                if x < row:
                    pieces.append(src[pl.ds(x * 8, (row - x) * 8), :])
                pieces.append(src[pl.ds(row * 8, 8), :] * keep)
                x = row + 1
            if x < hi + step:
                pieces.append(src[pl.ds(x * 8, (hi + step - x) * 8), :])
            return jnp.concatenate(pieces, axis=0)

        cur = src[pl.ds(lo * 8, count * 8), :]
        sub = lax.broadcasted_iota(jnp.int32, (count * 8, FZ), 0) & 7
        above = jnp.where(sub == 0, 0.0, src[pl.ds(lo * 8 - 1, count * 8), :])
        below = jnp.where(sub == 7, 0.0, src[pl.ds(lo * 8 + 1, count * 8), :])
        along = jnp.concatenate(
            [zsum(cur[: by_rolls * 8]), zsum_by_product([cur[by_rolls * 8 :]], tt[...])], axis=0
        )
        summed = (beside(-1, True) + beside(1, False)) + (above + below) + along
        span = pl.ds(lo * 8, count * 8)
        dst[span, :] = b_ref[span, :] + a_ref[span, :] * summed

    keep_first, keep_last = ml, mr
    fluid_span = (((13, 83), (14, 82)), ((19, 77), (20, 76)), ((25, 71), (26, 70)))
    solid_span = (((6, 42), (7, 41)), ((9, 39), (10, 38)), ((12, 36), (13, 35)))
    fluid_refs = (xf0, xf0, xf2)
    fluid_out = (xf0, xf2, xf0)
    for k in range(4):
        fluid_ref = (xf0, xf0, xf2, xf0)[k]
        project_fluid(xs0, k)
        project_solid(fluid_ref, k)
        if k == 3:
            break
        for par in range(2):
            xb[pl.ds(64 + par * 8, 40, stride=16), :] = fin[xb0[par]] + fin[4 + 2 * k + par]
        xsb[srows, :] = sin[0] + sin[1] * sin[2 + k]
        for n in range(2):
            lo, hi = fluid_span[k][n]
            src, dst = (fluid_refs[k], xf1) if n == 0 else (xf1, fluid_out[k])
            face_sweep(src, dst, xa, xb, FX, lo, hi)
            lo, hi = solid_span[k][n]
            src, dst = (xs0, xs1) if n == 0 else (xs1, xs0)
            face_sweep(src, dst, xsa, xsb, SX, lo, hi)
    recv["sinr"] = send(sins, sinr, 22, (gp, d))

    recv["bhlr"].wait_recv()
    recv["bhrr"].wait_recv()
    for ref, first_row, mask, film_at in ((bhlr, 0, ml, 28), (bhrr, 36, mr, 64)):
        for i in range(4):
            p[pl.ds((first_row + i) * FY, FY), :] = to_f32(ref[pl.ds(i * FY, FY), :]) * mask
        skip = 1 if first_row == 0 else 0
        for i in range(3):
            row = first_row + skip + i
            a[pl.ds(row * FY, FY), :] = to_f32(ref[pl.ds((4 + i) * FY, FY), :]) * mask
        for i in range(3):
            row = first_row + skip + i
            film = fxx[pl.ds(film_at + skip + i, 1), :]
            r0, s0 = a[pl.ds(row * FY, 1), :], p[pl.ds(row * FY, 1), :]
            a0, b0, _ = film_coef(r0, s0, film)
            coef(p, a, a, b, row * FY, FY)
            a[pl.ds(row * FY, 1), :] = a0
            b[pl.ds(row * FY, 1), :] = b0
    edges((None,) * 4)
    mhl[...] = p[pl.ds(4 * FY, 4 * FY), :].astype(BF16)
    mhr[...] = p[pl.ds(32 * FY, 4 * FY), :].astype(BF16)
    recv["mhrr"] = send(mhl, mhrr, 20, (g, dm))
    recv["mhlr"] = send(mhr, mhlr, 21, (g, dp))

    wide = lax.broadcasted_iota(jnp.int32, (20, FZ), 0)
    inside = jnp.where(wide < 2, ml, jnp.where(wide >= 18, mr, 1.0))
    for v in range(2):
        for i in range(1, 39):
            bt[pl.ds(v * 320 + i * 8, 8), :] = b[pl.ds(i * FY, 8), :]
        for par in range(2):
            rows = pl.ds(v * 320 + par * 8, 20, stride=16)
            bt[rows, :] = bt[rows, :] + fin[4 + 2 * (2 + v) + par][10:30] * inside

    def patch(i, mask):
        low = lax.broadcasted_iota(jnp.int32, (8, FZ), 0) < 4
        fresh = xf2[pl.ds((28 + i) * 8, 8), :]
        if mask is not None:
            fresh = fresh * mask
        p[pl.ds(i * FY, 8), :] = jnp.where(low, fresh, p[pl.ds(i * FY, 8), :])

    for i in range(4, 36):
        patch(i, None)
    second = (0, 0, 1, 1)
    interior(second)

    for name in ("scbl", "scbr", "shlr", "shrr", "sinr"):
        recv[name].wait_recv()
    for f, ref in ((0, sp), (1, sa)):
        ref[pl.ds(0, 8 * SY), :] = to_f32(shlr[f]) * ml
        ref[pl.ds(24 * SY, 8 * SY), :] = to_f32(shrr[f]) * mr
    fsx[pl.ds(0, 8), :] = scbl[pl.ds(8, 8), :] * ml
    fsx[pl.ds(8, SX), :] = scv[...]
    fsx[pl.ds(24, 8), :] = scbr[pl.ds(0, 8), :] * mr
    last_rows = pl.ds(SY - 1, 32, stride=SY)
    a0, b0, c0 = film_coef(sa[last_rows, :], sp[last_rows, :], fsx[...])
    rows_loop(0, 8, 2, lambda x: coef(sp, sa, sa, sbb, at_row(x, 96), 96))
    sa[last_rows, :] = a0
    sbb[last_rows, :] = b0
    for k in range(4):
        for i in range(32):
            sbt[pl.ds(k * 256 + i * 8, 8), :] = sbb[pl.ds(i * SY + 16, 8), :]
        sbt[pl.ds(k * 256 + 7, 32, stride=8), :] = b0 + c0 * sinr[k]

    for m in range(8):
        src, dst = (sp, sq) if m % 2 == 0 else (sq, sp)
        rows = range(1 + m, 31 - m)

        def fixed(n, tile):
            if tile == 2:
                return sbt[pl.ds((m // 2) * 256 + rows[n] * 8, 8), :]
            return sbb[pl.ds(rows[n] * SY + 8 * tile, 8), :]

        sweep_rows(
            [[((src, (x - 1) * SY), (src, x * SY), (src, (x + 1) * SY), (dst, x * SY)) for x in rows]],
            3, 1, tt[...], lambda n, tile: sa[pl.ds(rows[n] * SY + 8 * tile, 8), :], fixed,
        )

    recv["mhlr"].wait_recv()
    recv["mhrr"].wait_recv()
    p[pl.ds(0, 4 * FY), :] = to_f32(mhlr[...]) * ml
    p[pl.ds(36 * FY, 4 * FY), :] = to_f32(mhrr[...]) * mr
    for i in range(4):
        patch(i, ml)
        patch(36 + i, mr)
    for copy in sends:
        copy.wait_send()


def finish(p, q, a, b, bt, sp, fo, so, rows, tt, sem):
    copies = [
        pltpu.make_async_copy(p.at[pl.ds(8 * FY, 24 * FY)], fo.at[pl.ds(4 * FY, 24 * FY)], sem.at[0]),
        pltpu.make_async_copy(sp.at[pl.ds(8 * SY, SX * SY)], so, sem.at[1]),
    ]
    for copy in copies:
        copy.start()
    band(tt)
    for m in range(4):
        groups, xs = [], []
        for side, x0 in ((0, 1 + m), (1, 35 - m)):
            def at(x, side=side):
                lo = (m, 36 - m)[side]
                if m and lo <= x < lo + 4:
                    return rows, ((m - 1) * 8 + side * 4 + x - lo) * FY
                return (p, q)[m % 2], x * FY

            groups.append(
                [
                    (at(x - 1), at(x), at(x + 1), (rows, (m * 8 + side * 4 + x - x0) * FY))
                    for x in range(x0, x0 + 4)
                ]
            )
            xs.extend(range(x0, x0 + 4))

        def fixed(n, tile):
            if tile == 0:
                return bt[pl.ds((m // 2) * 320 + xs[n] * 8, 8), :]
            return b[pl.ds(xs[n] * FY + 8 * tile, 8), :]

        sweep_rows(
            groups, 12, 6, tt[...], lambda n, tile: a[pl.ds(xs[n] * FY + 8 * tile, 8), :], fixed
        )
    for side, x in ((0, 0), (1, 28)):
        copies.append(
            pltpu.make_async_copy(
                rows.at[pl.ds((24 + 4 * side) * FY, 4 * FY)],
                fo.at[pl.ds(x * FY, 4 * FY)], sem.at[2 + side],
            )
        )
        copies[-1].start()
    for copy in copies:
        copy.wait()


def vm(*shape, dtype=F32):
    return pltpu.VMEM(shape, dtype)


SCRATCH = [
    *(vm(32 * SY, FZ) for _ in range(3)), vm(4 * 256, FZ),
    vm(2 * SEG * FZ, FZ, dtype=BF16), vm(2 * SEG * 8, FZ),
    *(vm(96 * 8, FZ) for _ in range(6)), *(vm(48 * 8, FZ) for _ in range(5)),
    vm(6, 3 * SEG, FZ), vm(30, 40, FZ), vm(30, 40, FZ), vm(3, 64, FZ), vm(5, 64, FZ),
    vm(12, 40, FZ), vm(6, 40, FZ), vm(4, 32, FZ), vm(96, FZ), vm(32, FZ),
    vm(3 * SEG, FZ, dtype=jnp.int32),
    vm(FX, FZ), vm(SX, FZ), vm(1, SEG, dtype=jnp.int32), vm(2 * FZ, FZ, dtype=BF16),
    vm(2, 256, FZ, dtype=BF16), vm(2, 128, FZ, dtype=BF16), vm(6, SEG, FZ, dtype=BF16),
    vm(7 * FY, FZ, dtype=BF16), vm(7 * FY, FZ, dtype=BF16),
    vm(2, 8 * SY, FZ, dtype=BF16), vm(2, 8 * SY, FZ, dtype=BF16),
    vm(4 * FY, FZ, dtype=BF16), vm(4 * FY, FZ, dtype=BF16),
    vm(2, 192, FZ, dtype=BF16), vm(2, 192, FZ, dtype=BF16), vm(FX, FZ), vm(FX, FZ),
    vm(1, SEG, dtype=jnp.int32), vm(1, SEG, dtype=jnp.int32),
    *(vm(2, 128, FZ, dtype=BF16) for _ in range(3)), *(vm(SX, FZ) for _ in range(5)),
    vm(6, 80, FZ, dtype=BF16), vm(6, 80, FZ, dtype=BF16),
    vm(7 * FY, FZ, dtype=BF16), vm(7 * FY, FZ, dtype=BF16),
    vm(2, 8 * SY, FZ, dtype=BF16), vm(2, 8 * SY, FZ, dtype=BF16),
    vm(4 * FY, FZ, dtype=BF16), vm(4 * FY, FZ, dtype=BF16), vm(4, 32, FZ),
    pltpu.SemaphoreType.DMA((24,)), pltpu.SemaphoreType.DMA((23,)), pltpu.SemaphoreType.DMA((23,)),
]


STATE = (*(vm(40 * FY, FZ) for _ in range(4)), vm(2 * 320, FZ), vm(32 * SY, FZ))


def solution(mesh):
    n_grp, n_dom = mesh.shape["grp"], mesh.shape["dom"]

    def local(fs, fr, fc, ss, sr, sc, sb, ts, tf):
        state = pl.pallas_call(
            lambda *refs: kernel(n_grp, n_dom, *refs),
            out_shape=STATE,
            in_specs=[pl.BlockSpec(memory_space=pltpu.HBM)] * 9,
            out_specs=tuple(pl.BlockSpec(memory_space=pltpu.VMEM) for _ in STATE),
            scratch_shapes=SCRATCH,
            compiler_params=pltpu.CompilerParams(
                collective_id=0, has_side_effects=True, vmem_limit_bytes=58_458_112
            ),
            name="coupled",
        )(
            fs.reshape(FX * FY, FZ), fr.reshape(FX * FY, FZ), fc.reshape(FX, FZ),
            ss.reshape(SX * SY, FZ), sr.reshape(SX * SY, FZ), sc.reshape(SX, FZ),
            sb.reshape(1, SEG),
            ts.reshape(SEG * FZ, FZ), tf.reshape(SEG * FZ, FZ),
        )
        fo, so = pl.pallas_call(
            finish,
            out_shape=(
                jax.ShapeDtypeStruct((FX * FY, FZ), F32),
                jax.ShapeDtypeStruct((SX * SY, FZ), F32),
            ),
            in_specs=[pl.BlockSpec(memory_space=pltpu.VMEM)] * 6,
            out_specs=[pl.BlockSpec(memory_space=pltpu.HBM)] * 2,
            scratch_shapes=[
                vm(32 * FY, FZ), vm(2 * FZ, FZ, dtype=BF16), pltpu.SemaphoreType.DMA((4,))
            ],
            compiler_params=pltpu.CompilerParams(vmem_limit_bytes=16 * 1024 * 1024),
            name="finish",
        )(*state)
        return fo.reshape(1, FX, FY, FZ), so.reshape(1, SX, SY, FZ)

    cells = P("grp", "dom", None, None)
    faces = P("grp", "dom", None)
    split = P(("grp", "dom"))
    mats = P(("grp", "dom"), None, None)
    return jax.shard_map(
        local,
        mesh=mesh,
        in_specs=(cells, cells, faces, cells, cells, faces, split, mats, mats),
        out_specs=(cells, cells),
        check_vma=False,
    )
```

```python
import jax
import jax.numpy as jnp
from jax import lax
from jax.experimental import pallas as pl
from jax.experimental.pallas import tpu as pltpu
from jax.sharding import PartitionSpec as P

MESH = pl.DeviceIdType.MESH
F32 = jnp.float32
BF16 = jnp.bfloat16
FX, FY, FZ = 32, 96, 128
SX, SY = 16, 24
SEG = 96
GROUP = 16


def lane_iota(shape):
    return lax.broadcasted_iota(jnp.int32, shape, 1)


def zsum(v):
    lane = lane_iota(v.shape)
    return jnp.where(lane == 0, 0.0, pltpu.roll(v, 1, 1)) + jnp.where(
        lane == FZ - 1, 0.0, pltpu.roll(v, FZ - 1, 1)
    )


def split_terms(v):
    head = v.astype(BF16)
    return jnp.concatenate([head, (v - head.astype(F32)).astype(BF16)], axis=1)


def band(tt):
    apart = (lax.broadcasted_iota(jnp.int32, (2 * FZ, FZ), 0) & (FZ - 1)) - lane_iota((2 * FZ, FZ))
    tt[...] = jnp.where((apart == 1) | (apart == -1), 1.0, 0.0).astype(BF16)


def zsum_by_product(values, tt):
    return jnp.dot(
        jnp.concatenate([split_terms(v) for v in values], axis=0), tt, preferred_element_type=F32
    )


def ysum(v):
    zero = jnp.zeros((1, FZ), F32)
    return jnp.concatenate([zero, v[:-1]], axis=0) + jnp.concatenate([v[1:], zero], axis=0)


def rows_loop(lo, hi, unroll, body):
    count = hi - lo
    groups = count // unroll if count > unroll else 0
    if groups:

        def step(i, carry):
            for j in range(unroll):
                body(lo + i * unroll + j)
            return carry

        lax.fori_loop(0, groups, step, 0)
    for x in range(lo + groups * unroll, hi):
        body(x)


def at_row(x, pitch):
    return x * pitch if isinstance(x, int) else pl.multiple_of(x * pitch, 8)


def ysum_tile(ref, at, tile, tiles, cur):
    zero = jnp.zeros((1, FZ), F32)
    if 0 < tile < tiles - 1 and tile % 2 == 0:
        return ref[pl.ds(at - 1, 8), :] + ref[pl.ds(at + 1, 8), :]
    low = zero if tile == 0 else ref[pl.ds(at - 1, 1), :]
    high = zero if tile == tiles - 1 else ref[pl.ds(at + 8, 1), :]
    return jnp.concatenate([low, cur[:-1]], axis=0) + jnp.concatenate([cur[1:], high], axis=0)


def sweep_rows(groups, tiles, rolled, tt, coef_a, fixed):
    products = []
    for group in groups:
        halves = [group[: len(group) // 2], group[len(group) // 2 :]]
        for part in halves if len(group) > 1 and tiles > rolled else [group]:
            if tiles == rolled:
                products.extend([None] * len(part))
                continue
            height = 8 * (tiles - rolled)
            total = zsum_by_product(
                [ref[pl.ds(at + 8 * rolled, height), :] for _, (ref, at), _, _ in part], tt
            )
            products.extend(total[n * height : (n + 1) * height] for n in range(len(part)))
    for tile in range(tiles):
        n = 0
        for group in groups:
            cur = None
            for left, row, right, target in group:
                here = row[1] + 8 * tile
                before = cur if cur is not None else left[0][pl.ds(left[1] + 8 * tile, 8), :]
                cur = after if cur is not None else row[0][pl.ds(here, 8), :]
                after = right[0][pl.ds(right[1] + 8 * tile, 8), :]
                summed = (before + after) + ysum_tile(row[0], here, tile, tiles, cur)
                if tile < rolled:
                    summed = summed + zsum(cur)
                else:
                    summed = summed + products[n][8 * (tile - rolled) : 8 * (tile - rolled + 1)]
                target[0][pl.ds(target[1] + 8 * tile, 8), :] = (
                    fixed(n, tile) + coef_a(n, tile) * summed
                )
                n += 1


def to_f32(v):
    return v.astype(F32)


def rounded(v):
    return v.astype(BF16).astype(F32)


def kernel(
    n_grp, n_dom,
    fs, fr, fc, ss, sr, sc, sb, ts, tf,
    p, q, a, b, bt, sp, sa, sbb, sbt,
    mt, xf0, xf1, xf2, xr, xa, xb, xs0, xs1, xsr, xsa, xsb,
    dx, vv, ww, pad, tpad, fin, sin, sins, fxx, fsx, xoff,
    fcv, scv, sbv, tt,
    ifl, ifr, is_, wb, bhl, bhr, shl, shr, mhl, mhr,
    rfl, rfr, sbl, sbr, rso, rsr, rsl,
    wr, wl, bhrr, bhlr, shrr, shlr, mhrr, mhlr, sinr,
    load_sem, send_sem, recv_sem,
):
    g = lax.axis_index("grp")
    d = lax.axis_index("dom")
    gm, gp = lax.rem(g + n_grp - 1, n_grp), lax.rem(g + 1, n_grp)
    dm, dp = lax.rem(d + n_dom - 1, n_dom), lax.rem(d + 1, n_dom)
    ml = jnp.where(d > 0, 1.0, 0.0).astype(F32)
    mr = jnp.where(d < n_dom - 1, 1.0, 0.0).astype(F32)

    barrier = pltpu.get_barrier_semaphore()
    peers = ((g, dm), (g, dp), (gm, d), (gp, d), (gm, dm), (gm, dp), (gp, dm), (gp, dp))
    for peer in peers:
        pl.semaphore_signal(barrier, inc=1, device_id=peer, device_id_type=MESH)

    loads = {}

    def load(name, src, dst, index):
        loads[name] = pltpu.make_async_copy(src, dst, load_sem.at[index])
        loads[name].start()

    load("ss", ss, sp.at[pl.ds(8 * SY, SX * SY)], 0)
    load("sr", sr, sa.at[pl.ds(8 * SY, SX * SY)], 1)
    load("sc", sc, scv, 4)
    load("fc", fc, fcv, 5)
    load("sb", sb, sbv, 6)
    load("fs", fs, p.at[pl.ds(4 * FY, FX * FY)], 2)
    load("fr", fr, a.at[pl.ds(4 * FY, FX * FY)], 3)
    for t, src in ((0, ts), (1, tf)):
        load(("m", t), src, mt.at[pl.ds(t * SEG * FZ, SEG * FZ)], 7 + t)

    sends = []
    inner_left, inner_right = d > 0, d < n_dom - 1
    band(tt)

    def send(src, dst, index, peer, when=None, got=None):
        copy = pltpu.make_async_remote_copy(
            src_ref=src, dst_ref=dst, send_sem=send_sem.at[index], recv_sem=recv_sem.at[index],
            device_id=peer, device_id_type=MESH,
        )
        if when is None:
            copy.start()
        else:
            pl.when(when)(copy.start)
        sends.append((copy, when))
        return copy.wait_recv if got is None else lambda: pl.when(got)(copy.wait_recv)

    @pl.when(d == 0)
    def _():
        for ref in (bhlr, shlr, mhlr):
            ref[...] = jnp.zeros(ref.shape, BF16)

    @pl.when(d == n_dom - 1)
    def _():
        for ref in (bhrr, shrr, mhrr):
            ref[...] = jnp.zeros(ref.shape, BF16)

    loads["ss"].wait()
    loads["sr"].wait()
    loads["sc"].wait()
    for f, ref in ((0, sp), (1, sa)):
        for i in range(SX // 2):
            lo = (8 + 2 * i) * SY + 16
            is_[pl.ds(128 * f + 16 * i, 16), :] = jnp.concatenate(
                [ref[pl.ds(lo, 8), :], ref[pl.ds(lo + SY, 8), :]], axis=0
            ).astype(BF16)
        shl[pl.ds(192 * f, 192), :] = ref[pl.ds(8 * SY, 8 * SY), :].astype(BF16)
        shr[pl.ds(192 * f, 192), :] = ref[pl.ds(16 * SY, 8 * SY), :].astype(BF16)
    is_[pl.ds(256, SX), :] = scv[...].astype(BF16)
    shl[pl.ds(384, SX), :] = scv[...].astype(BF16)
    shr[pl.ds(384, SX), :] = scv[...].astype(BF16)

    def fluid_ready():
        loads["fs"].wait()
        loads["fr"].wait()
        loads["fc"].wait()
        loads["sb"].wait()
        for f, ref in ((0, p), (1, a)):
            for i in range(FX // 2):
                lo = (4 + 2 * i) * FY
                pair = jnp.concatenate([ref[pl.ds(lo, 8), :], ref[pl.ds(lo + FY, 8), :]], axis=0)
                if i < 12:
                    ifl[pl.ds(192 * f + 16 * i, 16), :] = pair.astype(BF16)
                if i >= 4:
                    ifr[pl.ds(192 * f + 16 * (i - 4), 16), :] = pair.astype(BF16)
                own = xf0 if f == 0 else xr
                own[pl.ds((FX + 2 * i) * 8, 16), :] = pair
        for ref in (ifl, ifr):
            ref[pl.ds(384, FX), :] = fcv[...].astype(BF16)
        for i in range(4):
            bhl[pl.ds(i * FY, FY), :] = p[pl.ds((4 + i) * FY, FY), :].astype(BF16)
            bhr[pl.ds(i * FY, FY), :] = p[pl.ds((32 + i) * FY, FY), :].astype(BF16)
        for i in range(3):
            bhl[pl.ds((4 + i) * FY, FY), :] = a[pl.ds((4 + i) * FY, FY), :].astype(BF16)
            bhr[pl.ds((4 + i) * FY, FY), :] = a[pl.ds((33 + i) * FY, FY), :].astype(BF16)

    def coef(start_ref, rate_ref, a_ref, b_ref, lo, size):
        r = rate_ref[pl.ds(lo, size), :]
        inv = 1.0 / (1.0 + 6.0 * r)
        b_ref[pl.ds(lo, size), :] = start_ref[pl.ds(lo, size), :] * inv
        a_ref[pl.ds(lo, size), :] = r * inv

    def film_coef(r0, s0, film):
        inv0 = 1.0 / (1.0 + 6.0 * r0 + film)
        return r0 * inv0, s0 * inv0, film * inv0

    def fluid_sweep(src, dst, variant, spans):
        groups, bases, rows = [], [], []
        for x0, count in spans:
            group = []
            for n in range(count):
                base = x0 * FY + n * FY if isinstance(x0, int) else pl.multiple_of(x0 * FY, 8) + n * FY
                bases.append(base)
                rows.append(x0 + n)
                group.append(((src, base - FY), (src, base), (src, base + FY), (dst, base)))
            groups.append(group)

        def fixed(n, tile):
            if tile == 0 and variant is not None:
                return bt[pl.ds(variant * 320 + at_row(rows[n], 8), 8), :]
            return b[pl.ds(bases[n] + 8 * tile, 8), :]

        sweep_rows(
            groups, 12, 6, tt[...], lambda n, tile: a[pl.ds(bases[n] + 8 * tile, 8), :], fixed
        )

    def interior(variants, sweeps=range(4)):
        for m in sweeps:
            block = (10, 7, 13, 8)[m]
            src, dst = (p, q) if m % 2 == 0 else (q, p)

            def step(i, carry):
                fluid_sweep(src, dst, variants[m], ((5 + m + i * block, block),))
                return carry

            lax.fori_loop(0, (30 - 2 * m) // block, step, 0)

    def edges(variants):
        for m in range(4):
            src, dst = (p, q) if m % 2 == 0 else (q, p)
            fluid_sweep(src, dst, variants[m], ((1 + m, 4), (35 - m, 4)))

    def local_work():
        own_rows = pl.ds(4 * FY, FX, stride=FY)
        a0, b0, _ = film_coef(a[own_rows, :], p[own_rows, :], fcv[...])
        rows_loop(4, 36, 4, lambda x: coef(p, a, a, b, at_row(x, FY), FY))
        a[own_rows, :] = a0
        b[own_rows, :] = b0
        interior((None,) * 4, range(1))
        folded_row = lax.broadcasted_iota(jnp.int32, (16, FZ), 0)
        folded_col = lane_iota((16, FZ))
        masks = [
            jnp.where(((folded_col + shift) & 15) == folded_row, 1.0, 0.0).astype(BF16)
            for shift in (0, 15, 1)
        ]
        owner = lax.broadcasted_iota(jnp.int32, (GROUP, GROUP * 16), 1) // 16
        gather = jnp.where(
            owner == lax.broadcasted_iota(jnp.int32, (GROUP, GROUP * 16), 0), 1.0, 0.0
        ).astype(BF16)
        for t in range(2):
            loads[("m", t)].wait()
            for c in range(SEG // GROUP):
                folded = []
                for n in range(GROUP):
                    at = (t * SEG + c * GROUP + n) * FZ
                    parts = [mt[pl.ds(at + 16 * r, 16), :] for r in range(8)]
                    while len(parts) > 1:
                        parts = [u + v for u, v in zip(parts[::2], parts[1::2])]
                    folded.append(parts[0])
                for k in range(3):
                    picked = jnp.dot(
                        gather, jnp.concatenate([f * masks[k] for f in folded], axis=0),
                        preferred_element_type=F32,
                    )
                    dx[3 * t + k, pl.ds(SEG + c * GROUP, GROUP), :] = picked
                    wb[3 * t + k, pl.ds(c * GROUP, GROUP), :] = picked.astype(BF16)

    early = (g == 0) | (d == 0)

    @pl.when(early)
    def _():
        fluid_ready()
        local_work()

    pl.semaphore_wait(barrier, 8)
    recv = {}
    recv["rso"] = send(is_, rso, 2, (gm, d))
    recv["rsr"] = send(is_, rsr, 3, (gm, dm))
    recv["rsl"] = send(is_, rsl, 4, (gm, dp))

    @pl.when(jnp.logical_not(early))
    def _():
        fluid_ready()

    recv["rfr"] = send(ifl, rfr, 0, (g, dm))
    recv["rfl"] = send(ifr, rfl, 1, (g, dp))
    recv["sbr"] = send(sbv, sbr, 5, (g, dm))
    recv["sbl"] = send(sbv, sbl, 6, (g, dp))

    @pl.when(jnp.logical_not(early))
    def _():
        local_work()

    recv["wr"] = send(wb.at[:, pl.ds(0, 80)], wr, 7, (g, dm))
    recv["wl"] = send(wb.at[:, pl.ds(16, 80)], wl, 8, (g, dp))
    recv["bhrr"] = send(bhl, bhrr, 9, (g, dm), inner_left, inner_right)
    recv["bhlr"] = send(bhr, bhlr, 10, (g, dp), inner_right, inner_left)
    recv["shrr"] = send(shl, shrr, 11, (g, dm), inner_left, inner_right)
    recv["shlr"] = send(shr, shlr, 12, (g, dp), inner_right, inner_left)

    interior((None,) * 4, range(1, 4))

    recv["rfl"]()
    recv["rfr"]()
    for f, ref in ((0, xf0), (1, xr)):
        ref[pl.ds(64, 192), :] = to_f32(rfl[pl.ds(192 * f, 192), :])
        ref[pl.ds(512, 192), :] = to_f32(rfr[pl.ds(192 * f, 192), :])
    fxx[pl.ds(0, FX), :] = to_f32(rfl[pl.ds(384, FX), :])
    fxx[pl.ds(FX, FX), :] = fcv[...]
    fxx[pl.ds(2 * FX, FX), :] = to_f32(rfr[pl.ds(384, FX), :])
    rows_loop(1, 11, 2, lambda x: coef(xf0, xr, xa, xb, at_row(x, 64), 64))
    xc = []
    xb0 = []
    for par in range(2):
        rows = pl.ds(64 + par * 8, 40, stride=16)
        film = fxx[pl.ds(8 + par, 40, stride=2), :]
        a0, b0, c0 = film_coef(xr[rows, :], xf0[rows, :], film)
        xa[rows, :] = a0
        fin[par] = b0
        fin[2 + par] = c0
        xc.append(2 + par)
        xb0.append(par)

    for name in ("rso", "rsr", "rsl"):
        recv[name]()
    for f, ref in ((0, xs0), (1, xsr)):
        for n, got in enumerate((rsl, rso, rsr)):
            ref[pl.ds(128 * n, 128), :] = to_f32(got[pl.ds(128 * f, 128), :])
    rows_loop(0, 6, 2, lambda x: coef(xs0, xsr, xsa, xsb, at_row(x, 64), 64))
    srows = pl.ds(32 + 7, 40, stride=8)
    film = jnp.concatenate([to_f32(got[pl.ds(256, SX), :]) for got in (rsl, rso, rsr)], axis=0)[4:44]
    a0, b0, c0 = film_coef(xsr[srows, :], xs0[srows, :], film)
    xsa[srows, :] = a0
    sin[0] = b0
    sin[1] = c0

    for name in ("sbl", "sbr", "wl", "wr"):
        recv[name]()
    for k in range(6):
        dx[k, pl.ds(16, 80), :] = to_f32(wl[k])
        dx[k, pl.ds(192, 80), :] = to_f32(wr[k])
    for n, ref in enumerate((sbl, sbv, sbr)):
        row = jnp.concatenate([ref[...].astype(F32), jnp.zeros((1, FZ - SEG), F32)], axis=1)
        spread = jnp.broadcast_to(row, (FZ, FZ)).T
        xoff[pl.ds(n * SEG, SEG), :] = spread[:SEG].astype(jnp.int32)
    first = SX * (d + n_dom - 1) - 2
    zone = SX * n_dom
    half = lax.broadcasted_iota(jnp.int32, (40, FZ), 0) + (first + 4)
    for par in range(2):
        offs = [
            lax.rem(xoff[pl.ds(24 + 3 * par + j, 40, stride=6), :] - half + 3 * zone, zone)
            for j in range(3)
        ]
        for t in range(2):
            for k in range(3):
                diag = [dx[3 * t + k, pl.ds(24 + 3 * par + j, 40, stride=6), :] for j in range(3)]
                for o in range(5):
                    total = jnp.where(offs[0] == o, diag[0], 0.0)
                    total = total + jnp.where(offs[1] == o, diag[1], 0.0)
                    total = total + jnp.where(offs[2] == o, diag[2], 0.0)
                    at = (o * 3 + k) * 2 + par
                    if t == 0:
                        ww[at] = total
                    else:
                        vv[at] = total * fin[xc[par]]

    def shifts(v):
        return (v, pltpu.roll(v, 1, 1), pltpu.roll(v, FZ - 1, 1))

    def project_fluid(solid_ref, k):
        for n, v in enumerate(shifts(rounded(solid_ref[srows, :]))):
            pad[n, pl.ds(8, 40), :] = v
        for par in range(2):
            total = jnp.zeros((40, FZ), F32)
            for o in range(5):
                for n in range(3):
                    total = total + vv[(o * 3 + n) * 2 + par] * pad[n, pl.ds(6 + o, 40), :]
            fin[4 + 2 * k + par] = total

    def project_solid(fluid_ref, k):
        faces = [
            shifts(rounded(fluid_ref[pl.ds(64 + par * 8, 40, stride=16), :])) for par in range(2)
        ]
        for o in range(5):
            total = jnp.zeros((40, FZ), F32)
            for par in range(2):
                for n in range(3):
                    total = total + ww[(o * 3 + n) * 2 + par] * faces[par][n]
            tpad[o, pl.ds(8, 40), :] = total
        total = tpad[0, pl.ds(10, 40), :]
        for o in range(1, 5):
            total = total + tpad[o, pl.ds(10 - o, 40), :]
        sin[2 + k] = total
        sins[k] = total[4:36]

    def face_sweep(src, dst, a_ref, b_ref, width, lo, hi):
        count = hi - lo
        by_rolls = count - 2 * (count // 4)

        def beside(step, first):
            pieces, x = [], lo + step
            for cut, keep in ((width, keep_first), (2 * width, keep_last)):
                row = cut - 1 if first else cut
                if x < row:
                    pieces.append(src[pl.ds(x * 8, (row - x) * 8), :])
                pieces.append(src[pl.ds(row * 8, 8), :] * keep)
                x = row + 1
            if x < hi + step:
                pieces.append(src[pl.ds(x * 8, (hi + step - x) * 8), :])
            return jnp.concatenate(pieces, axis=0)

        cur = src[pl.ds(lo * 8, count * 8), :]
        sub = lax.broadcasted_iota(jnp.int32, (count * 8, FZ), 0) & 7
        above = jnp.where(sub == 0, 0.0, src[pl.ds(lo * 8 - 1, count * 8), :])
        below = jnp.where(sub == 7, 0.0, src[pl.ds(lo * 8 + 1, count * 8), :])
        along = jnp.concatenate(
            [zsum(cur[: by_rolls * 8]), zsum_by_product([cur[by_rolls * 8 :]], tt[...])], axis=0
        )
        summed = (beside(-1, True) + beside(1, False)) + (above + below) + along
        span = pl.ds(lo * 8, count * 8)
        dst[span, :] = b_ref[span, :] + a_ref[span, :] * summed

    keep_first, keep_last = ml, mr
    fluid_span = (((13, 83), (14, 82)), ((19, 77), (20, 76)), ((25, 71), (26, 70)))
    solid_span = (((6, 42), (7, 41)), ((9, 39), (10, 38)), ((12, 36), (13, 35)))
    fluid_refs = (xf0, xf0, xf2)
    fluid_out = (xf0, xf2, xf0)
    for k in range(4):
        fluid_ref = (xf0, xf0, xf2, xf0)[k]
        project_fluid(xs0, k)
        project_solid(fluid_ref, k)
        if k == 3:
            break
        for par in range(2):
            xb[pl.ds(64 + par * 8, 40, stride=16), :] = fin[xb0[par]] + fin[4 + 2 * k + par]
        xsb[srows, :] = sin[0] + sin[1] * sin[2 + k]
        for n in range(2):
            lo, hi = fluid_span[k][n]
            src, dst = (fluid_refs[k], xf1) if n == 0 else (xf1, fluid_out[k])
            face_sweep(src, dst, xa, xb, FX, lo, hi)
            lo, hi = solid_span[k][n]
            src, dst = (xs0, xs1) if n == 0 else (xs1, xs0)
            face_sweep(src, dst, xsa, xsb, SX, lo, hi)
    recv["sinr"] = send(sins, sinr, 13, (gp, d))

    recv["bhlr"]()
    recv["bhrr"]()
    for ref, first_row, film_at in ((bhlr, 0, 28), (bhrr, 36, 64)):
        for i in range(4):
            p[pl.ds((first_row + i) * FY, FY), :] = to_f32(ref[pl.ds(i * FY, FY), :])
        skip = 1 if first_row == 0 else 0
        for i in range(3):
            row = first_row + skip + i
            a[pl.ds(row * FY, FY), :] = to_f32(ref[pl.ds((4 + i) * FY, FY), :])
        for i in range(3):
            row = first_row + skip + i
            film = fxx[pl.ds(film_at + skip + i, 1), :]
            r0, s0 = a[pl.ds(row * FY, 1), :], p[pl.ds(row * FY, 1), :]
            a0, b0, _ = film_coef(r0, s0, film)
            coef(p, a, a, b, row * FY, FY)
            a[pl.ds(row * FY, 1), :] = a0
            b[pl.ds(row * FY, 1), :] = b0
    edges((None,) * 4)
    mhl[...] = p[pl.ds(4 * FY, 4 * FY), :].astype(BF16)
    mhr[...] = p[pl.ds(32 * FY, 4 * FY), :].astype(BF16)
    recv["mhrr"] = send(mhl, mhrr, 14, (g, dm), inner_left, inner_right)
    recv["mhlr"] = send(mhr, mhlr, 15, (g, dp), inner_right, inner_left)

    wide = lax.broadcasted_iota(jnp.int32, (20, FZ), 0)
    inside = jnp.where(wide < 2, ml, jnp.where(wide >= 18, mr, 1.0))
    for v in range(2):
        for i in range(1, 39):
            bt[pl.ds(v * 320 + i * 8, 8), :] = b[pl.ds(i * FY, 8), :]
        for par in range(2):
            rows = pl.ds(v * 320 + par * 8, 20, stride=16)
            bt[rows, :] = bt[rows, :] + fin[4 + 2 * (2 + v) + par][10:30] * inside

    def patch(i, mask):
        low = lax.broadcasted_iota(jnp.int32, (8, FZ), 0) < 4
        fresh = xf2[pl.ds((28 + i) * 8, 8), :]
        if mask is not None:
            fresh = fresh * mask
        p[pl.ds(i * FY, 8), :] = jnp.where(low, fresh, p[pl.ds(i * FY, 8), :])

    for i in range(4, 36):
        patch(i, None)
    second = (0, 0, 1, 1)
    interior(second)

    recv["shlr"]()
    recv["shrr"]()
    for f, ref in ((0, sp), (1, sa)):
        ref[pl.ds(0, 8 * SY), :] = to_f32(shlr[pl.ds(192 * f, 192), :])
        ref[pl.ds(24 * SY, 8 * SY), :] = to_f32(shrr[pl.ds(192 * f, 192), :])
    fsx[pl.ds(0, 8), :] = to_f32(shlr[pl.ds(384, SX), :])[8:]
    fsx[pl.ds(8, SX), :] = scv[...]
    fsx[pl.ds(24, 8), :] = to_f32(shrr[pl.ds(384, SX), :])[:8]
    last_rows = pl.ds(SY - 1, 32, stride=SY)
    a0, b0, c0 = film_coef(sa[last_rows, :], sp[last_rows, :], fsx[...])
    rows_loop(0, 8, 2, lambda x: coef(sp, sa, sa, sbb, at_row(x, 96), 96))
    sa[last_rows, :] = a0
    sbb[last_rows, :] = b0
    for k in range(4):
        for i in range(32):
            sbt[pl.ds(k * 256 + i * 8, 8), :] = sbb[pl.ds(i * SY + 16, 8), :]
    recv["sinr"]()
    for k in range(4):
        sbt[pl.ds(k * 256 + 7, 32, stride=8), :] = b0 + c0 * sinr[k]

    recv["mhlr"]()
    recv["mhrr"]()
    p[pl.ds(0, 4 * FY), :] = to_f32(mhlr[...])
    p[pl.ds(36 * FY, 4 * FY), :] = to_f32(mhrr[...])
    for i in range(4):
        patch(i, ml)
        patch(36 + i, mr)
    for copy, when in sends:
        if when is None:
            copy.wait_send()
        else:
            pl.when(when)(copy.wait_send)


def finish(p, q, a, b, bt, sp, sa, sbb, sbt, fo, so, rows, s1, s2, tt, sem):
    copies = [
        pltpu.make_async_copy(p.at[pl.ds(8 * FY, 24 * FY)], fo.at[pl.ds(4 * FY, 24 * FY)], sem.at[0])
    ]
    copies[0].start()
    band(tt)

    def solid_sweep(m):
        span = range(1 + m, 31 - m)
        src = sp if m == 0 else (s2, s1)[m % 2]
        dst = (s1, s2)[m % 2]

        def fixed(n, tile):
            if tile == 2:
                return sbt[pl.ds((m // 2) * 256 + span[n] * 8, 8), :]
            return sbb[pl.ds(span[n] * SY + 8 * tile, 8), :]

        sweep_rows(
            [[((src, (x - 1) * SY), (src, x * SY), (src, (x + 1) * SY), (dst, x * SY)) for x in span]],
            3, 1, tt[...], lambda n, tile: sa[pl.ds(span[n] * SY + 8 * tile, 8), :], fixed,
        )

    for m in range(4):
        groups, xs = [], []
        for side, x0 in ((0, 1 + m), (1, 35 - m)):
            def at(x, side=side):
                lo = (m, 36 - m)[side]
                if m and lo <= x < lo + 4:
                    return rows, ((m - 1) * 8 + side * 4 + x - lo) * FY
                return (p, q)[m % 2], x * FY

            groups.append(
                [
                    (at(x - 1), at(x), at(x + 1), (rows, (m * 8 + side * 4 + x - x0) * FY))
                    for x in range(x0, x0 + 4)
                ]
            )
            xs.extend(range(x0, x0 + 4))

        def fixed(n, tile):
            if tile == 0:
                return bt[pl.ds((m // 2) * 320 + xs[n] * 8, 8), :]
            return b[pl.ds(xs[n] * FY + 8 * tile, 8), :]

        sweep_rows(
            groups, 12, 6, tt[...], lambda n, tile: a[pl.ds(xs[n] * FY + 8 * tile, 8), :], fixed
        )
        solid_sweep(2 * m)
        solid_sweep(2 * m + 1)
    copies.append(pltpu.make_async_copy(s2.at[pl.ds(8 * SY, SX * SY)], so, sem.at[1]))
    copies[-1].start()
    for side, x in ((0, 0), (1, 28)):
        copies.append(
            pltpu.make_async_copy(
                rows.at[pl.ds((24 + 4 * side) * FY, 4 * FY)],
                fo.at[pl.ds(x * FY, 4 * FY)], sem.at[2 + side],
            )
        )
        copies[-1].start()
    for copy in copies:
        copy.wait()


def vm(*shape, dtype=F32):
    return pltpu.VMEM(shape, dtype)


SCRATCH = [
    vm(2 * SEG * FZ, FZ, dtype=BF16),
    *(vm(96 * 8, FZ) for _ in range(6)), *(vm(48 * 8, FZ) for _ in range(5)),
    vm(6, 3 * SEG, FZ), vm(30, 40, FZ), vm(30, 40, FZ), vm(3, 64, FZ), vm(5, 64, FZ),
    vm(12, 40, FZ), vm(6, 40, FZ), vm(4, 32, FZ), vm(96, FZ), vm(32, FZ),
    vm(3 * SEG, FZ, dtype=jnp.int32),
    vm(FX, FZ), vm(SX, FZ), vm(1, SEG, dtype=jnp.int32), vm(2 * FZ, FZ, dtype=BF16),
    vm(416, FZ, dtype=BF16), vm(416, FZ, dtype=BF16), vm(272, FZ, dtype=BF16),
    vm(6, SEG, FZ, dtype=BF16), vm(7 * FY, FZ, dtype=BF16), vm(7 * FY, FZ, dtype=BF16),
    vm(400, FZ, dtype=BF16), vm(400, FZ, dtype=BF16),
    vm(4 * FY, FZ, dtype=BF16), vm(4 * FY, FZ, dtype=BF16),
    vm(416, FZ, dtype=BF16), vm(416, FZ, dtype=BF16),
    vm(1, SEG, dtype=jnp.int32), vm(1, SEG, dtype=jnp.int32),
    *(vm(272, FZ, dtype=BF16) for _ in range(3)),
    vm(6, 80, FZ, dtype=BF16), vm(6, 80, FZ, dtype=BF16),
    vm(7 * FY, FZ, dtype=BF16), vm(7 * FY, FZ, dtype=BF16),
    vm(400, FZ, dtype=BF16), vm(400, FZ, dtype=BF16),
    vm(4 * FY, FZ, dtype=BF16), vm(4 * FY, FZ, dtype=BF16), vm(4, 32, FZ),
    pltpu.SemaphoreType.DMA((9,)), pltpu.SemaphoreType.DMA((16,)), pltpu.SemaphoreType.DMA((16,)),
]


STATE = (
    *(vm(40 * FY, FZ) for _ in range(4)), vm(2 * 320, FZ),
    *(vm(32 * SY, FZ) for _ in range(3)), vm(4 * 256, FZ),
)


def solution(mesh):
    n_grp, n_dom = mesh.shape["grp"], mesh.shape["dom"]

    def local(fs, fr, fc, ss, sr, sc, sb, ts, tf):
        state = pl.pallas_call(
            lambda *refs: kernel(n_grp, n_dom, *refs),
            out_shape=STATE,
            in_specs=[pl.BlockSpec(memory_space=pltpu.HBM)] * 9,
            out_specs=tuple(pl.BlockSpec(memory_space=pltpu.VMEM) for _ in STATE),
            scratch_shapes=SCRATCH,
            compiler_params=pltpu.CompilerParams(
                collective_id=0, has_side_effects=True, vmem_limit_bytes=57_147_392
            ),
            name="coupled",
        )(
            fs.reshape(FX * FY, FZ), fr.reshape(FX * FY, FZ), fc.reshape(FX, FZ),
            ss.reshape(SX * SY, FZ), sr.reshape(SX * SY, FZ), sc.reshape(SX, FZ),
            sb.reshape(1, SEG),
            ts.reshape(SEG * FZ, FZ), tf.reshape(SEG * FZ, FZ),
        )
        fo, so = pl.pallas_call(
            finish,
            out_shape=(
                jax.ShapeDtypeStruct((FX * FY, FZ), F32),
                jax.ShapeDtypeStruct((SX * SY, FZ), F32),
            ),
            in_specs=[pl.BlockSpec(memory_space=pltpu.VMEM)] * 9,
            out_specs=[pl.BlockSpec(memory_space=pltpu.HBM)] * 2,
            scratch_shapes=[
                vm(32 * FY, FZ), vm(32 * SY, FZ), vm(32 * SY, FZ), vm(2 * FZ, FZ, dtype=BF16),
                pltpu.SemaphoreType.DMA((4,)),
            ],
            compiler_params=pltpu.CompilerParams(vmem_limit_bytes=16 * 1024 * 1024),
            name="finish",
        )(*state)
        return fo.reshape(1, FX, FY, FZ), so.reshape(1, SX, SY, FZ)

    cells = P("grp", "dom", None, None)
    faces = P("grp", "dom", None)
    split = P(("grp", "dom"))
    mats = P(("grp", "dom"), None, None)
    return jax.shard_map(
        local,
        mesh=mesh,
        in_specs=(cells, cells, faces, cells, cells, faces, split, mats, mats),
        out_specs=(cells, cells),
        check_vma=False,
    )
```

```python
import jax
import jax.numpy as jnp
from jax import lax
from jax.experimental import pallas as pl
from jax.experimental.pallas import tpu as pltpu
from jax.sharding import PartitionSpec as P

MESH = pl.DeviceIdType.MESH
F32 = jnp.float32
BF16 = jnp.bfloat16
FX, FY, FZ = 32, 96, 128
SX, SY = 16, 24
SEG = 96
GROUP = 16


def lane_iota(shape):
    return lax.broadcasted_iota(jnp.int32, shape, 1)


def zsum(v):
    lane = lane_iota(v.shape)
    return jnp.where(lane == 0, 0.0, pltpu.roll(v, 1, 1)) + jnp.where(
        lane == FZ - 1, 0.0, pltpu.roll(v, FZ - 1, 1)
    )


def split_terms(v):
    head = v.astype(BF16)
    return jnp.concatenate([head, (v - head.astype(F32)).astype(BF16)], axis=1)


def band(tt):
    apart = (lax.broadcasted_iota(jnp.int32, (2 * FZ, FZ), 0) & (FZ - 1)) - lane_iota((2 * FZ, FZ))
    tt[...] = jnp.where((apart == 1) | (apart == -1), 1.0, 0.0).astype(BF16)


def zsum_by_product(values, tt):
    return jnp.dot(
        jnp.concatenate([split_terms(v) for v in values], axis=0), tt, preferred_element_type=F32
    )


def ysum(v):
    zero = jnp.zeros((1, FZ), F32)
    return jnp.concatenate([zero, v[:-1]], axis=0) + jnp.concatenate([v[1:], zero], axis=0)


def rows_loop(lo, hi, unroll, body):
    count = hi - lo
    groups = count // unroll if count > unroll else 0
    if groups:

        def step(i, carry):
            for j in range(unroll):
                body(lo + i * unroll + j)
            return carry

        lax.fori_loop(0, groups, step, 0)
    for x in range(lo + groups * unroll, hi):
        body(x)


def at_row(x, pitch):
    return x * pitch if isinstance(x, int) else pl.multiple_of(x * pitch, 8)


def sweep_rows(groups, tiles, rolled, tt, coef_a, fixed, loaded=(1, 2, 4, 5, 6, 7, 9, 10)):
    products = []
    for group in groups:
        halves = [group[: len(group) // 2], group[len(group) // 2 :]]
        for part in halves if len(group) > 1 and tiles > rolled else [group]:
            if tiles == rolled:
                products.extend([None] * len(part))
                continue
            height = 8 * (tiles - rolled)
            total = zsum_by_product(
                [ref[pl.ds(at + 8 * rolled, height), :] for _, (ref, at), _, _ in part], tt
            )
            products.extend(total[n * height : (n + 1) * height] for n in range(len(part)))
    held = {}

    def cell(number, row, tile):
        key = number, row, tile
        if key not in held:
            group = groups[number]
            if row < 0:
                ref, at = group[0][0]
            elif row == len(group):
                ref, at = group[-1][2]
            else:
                ref, at = group[row][1]
            held[key] = ref[pl.ds(at + 8 * tile, 8), :]
        return held[key]

    zero = jnp.zeros((1, FZ), F32)
    for tile in range(tiles):
        n = 0
        for number, group in enumerate(groups):
            for row, (_, (ref, at), _, target) in enumerate(group):
                here = at + 8 * tile
                cur = cell(number, row, tile)
                beside = cell(number, row - 1, tile) + cell(number, row + 1, tile)
                if tile in loaded and tile < tiles - 1:
                    across = ref[pl.ds(here - 1, 8), :] + ref[pl.ds(here + 1, 8), :]
                else:
                    low = zero if tile == 0 else cell(number, row, tile - 1)[7:]
                    high = zero if tile == tiles - 1 else cell(number, row, tile + 1)[:1]
                    across = jnp.concatenate([low, cur[:-1]], axis=0)
                    across = across + jnp.concatenate([cur[1:], high], axis=0)
                summed = beside + across
                if tile < rolled:
                    summed = summed + zsum(cur)
                else:
                    summed = summed + products[n][8 * (tile - rolled) : 8 * (tile - rolled + 1)]
                target[0][pl.ds(target[1] + 8 * tile, 8), :] = (
                    fixed(n, tile) + coef_a(n, tile) * summed
                )
                n += 1


def to_f32(v):
    return v.astype(F32)


def rounded(v):
    return v.astype(BF16).astype(F32)


def kernel(
    n_grp, n_dom,
    fs, fr, fc, ss, sr, sc, sb, ts, tf,
    p, q, a, b, bt, sp, sa, sbb, sbt,
    mt, xf0, xf1, xf2, xr, xa, xb, xs0, xs1, xsr, xsa, xsb,
    dx, vv, ww, pad, tpad, fin, sin, sins, fxx, fsx, xoff,
    fcv, scv, sbv, tt,
    ifl, ifr, is_, wb, bhl, bhr, shl, shr, mhl, mhr,
    rfl, rfr, sbl, sbr, rso, rsr, rsl,
    wr, wl, bhrr, bhlr, shrr, shlr, mhrr, mhlr, sinr,
    load_sem, send_sem, recv_sem,
):
    g = lax.axis_index("grp")
    d = lax.axis_index("dom")
    gm, gp = lax.rem(g + n_grp - 1, n_grp), lax.rem(g + 1, n_grp)
    dm, dp = lax.rem(d + n_dom - 1, n_dom), lax.rem(d + 1, n_dom)
    ml = jnp.where(d > 0, 1.0, 0.0).astype(F32)
    mr = jnp.where(d < n_dom - 1, 1.0, 0.0).astype(F32)

    barrier = pltpu.get_barrier_semaphore()
    peers = ((g, dm), (g, dp), (gm, d), (gp, d), (gm, dm), (gm, dp), (gp, dm), (gp, dp))
    for peer in peers:
        pl.semaphore_signal(barrier, inc=1, device_id=peer, device_id_type=MESH)

    loads = {}

    def load(name, src, dst, index):
        loads[name] = pltpu.make_async_copy(src, dst, load_sem.at[index])
        loads[name].start()

    load("ss", ss, sp.at[pl.ds(8 * SY, SX * SY)], 0)
    load("sr", sr, sa.at[pl.ds(8 * SY, SX * SY)], 1)
    load("sc", sc, scv, 4)
    load("fc", fc, fcv, 5)
    load("sb", sb, sbv, 6)
    load("fs", fs, p.at[pl.ds(4 * FY, FX * FY)], 2)
    load("fr", fr, a.at[pl.ds(4 * FY, FX * FY)], 3)
    for t, src in ((0, ts), (1, tf)):
        load(("m", t), src, mt.at[pl.ds(t * SEG * FZ, SEG * FZ)], 7 + t)

    sends = []
    inner_left, inner_right = d > 0, d < n_dom - 1
    band(tt)

    def prepare(src, dst, index, peer, when=None):
        copy = pltpu.make_async_remote_copy(
            src_ref=src, dst_ref=dst, send_sem=send_sem.at[index], recv_sem=recv_sem.at[index],
            device_id=peer, device_id_type=MESH,
        )
        sends.append((copy, when))
        return copy

    def send(src, dst, index, peer, when=None, got=None):
        copy = prepare(src, dst, index, peer, when)
        if when is None:
            copy.start()
        else:
            pl.when(when)(copy.start)
        return copy.wait_recv if got is None else lambda: pl.when(got)(copy.wait_recv)

    @pl.when(d == 0)
    def _():
        for ref in (bhlr, shlr, mhlr):
            ref[...] = jnp.zeros(ref.shape, BF16)

    @pl.when(d == n_dom - 1)
    def _():
        for ref in (bhrr, shrr, mhrr):
            ref[...] = jnp.zeros(ref.shape, BF16)

    loads["ss"].wait()
    loads["sr"].wait()
    loads["sc"].wait()
    for f, ref in ((0, sp), (1, sa)):
        for i in range(SX // 2):
            lo = (8 + 2 * i) * SY + 16
            is_[pl.ds(128 * f + 16 * i, 16), :] = jnp.concatenate(
                [ref[pl.ds(lo, 8), :], ref[pl.ds(lo + SY, 8), :]], axis=0
            ).astype(BF16)
        shl[pl.ds(192 * f, 192), :] = ref[pl.ds(8 * SY, 8 * SY), :].astype(BF16)
        shr[pl.ds(192 * f, 192), :] = ref[pl.ds(16 * SY, 8 * SY), :].astype(BF16)
    is_[pl.ds(256, SX), :] = scv[...].astype(BF16)
    shl[pl.ds(384, SX), :] = scv[...].astype(BF16)
    shr[pl.ds(384, SX), :] = scv[...].astype(BF16)

    def fluid_ready():
        loads["fs"].wait()
        loads["fr"].wait()
        loads["fc"].wait()
        loads["sb"].wait()
        for f, ref in ((0, p), (1, a)):
            for i in range(FX // 2):
                lo = (4 + 2 * i) * FY
                pair = jnp.concatenate([ref[pl.ds(lo, 8), :], ref[pl.ds(lo + FY, 8), :]], axis=0)
                if i < 12:
                    ifl[pl.ds(192 * f + 16 * i, 16), :] = pair.astype(BF16)
                if i >= 4:
                    ifr[pl.ds(192 * f + 16 * (i - 4), 16), :] = pair.astype(BF16)
                own = xf0 if f == 0 else xr
                own[pl.ds((FX + 2 * i) * 8, 16), :] = pair
        for ref in (ifl, ifr):
            ref[pl.ds(384, FX), :] = fcv[...].astype(BF16)
        for i in range(4):
            bhl[pl.ds(i * FY, FY), :] = p[pl.ds((4 + i) * FY, FY), :].astype(BF16)
            bhr[pl.ds(i * FY, FY), :] = p[pl.ds((32 + i) * FY, FY), :].astype(BF16)
        for i in range(3):
            bhl[pl.ds((4 + i) * FY, FY), :] = a[pl.ds((4 + i) * FY, FY), :].astype(BF16)
            bhr[pl.ds((4 + i) * FY, FY), :] = a[pl.ds((33 + i) * FY, FY), :].astype(BF16)
        bhl[pl.ds(7 * FY, 16), :] = fcv[pl.ds(0, 16), :].astype(BF16)
        bhr[pl.ds(7 * FY, 16), :] = fcv[pl.ds(16, 16), :].astype(BF16)

    def coef(start_ref, rate_ref, a_ref, b_ref, lo, size):
        r = rate_ref[pl.ds(lo, size), :]
        inv = 1.0 / (1.0 + 6.0 * r)
        b_ref[pl.ds(lo, size), :] = start_ref[pl.ds(lo, size), :] * inv
        a_ref[pl.ds(lo, size), :] = r * inv

    def film_coef(r0, s0, film):
        inv0 = 1.0 / (1.0 + 6.0 * r0 + film)
        return r0 * inv0, s0 * inv0, film * inv0

    def fluid_sweep(src, dst, variant, spans):
        groups, bases, rows = [], [], []
        for x0, count in spans:
            group = []
            for n in range(count):
                base = x0 * FY + n * FY if isinstance(x0, int) else pl.multiple_of(x0 * FY, 8) + n * FY
                bases.append(base)
                rows.append(x0 + n)
                group.append(((src, base - FY), (src, base), (src, base + FY), (dst, base)))
            groups.append(group)

        def fixed(n, tile):
            if tile == 0 and variant is not None:
                return bt[pl.ds(variant * 320 + at_row(rows[n], 8), 8), :]
            return b[pl.ds(bases[n] + 8 * tile, 8), :]

        sweep_rows(
            groups, 12, 6, tt[...], lambda n, tile: a[pl.ds(bases[n] + 8 * tile, 8), :], fixed
        )

    def interior(variants, sweeps=range(4)):
        for m in sweeps:
            block = (10, 7, 13, 8)[m]
            src, dst = (p, q) if m % 2 == 0 else (q, p)

            def step(i, carry):
                fluid_sweep(src, dst, variants[m], ((5 + m + i * block, block),))
                return carry

            lax.fori_loop(0, (30 - 2 * m) // block, step, 0)

    def edges(variants):
        for m in range(4):
            src, dst = (p, q) if m % 2 == 0 else (q, p)
            fluid_sweep(src, dst, variants[m], ((1 + m, 4), (35 - m, 4)))

    def local_work():
        own_rows = pl.ds(4 * FY, FX, stride=FY)
        a0, b0, _ = film_coef(a[own_rows, :], p[own_rows, :], fcv[...])
        rows_loop(4, 36, 4, lambda x: coef(p, a, a, b, at_row(x, FY), FY))
        a[own_rows, :] = a0
        b[own_rows, :] = b0
        interior((None,) * 4, range(1))
        folded_row = lax.broadcasted_iota(jnp.int32, (16, FZ), 0)
        folded_col = lane_iota((16, FZ))
        masks = [
            jnp.where(((folded_col + shift) & 15) == folded_row, 1.0, 0.0).astype(BF16)
            for shift in (0, 15, 1)
        ]
        owner = lax.broadcasted_iota(jnp.int32, (GROUP, GROUP * 16), 1) // 16
        gather = jnp.where(
            owner == lax.broadcasted_iota(jnp.int32, (GROUP, GROUP * 16), 0), 1.0, 0.0
        ).astype(BF16)
        for t in range(2):
            loads[("m", t)].wait()
            for c in range(SEG // GROUP):
                folded = []
                for n in range(GROUP):
                    at = (t * SEG + c * GROUP + n) * FZ
                    parts = [mt[pl.ds(at + 16 * r, 16), :] for r in range(8)]
                    while len(parts) > 1:
                        parts = [u + v for u, v in zip(parts[::2], parts[1::2])]
                    folded.append(parts[0])
                for k in range(3):
                    picked = jnp.dot(
                        gather, jnp.concatenate([f * masks[k] for f in folded], axis=0),
                        preferred_element_type=F32,
                    )
                    dx[3 * t + k, pl.ds(SEG + c * GROUP, GROUP), :] = picked
                    wb[3 * t + k, pl.ds(c * GROUP, GROUP), :] = picked.astype(BF16)

    early = (g == 0) | (d == 0)

    @pl.when(early)
    def _():
        fluid_ready()
        local_work()

    pl.semaphore_wait(barrier, 8)
    recv = {}
    recv["rso"] = send(is_, rso, 2, (gm, d))
    recv["rsr"] = send(is_, rsr, 3, (gm, dm))
    recv["rsl"] = send(is_, rsl, 4, (gm, dp))

    @pl.when(jnp.logical_not(early))
    def _():
        fluid_ready()

    recv["rfr"] = send(ifl, rfr, 0, (g, dm))
    recv["rfl"] = send(ifr, rfl, 1, (g, dp))
    recv["sbr"] = send(sbv, sbr, 5, (g, dm))
    recv["sbl"] = send(sbv, sbl, 6, (g, dp))

    @pl.when(jnp.logical_not(early))
    def _():
        local_work()

    recv["wr"] = send(wb.at[:, pl.ds(0, 80)], wr, 7, (g, dm))
    recv["wl"] = send(wb.at[:, pl.ds(16, 80)], wl, 8, (g, dp))
    recv["bhrr"] = send(bhl, bhrr, 9, (g, dm), inner_left, inner_right)
    recv["bhlr"] = send(bhr, bhlr, 10, (g, dp), inner_right, inner_left)
    recv["shrr"] = send(shl, shrr, 11, (g, dm), inner_left, inner_right)
    recv["shlr"] = send(shr, shlr, 12, (g, dp), inner_right, inner_left)

    interior((None,) * 4, range(1, 4))

    at_end = (d == 0) | (d == n_dom - 1)
    mh_left = prepare(mhl, mhrr, 14, (g, dm), inner_left)
    mh_right = prepare(mhr, mhlr, 15, (g, dp), inner_right)
    recv["mhrr"] = lambda: pl.when(inner_right)(mh_left.wait_recv)
    recv["mhlr"] = lambda: pl.when(inner_left)(mh_right.wait_recv)

    def first_edges():
        recv["bhlr"]()
        recv["bhrr"]()
        for ref, first_row, film_at in ((bhlr, 1, 13), (bhrr, 36, 0)):
            films = to_f32(ref[pl.ds(7 * FY, 16), :])
            for i in range(4):
                row = (0, 36)[first_row == 36] + i
                p[pl.ds(row * FY, FY), :] = to_f32(ref[pl.ds(i * FY, FY), :])
            for i in range(3):
                row = first_row + i
                a[pl.ds(row * FY, FY), :] = to_f32(ref[pl.ds((4 + i) * FY, FY), :])
            for i in range(3):
                row = first_row + i
                r0, s0 = a[pl.ds(row * FY, 1), :], p[pl.ds(row * FY, 1), :]
                a0, b0, _ = film_coef(r0, s0, films[film_at + i : film_at + i + 1])
                coef(p, a, a, b, row * FY, FY)
                a[pl.ds(row * FY, 1), :] = a0
                b[pl.ds(row * FY, 1), :] = b0
        edges((None,) * 4)
        mhl[...] = p[pl.ds(4 * FY, 4 * FY), :].astype(BF16)
        mhr[...] = p[pl.ds(32 * FY, 4 * FY), :].astype(BF16)
        pl.when(inner_left)(mh_left.start)
        pl.when(inner_right)(mh_right.start)

    pl.when(at_end)(first_edges)

    recv["rfl"]()
    recv["rfr"]()
    for f, ref in ((0, xf0), (1, xr)):
        ref[pl.ds(64, 192), :] = to_f32(rfl[pl.ds(192 * f, 192), :])
        ref[pl.ds(512, 192), :] = to_f32(rfr[pl.ds(192 * f, 192), :])
    fxx[pl.ds(0, FX), :] = to_f32(rfl[pl.ds(384, FX), :])
    fxx[pl.ds(FX, FX), :] = fcv[...]
    fxx[pl.ds(2 * FX, FX), :] = to_f32(rfr[pl.ds(384, FX), :])
    rows_loop(1, 11, 2, lambda x: coef(xf0, xr, xa, xb, at_row(x, 64), 64))
    xc = []
    xb0 = []
    for par in range(2):
        rows = pl.ds(64 + par * 8, 40, stride=16)
        film = fxx[pl.ds(8 + par, 40, stride=2), :]
        a0, b0, c0 = film_coef(xr[rows, :], xf0[rows, :], film)
        xa[rows, :] = a0
        fin[par] = b0
        fin[2 + par] = c0
        xc.append(2 + par)
        xb0.append(par)

    for name in ("sbl", "sbr", "wl", "wr"):
        recv[name]()
    for k in range(6):
        dx[k, pl.ds(16, 80), :] = to_f32(wl[k])
        dx[k, pl.ds(192, 80), :] = to_f32(wr[k])
    for n, ref in enumerate((sbl, sbv, sbr)):
        row = jnp.concatenate([ref[...].astype(F32), jnp.zeros((1, FZ - SEG), F32)], axis=1)
        spread = jnp.broadcast_to(row, (FZ, FZ)).T
        xoff[pl.ds(n * SEG, SEG), :] = spread[:SEG].astype(jnp.int32)
    first = SX * (d + n_dom - 1) - 2
    zone = SX * n_dom
    half = lax.broadcasted_iota(jnp.int32, (40, FZ), 0) + (first + 4)
    for par in range(2):
        offs = [
            lax.rem(xoff[pl.ds(24 + 3 * par + j, 40, stride=6), :] - half + 3 * zone, zone)
            for j in range(3)
        ]
        for t in range(2):
            for k in range(3):
                diag = [dx[3 * t + k, pl.ds(24 + 3 * par + j, 40, stride=6), :] for j in range(3)]
                for o in range(5):
                    total = jnp.where(offs[0] == o, diag[0], 0.0)
                    total = total + jnp.where(offs[1] == o, diag[1], 0.0)
                    total = total + jnp.where(offs[2] == o, diag[2], 0.0)
                    at = (o * 3 + k) * 2 + par
                    if t == 0:
                        ww[at] = total
                    else:
                        vv[at] = total * fin[xc[par]]

    for name in ("rso", "rsr", "rsl"):
        recv[name]()
    for f, ref in ((0, xs0), (1, xsr)):
        for n, got in enumerate((rsl, rso, rsr)):
            ref[pl.ds(128 * n, 128), :] = to_f32(got[pl.ds(128 * f, 128), :])
    rows_loop(0, 6, 2, lambda x: coef(xs0, xsr, xsa, xsb, at_row(x, 64), 64))
    srows = pl.ds(32 + 7, 40, stride=8)
    film = jnp.concatenate([to_f32(got[pl.ds(256, SX), :]) for got in (rsl, rso, rsr)], axis=0)[4:44]
    a0, b0, c0 = film_coef(xsr[srows, :], xs0[srows, :], film)
    xsa[srows, :] = a0
    sin[0] = b0
    sin[1] = c0

    def shifts(v):
        return (v, pltpu.roll(v, 1, 1), pltpu.roll(v, FZ - 1, 1))

    def project_fluid(solid_ref, k):
        for n, v in enumerate(shifts(rounded(solid_ref[srows, :]))):
            pad[n, pl.ds(8, 40), :] = v
        for par in range(2):
            total = jnp.zeros((40, FZ), F32)
            for o in range(5):
                for n in range(3):
                    total = total + vv[(o * 3 + n) * 2 + par] * pad[n, pl.ds(6 + o, 40), :]
            fin[4 + 2 * k + par] = total

    def project_solid(fluid_ref, k):
        faces = [
            shifts(rounded(fluid_ref[pl.ds(64 + par * 8, 40, stride=16), :])) for par in range(2)
        ]
        for o in range(5):
            total = jnp.zeros((40, FZ), F32)
            for par in range(2):
                for n in range(3):
                    total = total + ww[(o * 3 + n) * 2 + par] * faces[par][n]
            tpad[o, pl.ds(8, 40), :] = total
        total = tpad[0, pl.ds(10, 40), :]
        for o in range(1, 5):
            total = total + tpad[o, pl.ds(10 - o, 40), :]
        sin[2 + k] = total
        sins[k] = total[4:36]

    def face_sweep(src, dst, a_ref, b_ref, width, lo, hi):
        count = hi - lo
        by_rolls = count - 2 * (count // 4)

        def beside(step, first):
            pieces, x = [], lo + step
            for cut, keep in ((width, keep_first), (2 * width, keep_last)):
                row = cut - 1 if first else cut
                if x < row:
                    pieces.append(src[pl.ds(x * 8, (row - x) * 8), :])
                pieces.append(src[pl.ds(row * 8, 8), :] * keep)
                x = row + 1
            if x < hi + step:
                pieces.append(src[pl.ds(x * 8, (hi + step - x) * 8), :])
            return jnp.concatenate(pieces, axis=0)

        cur = src[pl.ds(lo * 8, count * 8), :]
        sub = lax.broadcasted_iota(jnp.int32, (count * 8, FZ), 0) & 7
        above = jnp.where(sub == 0, 0.0, src[pl.ds(lo * 8 - 1, count * 8), :])
        below = jnp.where(sub == 7, 0.0, src[pl.ds(lo * 8 + 1, count * 8), :])
        along = jnp.concatenate(
            [zsum(cur[: by_rolls * 8]), zsum_by_product([cur[by_rolls * 8 :]], tt[...])], axis=0
        )
        summed = (beside(-1, True) + beside(1, False)) + (above + below) + along
        span = pl.ds(lo * 8, count * 8)
        dst[span, :] = b_ref[span, :] + a_ref[span, :] * summed

    keep_first, keep_last = ml, mr
    fluid_span = (((13, 83), (14, 82)), ((19, 77), (20, 76)), ((25, 71), (26, 70)))
    solid_span = (((6, 42), (7, 41)), ((9, 39), (10, 38)), ((12, 36), (13, 35)))
    fluid_refs = (xf0, xf0, xf2)
    fluid_out = (xf0, xf2, xf0)
    for k in range(4):
        fluid_ref = (xf0, xf0, xf2, xf0)[k]
        project_fluid(xs0, k)
        project_solid(fluid_ref, k)
        recv["sinr", k] = send(sins.at[k], sinr.at[k], (13, 16, 17, 18)[k], (gp, d))
        if k == 3:
            break
        for par in range(2):
            xb[pl.ds(64 + par * 8, 40, stride=16), :] = fin[xb0[par]] + fin[4 + 2 * k + par]
        xsb[srows, :] = sin[0] + sin[1] * sin[2 + k]
        for n in range(2):
            lo, hi = fluid_span[k][n]
            src, dst = (fluid_refs[k], xf1) if n == 0 else (xf1, fluid_out[k])
            face_sweep(src, dst, xa, xb, FX, lo, hi)
            lo, hi = solid_span[k][n]
            src, dst = (xs0, xs1) if n == 0 else (xs1, xs0)
            face_sweep(src, dst, xsa, xsb, SX, lo, hi)

    pl.when(jnp.logical_not(at_end))(first_edges)

    wide = lax.broadcasted_iota(jnp.int32, (20, FZ), 0)
    inside = jnp.where(wide < 2, ml, jnp.where(wide >= 18, mr, 1.0))
    for v in range(2):
        for i in range(1, 39):
            bt[pl.ds(v * 320 + i * 8, 8), :] = b[pl.ds(i * FY, 8), :]
        for par in range(2):
            rows = pl.ds(v * 320 + par * 8, 20, stride=16)
            bt[rows, :] = bt[rows, :] + fin[4 + 2 * (2 + v) + par][10:30] * inside

    def patch(i, mask):
        low = lax.broadcasted_iota(jnp.int32, (8, FZ), 0) < 4
        fresh = xf2[pl.ds((28 + i) * 8, 8), :]
        if mask is not None:
            fresh = fresh * mask
        p[pl.ds(i * FY, 8), :] = jnp.where(low, fresh, p[pl.ds(i * FY, 8), :])

    for i in range(4, 36):
        patch(i, None)
    second = (0, 0, 1, 1)
    interior(second)

    recv["shlr"]()
    recv["shrr"]()
    for f, ref in ((0, sp), (1, sa)):
        ref[pl.ds(0, 8 * SY), :] = to_f32(shlr[pl.ds(192 * f, 192), :])
        ref[pl.ds(24 * SY, 8 * SY), :] = to_f32(shrr[pl.ds(192 * f, 192), :])
    fsx[pl.ds(0, 8), :] = to_f32(shlr[pl.ds(384, SX), :])[8:]
    fsx[pl.ds(8, SX), :] = scv[...]
    fsx[pl.ds(24, 8), :] = to_f32(shrr[pl.ds(384, SX), :])[:8]
    last_rows = pl.ds(SY - 1, 32, stride=SY)
    a0, b0, c0 = film_coef(sa[last_rows, :], sp[last_rows, :], fsx[...])
    rows_loop(0, 8, 2, lambda x: coef(sp, sa, sa, sbb, at_row(x, 96), 96))
    sa[last_rows, :] = a0
    sbb[last_rows, :] = b0
    for k in range(4):
        for i in range(32):
            sbt[pl.ds(k * 256 + i * 8, 8), :] = sbb[pl.ds(i * SY + 16, 8), :]
    for k in range(4):
        recv["sinr", k]()
    for k in range(4):
        sbt[pl.ds(k * 256 + 7, 32, stride=8), :] = b0 + c0 * sinr[k]

    recv["mhlr"]()
    recv["mhrr"]()
    p[pl.ds(0, 4 * FY), :] = to_f32(mhlr[...])
    p[pl.ds(36 * FY, 4 * FY), :] = to_f32(mhrr[...])
    for i in range(4):
        patch(i, ml)
        patch(36 + i, mr)
    for copy, when in sends:
        if when is None:
            copy.wait_send()
        else:
            pl.when(when)(copy.wait_send)


def finish(p, q, a, b, bt, sp, sa, sbb, sbt, fo, so, rows, s1, s2, tt, sem):
    copies = [
        pltpu.make_async_copy(p.at[pl.ds(8 * FY, 24 * FY)], fo.at[pl.ds(4 * FY, 24 * FY)], sem.at[0])
    ]
    copies[0].start()
    band(tt)

    def solid_sweep(m):
        span = range(1 + m, 31 - m)
        src = sp if m == 0 else (s2, s1)[m % 2]
        dst = (s1, s2)[m % 2]

        def fixed(n, tile):
            if tile == 2:
                return sbt[pl.ds((m // 2) * 256 + span[n] * 8, 8), :]
            return sbb[pl.ds(span[n] * SY + 8 * tile, 8), :]

        sweep_rows(
            [[((src, (x - 1) * SY), (src, x * SY), (src, (x + 1) * SY), (dst, x * SY)) for x in span]],
            3, 1, tt[...], lambda n, tile: sa[pl.ds(span[n] * SY + 8 * tile, 8), :], fixed,
        )

    for m in range(4):
        groups, xs = [], []
        for side, x0 in ((0, 1 + m), (1, 35 - m)):
            def at(x, side=side):
                lo = (m, 36 - m)[side]
                if m and lo <= x < lo + 4:
                    return rows, ((m - 1) * 8 + side * 4 + x - lo) * FY
                return (p, q)[m % 2], x * FY

            groups.append(
                [
                    (at(x - 1), at(x), at(x + 1), (rows, (m * 8 + side * 4 + x - x0) * FY))
                    for x in range(x0, x0 + 4)
                ]
            )
            xs.extend(range(x0, x0 + 4))

        def fixed(n, tile):
            if tile == 0:
                return bt[pl.ds((m // 2) * 320 + xs[n] * 8, 8), :]
            return b[pl.ds(xs[n] * FY + 8 * tile, 8), :]

        sweep_rows(
            groups, 12, 6, tt[...], lambda n, tile: a[pl.ds(xs[n] * FY + 8 * tile, 8), :], fixed
        )
        solid_sweep(2 * m)
        solid_sweep(2 * m + 1)
    copies.append(pltpu.make_async_copy(s2.at[pl.ds(8 * SY, SX * SY)], so, sem.at[1]))
    copies[-1].start()
    for side, x in ((0, 0), (1, 28)):
        copies.append(
            pltpu.make_async_copy(
                rows.at[pl.ds((24 + 4 * side) * FY, 4 * FY)],
                fo.at[pl.ds(x * FY, 4 * FY)], sem.at[2 + side],
            )
        )
        copies[-1].start()
    for copy in copies:
        copy.wait()


def vm(*shape, dtype=F32):
    return pltpu.VMEM(shape, dtype)


SCRATCH = [
    vm(2 * SEG * FZ, FZ, dtype=BF16),
    *(vm(96 * 8, FZ) for _ in range(6)), *(vm(48 * 8, FZ) for _ in range(5)),
    vm(6, 3 * SEG, FZ), vm(30, 40, FZ), vm(30, 40, FZ), vm(3, 64, FZ), vm(5, 64, FZ),
    vm(12, 40, FZ), vm(6, 40, FZ), vm(4, 32, FZ), vm(96, FZ), vm(32, FZ),
    vm(3 * SEG, FZ, dtype=jnp.int32),
    vm(FX, FZ), vm(SX, FZ), vm(1, SEG, dtype=jnp.int32), vm(2 * FZ, FZ, dtype=BF16),
    vm(416, FZ, dtype=BF16), vm(416, FZ, dtype=BF16), vm(272, FZ, dtype=BF16),
    vm(6, SEG, FZ, dtype=BF16), vm(7 * FY + 16, FZ, dtype=BF16), vm(7 * FY + 16, FZ, dtype=BF16),
    vm(400, FZ, dtype=BF16), vm(400, FZ, dtype=BF16),
    vm(4 * FY, FZ, dtype=BF16), vm(4 * FY, FZ, dtype=BF16),
    vm(416, FZ, dtype=BF16), vm(416, FZ, dtype=BF16),
    vm(1, SEG, dtype=jnp.int32), vm(1, SEG, dtype=jnp.int32),
    *(vm(272, FZ, dtype=BF16) for _ in range(3)),
    vm(6, 80, FZ, dtype=BF16), vm(6, 80, FZ, dtype=BF16),
    vm(7 * FY + 16, FZ, dtype=BF16), vm(7 * FY + 16, FZ, dtype=BF16),
    vm(400, FZ, dtype=BF16), vm(400, FZ, dtype=BF16),
    vm(4 * FY, FZ, dtype=BF16), vm(4 * FY, FZ, dtype=BF16), vm(4, 32, FZ),
    pltpu.SemaphoreType.DMA((9,)), pltpu.SemaphoreType.DMA((19,)), pltpu.SemaphoreType.DMA((19,)),
]


STATE = (
    *(vm(40 * FY, FZ) for _ in range(4)), vm(2 * 320, FZ),
    *(vm(32 * SY, FZ) for _ in range(3)), vm(4 * 256, FZ),
)


def solution(mesh):
    n_grp, n_dom = mesh.shape["grp"], mesh.shape["dom"]

    def local(fs, fr, fc, ss, sr, sc, sb, ts, tf):
        state = pl.pallas_call(
            lambda *refs: kernel(n_grp, n_dom, *refs),
            out_shape=STATE,
            in_specs=[pl.BlockSpec(memory_space=pltpu.HBM)] * 9,
            out_specs=tuple(pl.BlockSpec(memory_space=pltpu.VMEM) for _ in STATE),
            scratch_shapes=SCRATCH,
            compiler_params=pltpu.CompilerParams(
                collective_id=0, has_side_effects=True, vmem_limit_bytes=57_147_392
            ),
            name="coupled",
        )(
            fs.reshape(FX * FY, FZ), fr.reshape(FX * FY, FZ), fc.reshape(FX, FZ),
            ss.reshape(SX * SY, FZ), sr.reshape(SX * SY, FZ), sc.reshape(SX, FZ),
            sb.reshape(1, SEG),
            ts.reshape(SEG * FZ, FZ), tf.reshape(SEG * FZ, FZ),
        )
        fo, so = pl.pallas_call(
            finish,
            out_shape=(
                jax.ShapeDtypeStruct((FX * FY, FZ), F32),
                jax.ShapeDtypeStruct((SX * SY, FZ), F32),
            ),
            in_specs=[pl.BlockSpec(memory_space=pltpu.VMEM)] * 9,
            out_specs=[pl.BlockSpec(memory_space=pltpu.HBM)] * 2,
            scratch_shapes=[
                vm(32 * FY, FZ), vm(32 * SY, FZ), vm(32 * SY, FZ), vm(2 * FZ, FZ, dtype=BF16),
                pltpu.SemaphoreType.DMA((4,)),
            ],
            compiler_params=pltpu.CompilerParams(vmem_limit_bytes=16 * 1024 * 1024),
            name="finish",
        )(*state)
        return fo.reshape(1, FX, FY, FZ), so.reshape(1, SX, SY, FZ)

    cells = P("grp", "dom", None, None)
    faces = P("grp", "dom", None)
    split = P(("grp", "dom"))
    mats = P(("grp", "dom"), None, None)
    return jax.shard_map(
        local,
        mesh=mesh,
        in_specs=(cells, cells, faces, cells, cells, faces, split, mats, mats),
        out_specs=(cells, cells),
        check_vma=False,
    )
```

```python
import jax
import jax.numpy as jnp
from jax import lax
from jax.experimental import pallas as pl
from jax.experimental.pallas import tpu as pltpu
from jax.sharding import PartitionSpec as P

MESH = pl.DeviceIdType.MESH
F32 = jnp.float32
BF16 = jnp.bfloat16
FX, FY, FZ = 32, 96, 128
SX, SY = 16, 24
SEG = 96
GROUP = 16


def lane_iota(shape):
    return lax.broadcasted_iota(jnp.int32, shape, 1)


def zsum(v):
    lane = lane_iota(v.shape)
    return jnp.where(lane == 0, 0.0, pltpu.roll(v, 1, 1)) + jnp.where(
        lane == FZ - 1, 0.0, pltpu.roll(v, FZ - 1, 1)
    )


def split_terms(v):
    head = v.astype(BF16)
    return jnp.concatenate([head, (v - head.astype(F32)).astype(BF16)], axis=1)


def band(tt):
    apart = (lax.broadcasted_iota(jnp.int32, (2 * FZ, FZ), 0) & (FZ - 1)) - lane_iota((2 * FZ, FZ))
    tt[...] = jnp.where((apart == 1) | (apart == -1), 1.0, 0.0).astype(BF16)


def zsum_by_product(values, tt):
    return jnp.dot(
        jnp.concatenate([split_terms(v) for v in values], axis=0), tt, preferred_element_type=F32
    )


def ysum(v):
    zero = jnp.zeros((1, FZ), F32)
    return jnp.concatenate([zero, v[:-1]], axis=0) + jnp.concatenate([v[1:], zero], axis=0)


def rows_loop(lo, hi, unroll, body):
    count = hi - lo
    groups = count // unroll if count > unroll else 0
    if groups:

        def step(i, carry):
            for j in range(unroll):
                body(lo + i * unroll + j)
            return carry

        lax.fori_loop(0, groups, step, 0)
    for x in range(lo + groups * unroll, hi):
        body(x)


def at_row(x, pitch):
    return x * pitch if isinstance(x, int) else pl.multiple_of(x * pitch, 8)


def sweep_rows(groups, tiles, rolled, tt, coef_a, fixed, loaded=(1, 2, 4, 5, 6, 7, 9, 10)):
    products = []
    for group in groups:
        halves = [group[: len(group) // 2], group[len(group) // 2 :]]
        for part in halves if len(group) > 1 and tiles > rolled else [group]:
            if tiles == rolled:
                products.extend([None] * len(part))
                continue
            height = 8 * (tiles - rolled)
            total = zsum_by_product(
                [ref[pl.ds(at + 8 * rolled, height), :] for _, (ref, at), _, _ in part], tt
            )
            products.extend(total[n * height : (n + 1) * height] for n in range(len(part)))
    held = {}

    def cell(number, row, tile):
        key = number, row, tile
        if key not in held:
            group = groups[number]
            if row < 0:
                ref, at = group[0][0]
            elif row == len(group):
                ref, at = group[-1][2]
            else:
                ref, at = group[row][1]
            held[key] = ref[pl.ds(at + 8 * tile, 8), :]
        return held[key]

    zero = jnp.zeros((1, FZ), F32)
    for tile in range(tiles):
        n = 0
        for number, group in enumerate(groups):
            for row, (_, (ref, at), _, target) in enumerate(group):
                here = at + 8 * tile
                cur = cell(number, row, tile)
                beside = cell(number, row - 1, tile) + cell(number, row + 1, tile)
                if tile in loaded and tile < tiles - 1:
                    across = ref[pl.ds(here - 1, 8), :] + ref[pl.ds(here + 1, 8), :]
                else:
                    low = zero if tile == 0 else cell(number, row, tile - 1)[7:]
                    high = zero if tile == tiles - 1 else cell(number, row, tile + 1)[:1]
                    across = jnp.concatenate([low, cur[:-1]], axis=0)
                    across = across + jnp.concatenate([cur[1:], high], axis=0)
                summed = beside + across
                if tile < rolled:
                    summed = summed + zsum(cur)
                else:
                    summed = summed + products[n][8 * (tile - rolled) : 8 * (tile - rolled + 1)]
                target[0][pl.ds(target[1] + 8 * tile, 8), :] = (
                    fixed(n, tile) + coef_a(n, tile) * summed
                )
                n += 1


def to_f32(v):
    return v.astype(F32)


def rounded(v):
    return v.astype(BF16).astype(F32)


def kernel(
    n_grp, n_dom,
    fs, fr, fc, ss, sr, sc, sb, ts, tf,
    p, q, a, b, bt, sp, sa, sbb, sbt,
    mt, xf0, xf1, xf2, xr, xa, xb, xs0, xs1, xsr, xsa, xsb,
    dx, vv, ww, pad, tpad, fin, sin, sins, fxx, fsx, xoff,
    fcv, scv, sbv, tt,
    ifl, ifr, is_, wb, bhl, bhr, shl, shr, mhl, mhr,
    rfl, rfr, sbl, sbr, rso, rsr, rsl,
    wr, wl, bhrr, bhlr, shrr, shlr, mhrr, mhlr, sinr,
    load_sem, send_sem, recv_sem,
):
    g = lax.axis_index("grp")
    d = lax.axis_index("dom")
    gm, gp = lax.rem(g + n_grp - 1, n_grp), lax.rem(g + 1, n_grp)
    dm, dp = lax.rem(d + n_dom - 1, n_dom), lax.rem(d + 1, n_dom)
    ml = jnp.where(d > 0, 1.0, 0.0).astype(F32)
    mr = jnp.where(d < n_dom - 1, 1.0, 0.0).astype(F32)

    barrier = pltpu.get_barrier_semaphore()
    peers = ((g, dm), (g, dp), (gm, d), (gp, d), (gm, dm), (gm, dp), (gp, dm), (gp, dp))
    for peer in peers:
        pl.semaphore_signal(barrier, inc=1, device_id=peer, device_id_type=MESH)

    loads = {}

    def load(name, src, dst, index):
        loads[name] = pltpu.make_async_copy(src, dst, load_sem.at[index])
        loads[name].start()

    load("ss", ss, sp.at[pl.ds(8 * SY, SX * SY)], 0)
    load("sr", sr, sa.at[pl.ds(8 * SY, SX * SY)], 1)
    load("sc", sc, scv, 4)
    load("fc", fc, fcv, 5)
    load("sb", sb, sbv, 6)
    load("fs", fs, p.at[pl.ds(4 * FY, FX * FY)], 2)
    load("fr", fr, a.at[pl.ds(4 * FY, FX * FY)], 3)
    for t, src in ((0, ts), (1, tf)):
        load(("m", t), src, mt.at[pl.ds(t * SEG * FZ, SEG * FZ)], 7 + t)

    sends = []
    inner_left, inner_right = d > 0, d < n_dom - 1
    band(tt)

    def prepare(src, dst, index, peer, when=None):
        copy = pltpu.make_async_remote_copy(
            src_ref=src, dst_ref=dst, send_sem=send_sem.at[index], recv_sem=recv_sem.at[index],
            device_id=peer, device_id_type=MESH,
        )
        sends.append((copy, when))
        return copy

    def send(src, dst, index, peer, when=None, got=None):
        copy = prepare(src, dst, index, peer, when)
        if when is None:
            copy.start()
        else:
            pl.when(when)(copy.start)
        return copy.wait_recv if got is None else lambda: pl.when(got)(copy.wait_recv)

    @pl.when(d == 0)
    def _():
        for ref in (bhlr, shlr, mhlr):
            ref[...] = jnp.zeros(ref.shape, BF16)

    @pl.when(d == n_dom - 1)
    def _():
        for ref in (bhrr, shrr, mhrr):
            ref[...] = jnp.zeros(ref.shape, BF16)

    loads["ss"].wait()
    loads["sr"].wait()
    loads["sc"].wait()
    for f, ref in ((0, sp), (1, sa)):
        for i in range(SX // 2):
            lo = (8 + 2 * i) * SY + 16
            is_[pl.ds(128 * f + 16 * i, 16), :] = jnp.concatenate(
                [ref[pl.ds(lo, 8), :], ref[pl.ds(lo + SY, 8), :]], axis=0
            ).astype(BF16)
        shl[pl.ds(192 * f, 192), :] = ref[pl.ds(8 * SY, 8 * SY), :].astype(BF16)
        shr[pl.ds(192 * f, 192), :] = ref[pl.ds(16 * SY, 8 * SY), :].astype(BF16)
    is_[pl.ds(256, SX), :] = scv[...].astype(BF16)
    shl[pl.ds(384, SX), :] = scv[...].astype(BF16)
    shr[pl.ds(384, SX), :] = scv[...].astype(BF16)

    def fluid_ready():
        loads["fs"].wait()
        loads["fr"].wait()
        loads["fc"].wait()
        loads["sb"].wait()
        for f, ref in ((0, p), (1, a)):
            for i in range(FX // 2):
                lo = (4 + 2 * i) * FY
                pair = jnp.concatenate([ref[pl.ds(lo, 8), :], ref[pl.ds(lo + FY, 8), :]], axis=0)
                if i < 12:
                    ifl[pl.ds(192 * f + 16 * i, 16), :] = pair.astype(BF16)
                if i >= 4:
                    ifr[pl.ds(192 * f + 16 * (i - 4), 16), :] = pair.astype(BF16)
                own = xf0 if f == 0 else xr
                own[pl.ds((FX + 2 * i) * 8, 16), :] = pair
        for ref in (ifl, ifr):
            ref[pl.ds(384, FX), :] = fcv[...].astype(BF16)
        for i in range(4):
            bhl[pl.ds(i * FY, FY), :] = p[pl.ds((4 + i) * FY, FY), :].astype(BF16)
            bhr[pl.ds(i * FY, FY), :] = p[pl.ds((32 + i) * FY, FY), :].astype(BF16)
        for i in range(3):
            bhl[pl.ds((4 + i) * FY, FY), :] = a[pl.ds((4 + i) * FY, FY), :].astype(BF16)
            bhr[pl.ds((4 + i) * FY, FY), :] = a[pl.ds((33 + i) * FY, FY), :].astype(BF16)
        bhl[pl.ds(7 * FY, 16), :] = fcv[pl.ds(0, 16), :].astype(BF16)
        bhr[pl.ds(7 * FY, 16), :] = fcv[pl.ds(16, 16), :].astype(BF16)

    def coef(start_ref, rate_ref, a_ref, b_ref, lo, size):
        r = rate_ref[pl.ds(lo, size), :]
        inv = 1.0 / (1.0 + 6.0 * r)
        b_ref[pl.ds(lo, size), :] = start_ref[pl.ds(lo, size), :] * inv
        a_ref[pl.ds(lo, size), :] = r * inv

    def film_coef(r0, s0, film):
        inv0 = 1.0 / (1.0 + 6.0 * r0 + film)
        return r0 * inv0, s0 * inv0, film * inv0

    def fluid_sweep(src, dst, variant, spans):
        groups, bases, rows = [], [], []
        for x0, count in spans:
            group = []
            for n in range(count):
                base = x0 * FY + n * FY if isinstance(x0, int) else pl.multiple_of(x0 * FY, 8) + n * FY
                bases.append(base)
                rows.append(x0 + n)
                group.append(((src, base - FY), (src, base), (src, base + FY), (dst, base)))
            groups.append(group)

        def fixed(n, tile):
            if tile == 0 and variant is not None:
                return bt[pl.ds(variant * 320 + at_row(rows[n], 8), 8), :]
            return b[pl.ds(bases[n] + 8 * tile, 8), :]

        sweep_rows(
            groups, 12, 6, tt[...], lambda n, tile: a[pl.ds(bases[n] + 8 * tile, 8), :], fixed
        )

    def interior(variants, sweeps=range(4)):
        for m in sweeps:
            block = (10, 7, 13, 8)[m]
            src, dst = (p, q) if m % 2 == 0 else (q, p)

            def step(i, carry):
                fluid_sweep(src, dst, variants[m], ((5 + m + i * block, block),))
                return carry

            lax.fori_loop(0, (30 - 2 * m) // block, step, 0)

    def edges(variants):
        for m in range(4):
            src, dst = (p, q) if m % 2 == 0 else (q, p)
            fluid_sweep(src, dst, variants[m], ((1 + m, 4), (35 - m, 4)))

    def local_work():
        own_rows = pl.ds(4 * FY, FX, stride=FY)
        a0, b0, _ = film_coef(a[own_rows, :], p[own_rows, :], fcv[...])
        rows_loop(4, 36, 4, lambda x: coef(p, a, a, b, at_row(x, FY), FY))
        a[own_rows, :] = a0
        b[own_rows, :] = b0
        interior((None,) * 4, range(1))
        folded_row = lax.broadcasted_iota(jnp.int32, (16, FZ), 0)
        folded_col = lane_iota((16, FZ))
        masks = [
            jnp.where(((folded_col + shift) & 15) == folded_row, 1.0, 0.0).astype(BF16)
            for shift in (0, 15, 1)
        ]
        owner = lax.broadcasted_iota(jnp.int32, (GROUP, GROUP * 16), 1) // 16
        gather = jnp.where(
            owner == lax.broadcasted_iota(jnp.int32, (GROUP, GROUP * 16), 0), 1.0, 0.0
        ).astype(BF16)
        for t in range(2):
            loads[("m", t)].wait()
            for c in range(SEG // GROUP):
                folded = []
                for n in range(GROUP):
                    at = (t * SEG + c * GROUP + n) * FZ
                    parts = [mt[pl.ds(at + 16 * r, 16), :] for r in range(8)]
                    while len(parts) > 1:
                        parts = [u + v for u, v in zip(parts[::2], parts[1::2])]
                    folded.append(parts[0])
                for k in range(3):
                    picked = jnp.dot(
                        gather, jnp.concatenate([f * masks[k] for f in folded], axis=0),
                        preferred_element_type=F32,
                    )
                    dx[3 * t + k, pl.ds(SEG + c * GROUP, GROUP), :] = picked
                    wb[3 * t + k, pl.ds(c * GROUP, GROUP), :] = picked.astype(BF16)

    early = (g == 0) | (d == 0)

    @pl.when(early)
    def _():
        fluid_ready()
        local_work()

    pl.semaphore_wait(barrier, 8)
    recv = {}
    recv["rso"] = send(is_, rso, 2, (gm, d))
    recv["rsr"] = send(is_, rsr, 3, (gm, dm))
    recv["rsl"] = send(is_, rsl, 4, (gm, dp))

    @pl.when(jnp.logical_not(early))
    def _():
        fluid_ready()

    recv["rfr"] = send(ifl, rfr, 0, (g, dm))
    recv["rfl"] = send(ifr, rfl, 1, (g, dp))
    recv["sbr"] = send(sbv, sbr, 5, (g, dm))
    recv["sbl"] = send(sbv, sbl, 6, (g, dp))

    @pl.when(jnp.logical_not(early))
    def _():
        local_work()

    recv["wr"] = send(wb.at[:, pl.ds(0, 80)], wr, 7, (g, dm))
    recv["wl"] = send(wb.at[:, pl.ds(16, 80)], wl, 8, (g, dp))
    recv["bhrr"] = send(bhl, bhrr, 9, (g, dm), inner_left, inner_right)
    recv["bhlr"] = send(bhr, bhlr, 10, (g, dp), inner_right, inner_left)
    recv["shrr"] = send(shl, shrr, 11, (g, dm), inner_left, inner_right)
    recv["shlr"] = send(shr, shlr, 12, (g, dp), inner_right, inner_left)

    interior((None,) * 4, range(1, 4))

    at_end = (d == 0) | (d == n_dom - 1)
    mh_left = prepare(mhl, mhrr, 14, (g, dm), inner_left)
    mh_right = prepare(mhr, mhlr, 15, (g, dp), inner_right)
    recv["mhrr"] = lambda: pl.when(inner_right)(mh_left.wait_recv)
    recv["mhlr"] = lambda: pl.when(inner_left)(mh_right.wait_recv)

    def first_edges():
        recv["bhlr"]()
        recv["bhrr"]()
        for ref, first_row, film_at in ((bhlr, 1, 13), (bhrr, 36, 0)):
            films = to_f32(ref[pl.ds(7 * FY, 16), :])
            for i in range(4):
                row = (0, 36)[first_row == 36] + i
                p[pl.ds(row * FY, FY), :] = to_f32(ref[pl.ds(i * FY, FY), :])
            for i in range(3):
                row = first_row + i
                a[pl.ds(row * FY, FY), :] = to_f32(ref[pl.ds((4 + i) * FY, FY), :])
            for i in range(3):
                row = first_row + i
                r0, s0 = a[pl.ds(row * FY, 1), :], p[pl.ds(row * FY, 1), :]
                a0, b0, _ = film_coef(r0, s0, films[film_at + i : film_at + i + 1])
                coef(p, a, a, b, row * FY, FY)
                a[pl.ds(row * FY, 1), :] = a0
                b[pl.ds(row * FY, 1), :] = b0
        edges((None,) * 4)
        mhl[...] = p[pl.ds(4 * FY, 4 * FY), :].astype(BF16)
        mhr[...] = p[pl.ds(32 * FY, 4 * FY), :].astype(BF16)
        pl.when(inner_left)(mh_left.start)
        pl.when(inner_right)(mh_right.start)

    pl.when(at_end)(first_edges)

    recv["rfl"]()
    recv["rfr"]()
    for f, ref in ((0, xf0), (1, xr)):
        ref[pl.ds(64, 192), :] = to_f32(rfl[pl.ds(192 * f, 192), :])
        ref[pl.ds(512, 192), :] = to_f32(rfr[pl.ds(192 * f, 192), :])
    fxx[pl.ds(0, FX), :] = to_f32(rfl[pl.ds(384, FX), :])
    fxx[pl.ds(FX, FX), :] = fcv[...]
    fxx[pl.ds(2 * FX, FX), :] = to_f32(rfr[pl.ds(384, FX), :])
    rows_loop(1, 11, 2, lambda x: coef(xf0, xr, xa, xb, at_row(x, 64), 64))
    xc = []
    xb0 = []
    for par in range(2):
        rows = pl.ds(64 + par * 8, 40, stride=16)
        film = fxx[pl.ds(8 + par, 40, stride=2), :]
        a0, b0, c0 = film_coef(xr[rows, :], xf0[rows, :], film)
        xa[rows, :] = a0
        fin[par] = b0
        fin[2 + par] = c0
        xc.append(2 + par)
        xb0.append(par)

    for name in ("sbl", "sbr", "wl", "wr"):
        recv[name]()
    for k in range(6):
        dx[k, pl.ds(16, 80), :] = to_f32(wl[k])
        dx[k, pl.ds(192, 80), :] = to_f32(wr[k])
    for n, ref in enumerate((sbl, sbv, sbr)):
        row = jnp.concatenate([ref[...].astype(F32), jnp.zeros((1, FZ - SEG), F32)], axis=1)
        spread = jnp.broadcast_to(row, (FZ, FZ)).T
        xoff[pl.ds(n * SEG, SEG), :] = spread[:SEG].astype(jnp.int32)
    first = SX * (d + n_dom - 1) - 2
    zone = SX * n_dom
    half = lax.broadcasted_iota(jnp.int32, (40, FZ), 0) + (first + 4)
    for par in range(2):
        offs = [
            lax.rem(xoff[pl.ds(24 + 3 * par + j, 40, stride=6), :] - half + 3 * zone, zone)
            for j in range(3)
        ]
        for t in range(2):
            for k in range(3):
                diag = [dx[3 * t + k, pl.ds(24 + 3 * par + j, 40, stride=6), :] for j in range(3)]
                for o in range(5):
                    total = jnp.where(offs[0] == o, diag[0], 0.0)
                    total = total + jnp.where(offs[1] == o, diag[1], 0.0)
                    total = total + jnp.where(offs[2] == o, diag[2], 0.0)
                    at = (o * 3 + k) * 2 + par
                    if t == 0:
                        ww[at] = total
                    else:
                        vv[at] = total * fin[xc[par]]

    for name in ("rso", "rsr", "rsl"):
        recv[name]()
    for f, ref in ((0, xs0), (1, xsr)):
        for n, got in enumerate((rsl, rso, rsr)):
            ref[pl.ds(128 * n, 128), :] = to_f32(got[pl.ds(128 * f, 128), :])
    rows_loop(0, 6, 2, lambda x: coef(xs0, xsr, xsa, xsb, at_row(x, 64), 64))
    srows = pl.ds(32 + 7, 40, stride=8)
    film = jnp.concatenate([to_f32(got[pl.ds(256, SX), :]) for got in (rsl, rso, rsr)], axis=0)[4:44]
    a0, b0, c0 = film_coef(xsr[srows, :], xs0[srows, :], film)
    xsa[srows, :] = a0
    sin[0] = b0
    sin[1] = c0

    def shifts(v):
        return (v, pltpu.roll(v, 1, 1), pltpu.roll(v, FZ - 1, 1))

    def project_fluid(solid_ref, k):
        for n, v in enumerate(shifts(rounded(solid_ref[srows, :]))):
            pad[n, pl.ds(8, 40), :] = v
        for par in range(2):
            total = jnp.zeros((40, FZ), F32)
            for o in range(5):
                for n in range(3):
                    total = total + vv[(o * 3 + n) * 2 + par] * pad[n, pl.ds(6 + o, 40), :]
            fin[4 + 2 * k + par] = total

    def project_solid(fluid_ref, k):
        faces = [
            shifts(rounded(fluid_ref[pl.ds(64 + par * 8, 40, stride=16), :])) for par in range(2)
        ]
        for o in range(5):
            total = jnp.zeros((40, FZ), F32)
            for par in range(2):
                for n in range(3):
                    total = total + ww[(o * 3 + n) * 2 + par] * faces[par][n]
            tpad[o, pl.ds(8, 40), :] = total
        total = tpad[0, pl.ds(10, 40), :]
        for o in range(1, 5):
            total = total + tpad[o, pl.ds(10 - o, 40), :]
        sin[2 + k] = total
        sins[k] = total[4:36]

    def face_sweep(src, dst, a_ref, b_ref, width, lo, hi):
        count = hi - lo
        by_rolls = count - 2 * (count // 4)

        def beside(step, first):
            pieces, x = [], lo + step
            for cut, keep in ((width, keep_first), (2 * width, keep_last)):
                row = cut - 1 if first else cut
                if x < row:
                    pieces.append(src[pl.ds(x * 8, (row - x) * 8), :])
                pieces.append(src[pl.ds(row * 8, 8), :] * keep)
                x = row + 1
            if x < hi + step:
                pieces.append(src[pl.ds(x * 8, (hi + step - x) * 8), :])
            return jnp.concatenate(pieces, axis=0)

        cur = src[pl.ds(lo * 8, count * 8), :]
        sub = lax.broadcasted_iota(jnp.int32, (count * 8, FZ), 0) & 7
        above = jnp.where(sub == 0, 0.0, src[pl.ds(lo * 8 - 1, count * 8), :])
        below = jnp.where(sub == 7, 0.0, src[pl.ds(lo * 8 + 1, count * 8), :])
        along = jnp.concatenate(
            [zsum(cur[: by_rolls * 8]), zsum_by_product([cur[by_rolls * 8 :]], tt[...])], axis=0
        )
        summed = (beside(-1, True) + beside(1, False)) + (above + below) + along
        span = pl.ds(lo * 8, count * 8)
        dst[span, :] = b_ref[span, :] + a_ref[span, :] * summed

    keep_first, keep_last = ml, mr
    fluid_span = (((13, 83), (14, 82)), ((19, 77), (20, 76)), ((25, 71), (26, 70)))
    solid_span = (((6, 42), (7, 41)), ((9, 39), (10, 38)), ((12, 36), (13, 35)))
    fluid_refs = (xf0, xf0, xf2)
    fluid_out = (xf0, xf2, xf0)
    for k in range(4):
        fluid_ref = (xf0, xf0, xf2, xf0)[k]
        project_fluid(xs0, k)
        project_solid(fluid_ref, k)
        recv["sinr", k] = send(sins.at[k], sinr.at[k], (13, 16, 17, 18)[k], (gp, d))
        if k == 3:
            break
        for par in range(2):
            xb[pl.ds(64 + par * 8, 40, stride=16), :] = fin[xb0[par]] + fin[4 + 2 * k + par]
        xsb[srows, :] = sin[0] + sin[1] * sin[2 + k]
        for n in range(2):
            lo, hi = fluid_span[k][n]
            src, dst = (fluid_refs[k], xf1) if n == 0 else (xf1, fluid_out[k])
            face_sweep(src, dst, xa, xb, FX, lo, hi)
            lo, hi = solid_span[k][n]
            src, dst = (xs0, xs1) if n == 0 else (xs1, xs0)
            face_sweep(src, dst, xsa, xsb, SX, lo, hi)

    pl.when(jnp.logical_not(at_end))(first_edges)

    wide = lax.broadcasted_iota(jnp.int32, (20, FZ), 0)
    inside = jnp.where(wide < 2, ml, jnp.where(wide >= 18, mr, 1.0))
    for v in range(2):
        for i in range(1, 39):
            bt[pl.ds(v * 320 + i * 8, 8), :] = b[pl.ds(i * FY, 8), :]
        for par in range(2):
            rows = pl.ds(v * 320 + par * 8, 20, stride=16)
            bt[rows, :] = bt[rows, :] + fin[4 + 2 * (2 + v) + par][10:30] * inside

    def patch(i, mask):
        low = lax.broadcasted_iota(jnp.int32, (8, FZ), 0) < 4
        fresh = xf2[pl.ds((28 + i) * 8, 8), :]
        if mask is not None:
            fresh = fresh * mask
        p[pl.ds(i * FY, 8), :] = jnp.where(low, fresh, p[pl.ds(i * FY, 8), :])

    for i in range(4, 36):
        patch(i, None)
    second = (0, 0, 1, 1)
    interior(second)

    recv["shlr"]()
    recv["shrr"]()
    for f, ref in ((0, sp), (1, sa)):
        ref[pl.ds(0, 8 * SY), :] = to_f32(shlr[pl.ds(192 * f, 192), :])
        ref[pl.ds(24 * SY, 8 * SY), :] = to_f32(shrr[pl.ds(192 * f, 192), :])
    fsx[pl.ds(0, 8), :] = to_f32(shlr[pl.ds(384, SX), :])[8:]
    fsx[pl.ds(8, SX), :] = scv[...]
    fsx[pl.ds(24, 8), :] = to_f32(shrr[pl.ds(384, SX), :])[:8]
    last_rows = pl.ds(SY - 1, 32, stride=SY)
    a0, b0, c0 = film_coef(sa[last_rows, :], sp[last_rows, :], fsx[...])
    rows_loop(0, 8, 2, lambda x: coef(sp, sa, sa, sbb, at_row(x, 96), 96))
    sa[last_rows, :] = a0
    sbb[last_rows, :] = b0
    for k in range(4):
        for i in range(32):
            sbt[pl.ds(k * 256 + i * 8, 8), :] = sbb[pl.ds(i * SY + 16, 8), :]
    for k in range(4):
        recv["sinr", k]()
    for k in range(4):
        sbt[pl.ds(k * 256 + 7, 32, stride=8), :] = b0 + c0 * sinr[k]

    recv["mhlr"]()
    recv["mhrr"]()
    p[pl.ds(0, 4 * FY), :] = to_f32(mhlr[...])
    p[pl.ds(36 * FY, 4 * FY), :] = to_f32(mhrr[...])
    for i in range(4):
        patch(i, ml)
        patch(36 + i, mr)
    for copy, when in sends:
        if when is None:
            copy.wait_send()
        else:
            pl.when(when)(copy.wait_send)


def finish(p, q, a, b, bt, sp, sa, sbb, sbt, fo, so, rows, s1, s2, tt, sem):
    copies = [
        pltpu.make_async_copy(p.at[pl.ds(8 * FY, 24 * FY)], fo.at[pl.ds(4 * FY, 24 * FY)], sem.at[0])
    ]
    copies[0].start()
    band(tt)

    def solid_sweep(m):
        span = range(1 + m, 31 - m)
        src = sp if m == 0 else (s2, s1)[m % 2]
        dst = (s1, s2)[m % 2]

        def fixed(n, tile):
            if tile == 2:
                return sbt[pl.ds((m // 2) * 256 + span[n] * 8, 8), :]
            return sbb[pl.ds(span[n] * SY + 8 * tile, 8), :]

        sweep_rows(
            [[((src, (x - 1) * SY), (src, x * SY), (src, (x + 1) * SY), (dst, x * SY)) for x in span]],
            3, 1, tt[...], lambda n, tile: sa[pl.ds(span[n] * SY + 8 * tile, 8), :], fixed,
        )

    for m in range(4):
        groups, xs = [], []
        for side, x0 in ((0, 1 + m), (1, 35 - m)):
            def at(x, side=side):
                lo = (m, 36 - m)[side]
                if m and lo <= x < lo + 4:
                    return rows, ((m - 1) * 8 + side * 4 + x - lo) * FY
                return (p, q)[m % 2], x * FY

            groups.append(
                [
                    (at(x - 1), at(x), at(x + 1), (rows, (m * 8 + side * 4 + x - x0) * FY))
                    for x in range(x0, x0 + 4)
                ]
            )
            xs.extend(range(x0, x0 + 4))

        def fixed(n, tile):
            if tile == 0:
                return bt[pl.ds((m // 2) * 320 + xs[n] * 8, 8), :]
            return b[pl.ds(xs[n] * FY + 8 * tile, 8), :]

        sweep_rows(
            groups, 12, 6, tt[...], lambda n, tile: a[pl.ds(xs[n] * FY + 8 * tile, 8), :], fixed
        )
        solid_sweep(2 * m)
        solid_sweep(2 * m + 1)
    copies.append(pltpu.make_async_copy(s2.at[pl.ds(8 * SY, SX * SY)], so, sem.at[1]))
    copies[-1].start()
    for side, x in ((0, 0), (1, 28)):
        copies.append(
            pltpu.make_async_copy(
                rows.at[pl.ds((24 + 4 * side) * FY, 4 * FY)],
                fo.at[pl.ds(x * FY, 4 * FY)], sem.at[2 + side],
            )
        )
        copies[-1].start()
    for copy in copies:
        copy.wait()


def vm(*shape, dtype=F32):
    return pltpu.VMEM(shape, dtype)


SCRATCH = [
    vm(2 * SEG * FZ, FZ, dtype=BF16),
    *(vm(96 * 8, FZ) for _ in range(6)), *(vm(48 * 8, FZ) for _ in range(5)),
    vm(6, 3 * SEG, FZ), vm(30, 40, FZ), vm(30, 40, FZ), vm(3, 64, FZ), vm(5, 64, FZ),
    vm(12, 40, FZ), vm(6, 40, FZ), vm(4, 32, FZ), vm(96, FZ), vm(32, FZ),
    vm(3 * SEG, FZ, dtype=jnp.int32),
    vm(FX, FZ), vm(SX, FZ), vm(1, SEG, dtype=jnp.int32), vm(2 * FZ, FZ, dtype=BF16),
    vm(416, FZ, dtype=BF16), vm(416, FZ, dtype=BF16), vm(272, FZ, dtype=BF16),
    vm(6, SEG, FZ, dtype=BF16), vm(7 * FY + 16, FZ, dtype=BF16), vm(7 * FY + 16, FZ, dtype=BF16),
    vm(400, FZ, dtype=BF16), vm(400, FZ, dtype=BF16),
    vm(4 * FY, FZ, dtype=BF16), vm(4 * FY, FZ, dtype=BF16),
    vm(416, FZ, dtype=BF16), vm(416, FZ, dtype=BF16),
    vm(1, SEG, dtype=jnp.int32), vm(1, SEG, dtype=jnp.int32),
    *(vm(272, FZ, dtype=BF16) for _ in range(3)),
    vm(6, 80, FZ, dtype=BF16), vm(6, 80, FZ, dtype=BF16),
    vm(7 * FY + 16, FZ, dtype=BF16), vm(7 * FY + 16, FZ, dtype=BF16),
    vm(400, FZ, dtype=BF16), vm(400, FZ, dtype=BF16),
    vm(4 * FY, FZ, dtype=BF16), vm(4 * FY, FZ, dtype=BF16), vm(4, 32, FZ),
    pltpu.SemaphoreType.DMA((9,)), pltpu.SemaphoreType.DMA((19,)), pltpu.SemaphoreType.DMA((19,)),
]


STATE = (
    *(vm(40 * FY, FZ) for _ in range(4)), vm(2 * 320 + 64, FZ),
    *(vm(32 * SY, FZ) for _ in range(3)), vm(4 * 256, FZ),
)


def solution(mesh):
    n_grp, n_dom = mesh.shape["grp"], mesh.shape["dom"]

    def local(fs, fr, fc, ss, sr, sc, sb, ts, tf):
        state = pl.pallas_call(
            lambda *refs: kernel(n_grp, n_dom, *refs),
            out_shape=STATE,
            in_specs=[pl.BlockSpec(memory_space=pltpu.HBM)] * 9,
            out_specs=tuple(pl.BlockSpec(memory_space=pltpu.VMEM) for _ in STATE),
            scratch_shapes=SCRATCH,
            compiler_params=pltpu.CompilerParams(
                collective_id=0, has_side_effects=True, vmem_limit_bytes=57_114_624
            ),
            name="coupled",
        )(
            fs.reshape(FX * FY, FZ), fr.reshape(FX * FY, FZ), fc.reshape(FX, FZ),
            ss.reshape(SX * SY, FZ), sr.reshape(SX * SY, FZ), sc.reshape(SX, FZ),
            sb.reshape(1, SEG),
            ts.reshape(SEG * FZ, FZ), tf.reshape(SEG * FZ, FZ),
        )
        fo, so = pl.pallas_call(
            finish,
            out_shape=(
                jax.ShapeDtypeStruct((FX * FY, FZ), F32),
                jax.ShapeDtypeStruct((SX * SY, FZ), F32),
            ),
            in_specs=[pl.BlockSpec(memory_space=pltpu.VMEM)] * 9,
            out_specs=[pl.BlockSpec(memory_space=pltpu.HBM)] * 2,
            scratch_shapes=[
                vm(32 * FY, FZ), vm(32 * SY, FZ), vm(32 * SY, FZ), vm(2 * FZ, FZ, dtype=BF16),
                pltpu.SemaphoreType.DMA((4,)),
            ],
            compiler_params=pltpu.CompilerParams(vmem_limit_bytes=16 * 1024 * 1024),
            name="finish",
        )(*state)
        return fo.reshape(1, FX, FY, FZ), so.reshape(1, SX, SY, FZ)

    cells = P("grp", "dom", None, None)
    faces = P("grp", "dom", None)
    split = P(("grp", "dom"))
    mats = P(("grp", "dom"), None, None)
    return jax.shard_map(
        local,
        mesh=mesh,
        in_specs=(cells, cells, faces, cells, cells, faces, split, mats, mats),
        out_specs=(cells, cells),
        check_vma=False,
    )
```
